128 devices in a mesh: section: 4 (over x), dp: 32 (over y, z, core).
Axes of the slice: x: 4, y: 4, z: 4, core: 2. Of those that a mesh axis runs over, the one named last changes fastest.
Arguments:
- clip_pool: bfloat16 [1024, 256, 512], P('dp'), may hold values from -8 to 8
- clip_index: int32 [8, 128], P(None, 'dp'), may hold values from 0 to 31, as said below
- batch_order: int32 [8], replicated, may hold values from 0 to 7, each once
- tap_weights: bfloat16 [4, 3, 512, 512], P('section'), may hold values from -0.15625 to 0.15625
- out_weights: bfloat16 [4, 512, 512], P('section'), may hold values from -0.25 to 0.25
- norm_gains: bfloat16 [4, 512], P('section'), may hold values from 0.099609375 to 1.8984375
- quant_weight: bfloat16 [512, 18], replicated, may hold values from -0.25 to 0.25
- quant_bias: float32 [18], replicated, may hold values from -3 to 3
- post_weight: bfloat16 [18, 512], replicated, may hold values from -1.5 to 1.5
Outputs:
- row_error: float32 [8, 128, 256], P('section', 'dp')
- entropy_loss: float32 [8], replicated
The draws below stay inside these ranges and needn't reach their ends.
Inputs may be any that keep to these rules, and one draw needn't show every extreme that they name: `clip_index`: entries index the clips of the replica that holds the column; over all 8 micro-batches, the 4 columns of one replica name each of its 32 clips exactly once. `batch_order`: each micro-batch number 0 to 7 once.
All inputs are finite; a program needn't handle non-finite values.
Results may differ from the reference program's by a relative error of at most 0.0015.
Values may be sent and summed in bfloat16 or wider, within the bound.
No kernel may reach another device: no remote copies, remote signals or barrier semaphores. Data moves between devices by JAX's collectives and lax.ppermute only.
A program may use at most 128 MiB of HBM per device.

```python
import jax
import jax.numpy as jnp
from jax import lax

C = 512
BITS = 18
TAPS = 3
SPATIAL = 64
CLIPS = 4
MB = 8
POOL = 32
ROWS = 256
CL_ALL = 128
POOL_ALL = 1024
N_SECTION = 4


def draw_clip_pool(key, part):
    first, second, third = jax.random.split(jax.random.fold_in(key, 17), 3)
    offset = jax.random.normal(first, (POOL_ALL, 1, C), jnp.float32)
    noise = jax.random.normal(second, (POOL_ALL, ROWS, C), jnp.float32)
    value = jnp.clip(0.8 * offset + 0.6 * noise, -8.0, 8.0)
    return value.astype(jnp.bfloat16)


def draw_clip_index(key, part):
    groups = CL_ALL // CLIPS
    keys = jax.random.split(jax.random.fold_in(key, 29), groups)
    ordered = jnp.arange(POOL, dtype=jnp.int32)
    shuffled = jax.vmap(lambda single: jax.random.permutation(single, ordered))(keys)
    arranged = shuffled.reshape(groups, MB, CLIPS).transpose(1, 0, 2)
    return arranged.reshape(MB, CL_ALL).astype(jnp.int32)


def levels(stream_key, shape, pieces, least, high):
    level, own = 1.0, jax.random.fold_in(stream_key, 6)
    for dim, parts in pieces:
        draws = jnp.exp(jax.random.uniform(jax.random.fold_in(own, dim), (parts,), jnp.float32, least / len(pieces), high / len(pieces)))
        level = level * jnp.repeat(draws, shape[dim] // parts).reshape([-1 if axis == dim else 1 for axis in range(len(shape))])
    return level


def normal_values(key, extent, deviation, reach, shards=(), kind=jnp.bfloat16):
    drawn = deviation * jax.random.normal(key, extent, jnp.float32)
    if shards:
        drawn = drawn * levels(key, extent, shards, -0.22, 0.18)
    return jnp.clip(drawn, -reach, reach).astype(kind)


def setup_inputs(seed: int = 0) -> dict:
    splits = jax.random.split(jax.random.key(seed), 10)
    return {
        "clip_pool": draw_clip_pool(jax.random.fold_in(splits[9], 71), 0),
        "clip_index": draw_clip_index(jax.random.fold_in(splits[9], 71), 0),
        "batch_order": jax.random.permutation(splits[2], MB).astype(jnp.int32),
        "tap_weights": normal_values(splits[3], (N_SECTION, TAPS, C, C), (TAPS * C) ** -0.5, 0.15625, ((0, 4),)),
        "out_weights": normal_values(splits[4], (N_SECTION, C, C), C ** -0.5, 0.25, ((0, 4),)),
        "norm_gains": jnp.clip(1.0 + 0.18 * jax.random.normal(splits[5], (N_SECTION, C), jnp.float32), 0.099609375, 1.8984375).astype(jnp.bfloat16),
        "quant_weight": normal_values(splits[6], (C, BITS), C ** -0.5, 0.25),
        "quant_bias": normal_values(splits[7], (BITS,), 1.0, 3.0, (), jnp.float32),
        "post_weight": normal_values(splits[8], (BITS, C), BITS ** -0.5, 1.5),
    }


norm_eps = 1e-06
quant_section = 1

def run_block(current, tap_set, out_weight, gain_row):
    clip_count, row_count, channels = current.shape
    widened = current.astype(jnp.float32)
    scale = lax.rsqrt(lax.optimization_barrier(jnp.mean(widened * widened, axis=-1, keepdims=True)) + norm_eps)
    normed = (widened * scale * gain_row.astype(jnp.float32)).astype(jnp.bfloat16)
    flat = normed.reshape(-1, channels)
    mixed = jnp.zeros((clip_count, row_count, channels), jnp.float32)
    for k in range(tap_set.shape[0]):
        product = jnp.dot(flat, tap_set[k], preferred_element_type=jnp.float32).reshape(clip_count, row_count, channels)
        moved = jnp.pad(product, ((0, 0), (k * SPATIAL, 0), (0, 0)))[:, :row_count]
        mixed = mixed + moved
    activated = jax.nn.silu(mixed).astype(jnp.bfloat16)
    update = jnp.dot(activated.reshape(-1, channels), out_weight, preferred_element_type=jnp.float32)
    return (widened + update.reshape(clip_count, row_count, channels)).astype(jnp.bfloat16)

def quantize(current, quant_weight, quant_bias, post_weight):
    channels = current.shape[-1]
    logits = jnp.dot(current.reshape(-1, channels), quant_weight, preferred_element_type=jnp.float32) + quant_bias
    bit_prob = jax.nn.sigmoid(4.0 * logits)
    codes = (2.0 * bit_prob - 1.0).astype(jnp.bfloat16)
    quantized = jnp.dot(codes, post_weight, preferred_element_type=jnp.float32).astype(jnp.bfloat16)
    bit_sums = lax.optimization_barrier(jnp.sum(bit_prob, axis=0))
    entropy_sum = -jnp.sum(bit_prob * jax.nn.log_sigmoid(4.0 * logits) + (1.0 - bit_prob) * jax.nn.log_sigmoid(-4.0 * logits))
    return (quantized.reshape(current.shape), bit_sums, entropy_sum)

def squared_error(decoded, source):
    differ = decoded.astype(jnp.float32) - source.astype(jnp.float32)
    return lax.optimization_barrier(jnp.mean(differ * differ, axis=-1))

def final_entropy(bit_buffer, entropy_buffer, batch_order, rows_total):
    marginal = bit_buffer / rows_total
    sample_entropy = entropy_buffer / rows_total
    averaged = jnp.zeros_like(marginal)
    running = marginal[batch_order[0]]
    for t in range(batch_order.shape[0]):
        if t > 0:
            running = 0.5 * running + 0.5 * marginal[batch_order[t]]
        averaged = averaged.at[batch_order[t]].set(running)
    smoothed = 0.05 + 0.9 * averaged
    code_entropy = -lax.optimization_barrier(jnp.sum(smoothed * jnp.log(smoothed) + (1.0 - smoothed) * jnp.log(1.0 - smoothed), axis=-1))
    return sample_entropy - code_entropy

def reference(clip_pool, clip_index, batch_order, tap_weights, out_weights, norm_gains, quant_weight, quant_bias, post_weight):
    replica = jnp.arange(CL_ALL, dtype=jnp.int32) // CLIPS
    error_list = []
    bit_list = []
    entropy_list = []
    for j in range(MB):
        chosen = (replica * POOL + clip_index[j]).astype(jnp.int32)
        source = clip_pool[chosen]
        current = source
        for s in range(N_SECTION):
            current = run_block(current, tap_weights[s], out_weights[s], norm_gains[s])
            if s == quant_section:
                current, bit_sums, entropy_sum = quantize(current, quant_weight, quant_bias, post_weight)
                bit_list.append(bit_sums)
                entropy_list.append(entropy_sum)
        error_list.append(squared_error(current, source))
    rows_total = float(CL_ALL * ROWS)
    losses = final_entropy(jnp.stack(bit_list), jnp.stack(entropy_list), batch_order, rows_total)
    return (jnp.stack(error_list), losses)
```

```python
import functools

import jax
import jax.numpy as jnp
from jax import lax
from jax.experimental import pallas as pl
from jax.experimental.pallas import tpu as pltpu
from jax.sharding import Mesh
from jax.sharding import PartitionSpec as P


DP = ("dp_0", "dp_1", "dp_2")
EPS = 1e-06
C = 512
BITS = 18
FRAME = 64
ROWS = 256
CLIPS = 4
FRAMES = ROWS // FRAME
ORDER_A = (0, 1, 2, 6, 7)
ORDER_B = (3, 4, 5)
HALF = 1024
PIECE = HALF + 16
VM = pl.BlockSpec(memory_space=pltpu.VMEM)
SM = pl.BlockSpec(memory_space=pltpu.SMEM)
HB = pl.BlockSpec(memory_space=pl.ANY)


def call(body, ins, outs, scratch=(), limit=24, name=None):
    return pl.pallas_call(
        body,
        in_specs=list(ins),
        out_specs=[VM] * len(outs),
        out_shape=[jax.ShapeDtypeStruct(shape, kind) for shape, kind in outs],
        scratch_shapes=list(scratch),
        compiler_params=pltpu.CompilerParams(vmem_limit_bytes=limit * 2**20),
        name=name,
    )


def run_block(src, dst, taps, out_weight, half_gain):
    frames = [
        src[:, f * FRAME : (f + 1) * FRAME, :].reshape(CLIPS * FRAME, C) for f in range(FRAMES)
    ]
    normed = []
    for v in frames:
        w = v.astype(jnp.float32)
        mean = jnp.mean(w * w, axis=-1, keepdims=True)
        normed.append((w * lax.rsqrt(mean + EPS) * half_gain).astype(jnp.bfloat16))
    first = jnp.dot(normed[0], taps(C), preferred_element_type=jnp.float32)
    second = jnp.dot(
        jnp.concatenate([normed[1], normed[0]], axis=1),
        taps(2 * C),
        preferred_element_type=jnp.float32,
    )
    rest = jnp.concatenate(
        [
            jnp.concatenate([normed[f], normed[f - 1], normed[f - 2]], axis=1)
            for f in range(2, FRAMES)
        ],
        axis=0,
    )
    third = jnp.dot(rest, taps(3 * C), preferred_element_type=jnp.float32)
    h = jnp.concatenate([first, second, third], axis=0)
    activated = (h + h * jnp.tanh(h)).astype(jnp.bfloat16)
    update = jnp.dot(activated, out_weight(), preferred_element_type=jnp.float32)
    for f in range(FRAMES):
        part = update[f * CLIPS * FRAME : (f + 1) * CLIPS * FRAME]
        dst[:, f * FRAME : (f + 1) * FRAME, :] = (
            (frames[f].astype(jnp.float32) + part)
            .astype(jnp.bfloat16)
            .reshape(CLIPS, FRAME, C)
        )


def prep_body(taps, out_weight, gain, piece, sems):
    colour = lax.rem(lax.axis_index("dp_0") + 2 * lax.axis_index("dp_1"), 4)
    at = pl.ds(pl.multiple_of(colour * 128, 128), 128)
    core = lax.axis_index("dp_2")

    @pl.when(core == 0)
    def _():
        copy = pltpu.make_async_copy(
            taps.at[pl.ds(0, HALF), at], piece.at[pl.ds(0, HALF)], sems.at[0]
        )
        copy.start()
        copy.wait()

    @pl.when(core == 1)
    def _():
        copies = [
            pltpu.make_async_copy(
                taps.at[pl.ds(HALF, 512), at], piece.at[pl.ds(0, 512)], sems.at[0]
            )
        ]
        for j in range(4):
            copies.append(
                pltpu.make_async_copy(
                    out_weight.at[at, pl.ds(128 * j, 128)],
                    piece.at[pl.ds(512 + 128 * j, 128)],
                    sems.at[1 + j],
                )
            )
        for copy in copies:
            copy.start()
        for copy in copies:
            copy.wait()

    wide = gain[...].astype(jnp.float32)
    rows = [wide[:, 128 * j : 128 * (j + 1)] for j in range(4)]
    rows.append(jnp.zeros((12, 128), jnp.float32))
    piece[HALF:, :] = jnp.concatenate(rows, axis=0).astype(jnp.bfloat16)


def load_body(steps, pool, index, taps, out_weight, gain, v, sems):
    section = lax.axis_index("section")
    outer = (section == 0) | (section == 3)
    copies = []
    for i, t in enumerate(steps):
        batch = jnp.where(outer, ORDER_A[t], ORDER_B[t % 3])
        for c in range(CLIPS):
            copy = pltpu.make_async_copy(
                pool.at[index[batch, c]], v.at[i, c], sems.at[i * CLIPS + c]
            )
            copy.start()
            copies.append(copy)
    half_gain = 0.5 * gain[...].astype(jnp.float32)
    for i in range(len(steps)):
        for c in range(CLIPS):
            copies[i * CLIPS + c].wait()

    @pl.when(section == 0)
    def _():
        def step(i, _):
            run_block(
                v.at[i],
                v.at[i],
                lambda k: taps[:k, :],
                lambda: out_weight[...],
                half_gain,
            )
            return 0

        lax.fori_loop(0, len(steps), step, 0)


def join_body(taps, out_weight, gain, *rest):
    pieces, (all_taps, all_out, all_gain), sems = rest[:8], rest[8:11], rest[11]
    section = lax.axis_index("section")
    core = lax.axis_index("dp_2")
    own = lax.rem(section, 2)
    other = 1 - own
    own_copies = [
        pltpu.make_async_copy(taps, all_taps.at[own], sems.at[0]),
        pltpu.make_async_copy(out_weight, all_out.at[own], sems.at[1]),
    ]
    for copy in own_copies:
        copy.start()

    def place(lower, upper):
        copies = []
        for j in range(4):
            lanes = pl.ds(128 * j, 128)
            copies.append(
                pltpu.make_async_copy(
                    lower[j].at[pl.ds(0, HALF)],
                    all_taps.at[other, pl.ds(0, HALF), lanes],
                    sems.at[2 + j],
                )
            )
            copies.append(
                pltpu.make_async_copy(
                    upper[j].at[pl.ds(0, 512)],
                    all_taps.at[other, pl.ds(HALF, 512), lanes],
                    sems.at[6 + j],
                )
            )
            for k in range(4):
                copies.append(
                    pltpu.make_async_copy(
                        upper[j].at[pl.ds(512 + 128 * k, 128)],
                        all_out.at[other, pl.ds(128 * j, 128), pl.ds(128 * k, 128)],
                        sems.at[10 + 4 * j + k],
                    )
                )
        for copy in copies:
            copy.start()
        for copy in copies:
            copy.wait()

    @pl.when(core == 0)
    def _():
        place(pieces[:4], pieces[4:])

    @pl.when(core == 1)
    def _():
        place(pieces[4:], pieces[:4])

    all_gain[own] = jnp.broadcast_to(0.5 * gain[...].astype(jnp.float32), (8, C))
    rows = pieces[0][HALF:, :].astype(jnp.float32)
    row = jnp.concatenate([rows[k : k + 1, :] for k in range(4)], axis=1)
    all_gain[other] = jnp.broadcast_to(0.5 * row, (8, C))
    for copy in own_copies:
        copy.wait()


def block_at(b, buf, all_taps, all_out, all_gain):
    run_block(
        buf,
        buf,
        lambda k: all_taps[b, :k, :],
        lambda: all_out[b],
        all_gain[b, 0:1, :],
    )


def encode_body(steps, base, v, all_taps, all_out, all_gain, qw, qb, before, codes, stats, buf):
    section = lax.axis_index("section")
    stats[...] = before[...]
    bias = qb[:, 0:1]
    row = lax.broadcasted_iota(jnp.int32, (32, CLIPS * ROWS), 0)
    top = lax.broadcasted_iota(jnp.int32, (32, 128), 0)
    lane = lax.broadcasted_iota(jnp.int32, (32, 128), 1)

    def chunk(i, t):
        buf[...] = v[base + i]

        def step(b, _):
            block_at(b, buf, all_taps, all_out, all_gain)
            return 0

        lax.fori_loop(1 - section, 2, step, 0)
        logits = jnp.dot(
            buf[...].reshape(CLIPS * ROWS, C), qw[...], preferred_element_type=jnp.float32
        )
        z = 4.0 * (logits.T[:32] + bias)
        size = jnp.abs(z)
        e = jnp.exp(-size)
        r = 1.0 / (1.0 + e)
        p = jnp.where(z >= 0, r, e * r)
        entropy = jnp.log1p(e) + size * (e * r)
        valid = row < BITS
        codes[i] = jnp.where(valid, 2.0 * p - 1.0, 0.0).astype(jnp.bfloat16)
        bit_sums = jnp.sum(jnp.where(valid, p, 0.0), axis=1, keepdims=True)
        total = jnp.sum(
            jnp.sum(jnp.where(valid, entropy, 0.0), axis=1, keepdims=True), axis=0, keepdims=True
        )
        column = jnp.where(top == BITS, total, bit_sums)
        batch = jnp.where(section == 0, ORDER_A[t], ORDER_B[t % 3])
        stats[...] += jnp.where(lane == batch, column, 0.0)

    for i, t in enumerate(steps):
        active = section <= 1 if t < len(ORDER_B) else section == 0
        pl.when(active)(functools.partial(chunk, i, t))


def decode_body(steps, base, v, all_taps, all_out, all_gain, post, codes, errors, buf):
    section = lax.axis_index("section")

    def chunk(i, t):
        quantized = lax.dot_general(
            codes[i], post[...], (((0,), (0,)), ((), ())), preferred_element_type=jnp.float32
        )
        buf[...] = quantized.astype(jnp.bfloat16).reshape(CLIPS, ROWS, C)

        def step(b, _):
            block_at(b, buf, all_taps, all_out, all_gain)
            return 0

        lax.fori_loop(0, 2, step, 0)
        for c in range(CLIPS):
            differ = buf[c].astype(jnp.float32) - v[base + i, c].astype(jnp.float32)
            square = differ * differ
            part = (
                square[:, :128] + square[:, 128:256] + square[:, 256:384] + square[:, 384:]
            )
            errors[i, c : c + 1, :] = jnp.sum(part.T, axis=0, keepdims=True) * (1.0 / C)

    for i, t in enumerate(steps):
        active = section >= 2 if t < len(ORDER_B) else section == 3
        pl.when(active)(functools.partial(chunk, i, t))


def final_body(rows_total, order, own, near, far_a, far_b, e01, e2, e34, err_a, err_b, error, loss):
    sums = (own[...] + near[...] + far_a[...] + far_b[...]) * (1.0 / rows_total)
    lane = lax.broadcasted_iota(jnp.int32, sums.shape, 1)
    averaged = jnp.zeros_like(sums)
    running = None
    for t in range(8):
        here = lane == order[t]
        marginal = jnp.sum(jnp.where(here, sums, 0.0), axis=1, keepdims=True)
        running = marginal if t == 0 else 0.5 * running + 0.5 * marginal
        averaged = jnp.where(here, running, averaged)
    smoothed = 0.05 + 0.9 * averaged
    row = lax.broadcasted_iota(jnp.int32, sums.shape, 0)
    smoothed = jnp.where(row < BITS, smoothed, 0.5)
    term = smoothed * jnp.log(smoothed) + (1.0 - smoothed) * jnp.log(1.0 - smoothed)
    code = jnp.sum(jnp.where(row < BITS, term, 0.0), axis=0, keepdims=True)
    loss[...] = sums[BITS : BITS + 1, :] + code

    section = lax.axis_index("section")

    @pl.when(section == 0)
    def _():
        error[...] = err_a[...]

    @pl.when(section == 1)
    def _():
        error[0] = err_b[0]
        error[1] = err_a[0]

    @pl.when(section == 2)
    def _():
        error[0] = e01[1]
        error[1] = e2[0]

    @pl.when(section == 3)
    def _():
        error[...] = e34[...]


PAIR = ((0, 1), (1, 0), (2, 3), (3, 2))
CROSS = ((1, 2), (2, 1), (3, 0), (0, 3))
ENCODERS = (0, 1)


def shifted(x, axis, by):
    n = lax.axis_size(axis)
    return lax.ppermute(x, axis, [(i, (i + by) % n) for i in range(n)])


def split_shift(x, axis):
    n = lax.axis_size(axis)
    pairs = []
    for i in range(n):
        pairs.append((2 * i, 2 * ((i + 1) % n)))
        pairs.append((2 * i + 1, 2 * ((i - 1) % n) + 1))
    return lax.ppermute(x, (axis, "dp_2"), pairs)


def among_encoders(x, axis, pairs):
    n = lax.axis_size(axis)
    return lax.ppermute(
        x, ("section", axis), [(s * n + a, s * n + b) for s in ENCODERS for a, b in pairs]
    )


def on_device(pool, index, order, taps, out_weight, gain, quant_weight, quant_bias, post_weight):
    bf16, f32 = jnp.bfloat16, jnp.float32
    taps = taps.reshape(3 * C, C)
    out_weight = out_weight.reshape(C, C)
    dma = pltpu.SemaphoreType.DMA
    qw = jnp.pad(quant_weight, ((0, 0), (0, 128 - BITS)))
    qb = jnp.broadcast_to(jnp.pad(quant_bias, (0, 32 - BITS))[:, None], (32, 128))
    post = jnp.pad(post_weight, ((0, 32 - BITS), (0, 0)))

    def load(steps, index):
        n = len(steps)
        return call(
            functools.partial(load_body, steps),
            [HB, SM, VM, VM, VM],
            [((n, CLIPS, ROWS, C), bf16)],
            [dma((n * CLIPS,))],
            name="load_%d" % steps[0],
        )(pool, index, taps, out_weight, gain)[0]

    (piece,) = call(
        prep_body, [HB, HB, VM], [((PIECE, 128), bf16)], [dma((5,))], name="prep"
    )(taps, out_weight, gain)
    mine = lax.ppermute(piece, "section", PAIR)
    v_a = load((0, 1, 2), index)
    mine, v_a, index = lax.optimization_barrier((mine, v_a, index))
    up = shifted(mine, "dp_0", 1)
    down = shifted(mine, "dp_0", -1)
    side = split_shift(mine, "dp_1")
    mine_s = shifted(mine, "dp_2", 1)
    v_b = load((3, 4), index)
    up, down, side, mine_s, v_b = lax.optimization_barrier((up, down, side, mine_s, v_b))
    swapped = [mine_s] + [shifted(x, "dp_2", 1) for x in (up, down, side)]
    weights = call(
        join_body,
        [HB, HB, VM, VM] + [HB] * 7,
        [((2, 3 * C, C), bf16), ((2, C, C), bf16), ((2, 8, C), f32)],
        [dma((26,))],
        name="join",
    )(taps, out_weight, gain, mine, up, down, side, *swapped)

    def encode(steps, base, v, before):
        n = len(steps)
        return call(
            functools.partial(encode_body, steps, base),
            [VM] * 7,
            [((n, 32, CLIPS * ROWS), bf16), ((32, 128), f32)],
            [pltpu.VMEM((CLIPS, ROWS, C), bf16)],
            name="encode_%d" % steps[0],
        )(v, *weights, qw, qb, before)

    def decode(steps, base, v, codes):
        n = len(steps)
        return call(
            functools.partial(decode_body, steps, base),
            [VM] * 6,
            [((n, CLIPS, ROWS), f32)],
            [pltpu.VMEM((CLIPS, ROWS, C), bf16)],
            name="decode_%d" % steps[0],
        )(v, *weights, post, codes)[0]

    def ship(codes):
        return lax.ppermute(codes, "section", [(0, 3), (1, 2)])

    zero = jnp.zeros((32, 128), f32)
    codes, stats = encode((0, 1), 0, v_a, zero)
    codes01 = ship(codes)
    codes, stats = encode((2,), 2, v_a, stats)
    codes2 = ship(codes)
    codes, stats = encode((3, 4), 0, v_b, stats)
    codes34 = ship(codes)
    codes01, stats = lax.optimization_barrier((codes01, stats))
    e01 = decode((0, 1), 0, v_a, codes01)
    e2 = decode((2,), 2, v_a, codes2)
    err_a = lax.ppermute(e01, "section", [(3, 0), (2, 1)])
    err_b = lax.ppermute(e2, "section", [(3, 1)])
    stats, e2 = lax.optimization_barrier((stats, e2))
    total = stats
    total = total + among_encoders(total, "dp_2", [(0, 1), (1, 0)])
    for axis in ("dp_0", "dp_1"):
        total = total + among_encoders(total, axis, PAIR)
        total = total + among_encoders(total, axis, CROSS)
    near = lax.ppermute(total, "section", [(0, 1), (1, 0)])
    far_a = lax.ppermute(total, "section", [(0, 2), (1, 3)])
    far_b = lax.ppermute(total, "section", [(0, 3), (1, 2)])
    e34 = decode((3, 4), 0, v_b, codes34)
    rows_total = float(index.shape[1] * lax.axis_size(DP) * ROWS)
    error, loss = call(
        functools.partial(final_body, rows_total),
        [SM] + [VM] * 9,
        [((2, CLIPS, ROWS), f32), ((1, 128), f32)],
        name="final",
    )(order, total, near, far_a, far_b, e01, e2, e34, err_a, err_b)
    return error, loss[0, : order.shape[0]]


def solution(mesh):
    torus = Mesh(
        mesh.devices.reshape(mesh.shape["section"], 4, 4, 2), ("section", "dp_0", "dp_1", "dp_2")
    )
    return jax.shard_map(
        on_device,
        mesh=torus,
        in_specs=(
            P(DP, None, None),
            P(None, DP),
            P(),
            P("section", None, None, None),
            P("section", None, None),
            P("section", None),
            P(),
            P(),
            P(),
        ),
        out_specs=(P("section", DP, None), P()),
        check_vma=False,
    )
```

```python
import functools

import jax
import jax.numpy as jnp
from jax import lax
from jax.experimental import pallas as pl
from jax.experimental.pallas import tpu as pltpu
from jax.sharding import Mesh
from jax.sharding import PartitionSpec as P


DP = ("dp_0", "dp_1", "dp_2")
EPS = 1e-06
C = 512
BITS = 18
FRAME = 64
ROWS = 256
CLIPS = 4
FRAMES = ROWS // FRAME
ORDER_A = (0, 1, 2, 6, 7)
ORDER_B = (3, 4, 5)
HALF = 1024
PIECE = HALF + 16
VM = pl.BlockSpec(memory_space=pltpu.VMEM)
SM = pl.BlockSpec(memory_space=pltpu.SMEM)
HB = pl.BlockSpec(memory_space=pltpu.HBM)
ANY = pl.BlockSpec(memory_space=pl.ANY)


def call(body, ins, outs, scratch=(), limit=24, name=None, aliases={}, blocks=0):
    return pl.pallas_call(
        body,
        in_specs=list(ins),
        out_specs=[VM] * len(outs),
        out_shape=[jax.ShapeDtypeStruct(shape, kind) for shape, kind in outs],
        scratch_shapes=list(scratch),
        compiler_params=pltpu.CompilerParams(vmem_limit_bytes=limit * 2**20),
        name=name,
        input_output_aliases=aliases,
        cost_estimate=pl.CostEstimate(
            flops=blocks * CLIPS * ROWS * C * C * 8, transcendentals=0, bytes_accessed=0
        ),
    )


def run_block(src, dst, taps, out_weight, half_gain):
    frames = [
        src[:, f * FRAME : (f + 1) * FRAME, :].reshape(CLIPS * FRAME, C) for f in range(FRAMES)
    ]
    normed = []
    for v in frames:
        w = v.astype(jnp.float32)
        mean = jnp.mean(w * w, axis=-1, keepdims=True)
        normed.append((w * lax.rsqrt(mean + EPS) * half_gain).astype(jnp.bfloat16))
    first = jnp.dot(normed[0], taps(C), preferred_element_type=jnp.float32)
    second = jnp.dot(
        jnp.concatenate([normed[1], normed[0]], axis=1),
        taps(2 * C),
        preferred_element_type=jnp.float32,
    )
    rest = jnp.concatenate(
        [
            jnp.concatenate([normed[f], normed[f - 1], normed[f - 2]], axis=1)
            for f in range(2, FRAMES)
        ],
        axis=0,
    )
    third = jnp.dot(rest, taps(3 * C), preferred_element_type=jnp.float32)
    h = jnp.concatenate([first, second, third], axis=0)
    activated = (h + h * jnp.tanh(h)).astype(jnp.bfloat16)
    update = jnp.dot(activated, out_weight(), preferred_element_type=jnp.float32)
    for f in range(FRAMES):
        part = update[f * CLIPS * FRAME : (f + 1) * CLIPS * FRAME]
        dst[:, f * FRAME : (f + 1) * FRAME, :] = (
            (frames[f].astype(jnp.float32) + part)
            .astype(jnp.bfloat16)
            .reshape(CLIPS, FRAME, C)
        )


def prep_body(taps, out_weight, gain, piece, sems):
    colour = lax.rem(lax.axis_index("dp_0") + 2 * lax.axis_index("dp_1"), 4)
    at = pl.ds(pl.multiple_of(colour * 128, 128), 128)
    core = lax.axis_index("dp_2")

    @pl.when(core == 0)
    def _():
        copy = pltpu.make_async_copy(
            taps.at[pl.ds(0, HALF), at], piece.at[pl.ds(0, HALF)], sems.at[0]
        )
        copy.start()
        copy.wait()

    @pl.when(core == 1)
    def _():
        copies = [
            pltpu.make_async_copy(
                taps.at[pl.ds(HALF, 512), at], piece.at[pl.ds(0, 512)], sems.at[0]
            )
        ]
        for j in range(4):
            copies.append(
                pltpu.make_async_copy(
                    out_weight.at[at, pl.ds(128 * j, 128)],
                    piece.at[pl.ds(512 + 128 * j, 128)],
                    sems.at[1 + j],
                )
            )
        for copy in copies:
            copy.start()
        for copy in copies:
            copy.wait()

    wide = gain[...].astype(jnp.float32)
    rows = [wide[:, 128 * j : 128 * (j + 1)] for j in range(4)]
    rows.append(jnp.zeros((12, 128), jnp.float32))
    piece[HALF:, :] = jnp.concatenate(rows, axis=0).astype(jnp.bfloat16)


def start_body(
    steps, pool, index, taps, out_weight, gain, qwt, qbias, postw,
    v, all_taps, all_out, all_gain, qw, qb, post, sems,
):
    own = lax.rem(lax.axis_index("section"), 2)
    own_copies = [
        pltpu.make_async_copy(taps, all_taps.at[own], sems.at[0]),
        pltpu.make_async_copy(out_weight, all_out.at[own], sems.at[1]),
    ]
    for copy in own_copies:
        copy.start()
    copies = load_clips(steps, pool, index, v, sems, 2)
    half_gain = 0.5 * gain[...].astype(jnp.float32)
    all_gain[own] = jnp.broadcast_to(half_gain, (8, C))
    wide = jnp.concatenate(
        [qwt[...].astype(jnp.float32), jnp.zeros((128 - BITS, C), jnp.float32)], axis=0
    )
    qw[...] = wide.T.astype(jnp.bfloat16)
    qb[...] = jnp.zeros((8, 128), jnp.float32)
    qb[0:1, 0:BITS] = qbias[...]
    post[...] = jnp.zeros((32, C), jnp.bfloat16)
    post[0:BITS, :] = postw[...]
    for copy in own_copies:
        copy.wait()
    for copy in copies:
        copy.wait()
    first_block(steps, v, all_taps, all_out, all_gain)


def load_clips(steps, pool, index, v, sems, at):
    section = lax.axis_index("section")
    outer = (section == 0) | (section == 3)
    copies = []
    for i, t in enumerate(steps):
        batch = jnp.where(outer, ORDER_A[t], ORDER_B[t % 3])
        for c in range(CLIPS):
            copy = pltpu.make_async_copy(
                pool.at[index[c, batch]], v.at[i, c], sems.at[at + i * CLIPS + c]
            )
            copy.start()
            copies.append(copy)
    return copies


def first_block(steps, v, all_taps, all_out, all_gain):
    @pl.when(lax.axis_index("section") == 0)
    def _():
        def step(i, _):
            block_at(0, v.at[i], all_taps, all_out, all_gain)
            return 0

        lax.fori_loop(0, len(steps), step, 0)


def load_body(steps, pool, index, all_taps, all_out, all_gain, v, sems):
    for copy in load_clips(steps, pool, index, v, sems, 0):
        copy.wait()
    first_block(steps, v, all_taps, all_out, all_gain)


def join_body(*refs):
    pieces, (all_taps, all_out, all_gain), sems = refs[:8], refs[11:14], refs[14]
    section = lax.axis_index("section")
    core = lax.axis_index("dp_2")
    other = 1 - lax.rem(section, 2)

    def place(lower, upper):
        copies = []
        for j in range(4):
            lanes = pl.ds(128 * j, 128)
            copies.append(
                pltpu.make_async_copy(
                    lower[j].at[pl.ds(0, HALF)],
                    all_taps.at[other, pl.ds(0, HALF), lanes],
                    sems.at[j],
                )
            )
            copies.append(
                pltpu.make_async_copy(
                    upper[j].at[pl.ds(0, 512)],
                    all_taps.at[other, pl.ds(HALF, 512), lanes],
                    sems.at[4 + j],
                )
            )
            for k in range(4):
                copies.append(
                    pltpu.make_async_copy(
                        upper[j].at[pl.ds(512 + 128 * k, 128)],
                        all_out.at[other, pl.ds(128 * j, 128), pl.ds(128 * k, 128)],
                        sems.at[8 + 4 * j + k],
                    )
                )
        for copy in copies:
            copy.start()
        for copy in copies:
            copy.wait()

    @pl.when(core == 0)
    def _():
        place(pieces[:4], pieces[4:])

    @pl.when(core == 1)
    def _():
        place(pieces[4:], pieces[:4])

    rows = pieces[0][HALF:, :].astype(jnp.float32)
    row = jnp.concatenate([rows[k : k + 1, :] for k in range(4)], axis=1)
    all_gain[other] = jnp.broadcast_to(0.5 * row, (8, C))


def block_at(b, buf, all_taps, all_out, all_gain):
    run_block(
        buf,
        buf,
        lambda k: all_taps[b, :k, :],
        lambda: all_out[b],
        all_gain[b, 0:1, :],
    )


def encode_body(steps, last, v, all_taps, all_out, all_gain, qw, qb, before, codes, stats, buf, sums):
    section = lax.axis_index("section")
    sums[...] = before[...]
    row = lax.broadcasted_iota(jnp.int32, (32, CLIPS * ROWS), 0)
    top = lax.broadcasted_iota(jnp.int32, (32, 128), 0)
    lane = lax.broadcasted_iota(jnp.int32, (32, 128), 1)

    def chunk(i, t):
        buf[...] = v[i]

        def step(b, _):
            block_at(b, buf, all_taps, all_out, all_gain)
            return 0

        lax.fori_loop(1 - section, 2, step, 0)
        logits = jnp.dot(
            buf[...].reshape(CLIPS * ROWS, C), qw[...], preferred_element_type=jnp.float32
        )
        z = (4.0 * (logits + qb[0:1, :])).T[:32]
        size = jnp.abs(z)
        e = jnp.exp(-size)
        r = 1.0 / (1.0 + e)
        p = jnp.where(z >= 0, r, e * r)
        entropy = jnp.log1p(e) + size * (e * r)
        valid = row < BITS
        codes[i] = jnp.where(valid, 2.0 * p - 1.0, 0.0).astype(jnp.bfloat16)
        bit_sums = jnp.sum(jnp.where(valid, p, 0.0), axis=1, keepdims=True)
        total = jnp.sum(
            jnp.sum(jnp.where(valid, entropy, 0.0), axis=1, keepdims=True), axis=0, keepdims=True
        )
        column = jnp.where(top == BITS, total, bit_sums)
        batch = jnp.where(section == 0, ORDER_A[t], ORDER_B[t % 3])
        sums[...] += jnp.where(lane == batch, column, 0.0)

    for i, t in enumerate(steps):
        active = section <= 1 if t < len(ORDER_B) else section == 0
        pl.when(active)(functools.partial(chunk, i, t))

    if last:
        full = jnp.concatenate([sums[...], jnp.zeros((96, 128), jnp.float32)], axis=0)
        stats[...] = full.T[:8]
    else:
        stats[...] = sums[...]


def decode_chunks(steps, v, all_taps, all_out, all_gain, post, codes, errors, buf):
    section = lax.axis_index("section")

    def chunk(i, t):
        quantized = lax.dot_general(
            codes[i], post[...], (((0,), (0,)), ((), ())), preferred_element_type=jnp.float32
        )
        buf[...] = quantized.astype(jnp.bfloat16).reshape(CLIPS, ROWS, C)

        def step(b, _):
            block_at(b, buf, all_taps, all_out, all_gain)
            return 0

        lax.fori_loop(0, 2, step, 0)
        for c in range(CLIPS):
            differ = buf[c].astype(jnp.float32) - v[i, c].astype(jnp.float32)
            square = differ * differ
            part = (
                square[:, :128] + square[:, 128:256] + square[:, 256:384] + square[:, 384:]
            )
            mean = jnp.sum(part.T, axis=0, keepdims=True) * (1.0 / C)
            errors(i, c, mean)

    for i, t in enumerate(steps):
        active = section >= 2 if t < len(ORDER_B) else section == 3
        pl.when(active)(functools.partial(chunk, i, t))


def decode_body(steps, v, all_taps, all_out, all_gain, post, codes, errors, buf):
    def put(i, c, mean):
        errors[i, 2 * c : 2 * c + 1, :] = mean[:, :128]
        errors[i, 2 * c + 1 : 2 * c + 2, :] = mean[:, 128:]

    decode_chunks(steps, v, all_taps, all_out, all_gain, post, codes, put, buf)


def decode_last_body(
    steps, v, all_taps, all_out, all_gain, post, codes, e01, packed, own, buf
):
    packed[0:8] = e01[0]
    packed[8:16] = e01[1]

    def put(i, c, mean):
        if i == 0:
            packed[16 + 2 * c : 17 + 2 * c, :] = mean[:, :128]
            packed[17 + 2 * c : 18 + 2 * c, :] = mean[:, 128:]
        own[i, c : c + 1, :] = mean

    decode_chunks(steps, v, all_taps, all_out, all_gain, post, codes, put, buf)


def unpack(target, source, at):
    for c in range(CLIPS):
        row = source[at + 2 * c : at + 2 * c + 2, :]
        target[c : c + 1, :] = jnp.concatenate([row[0:1], row[1:2]], axis=1)


def final_body(rows_total, order, mine, next_, cross, far, own, error, loss):
    section = lax.axis_index("section")
    a, b, c, d = mine[0:8], next_[0:8], cross[0:8], far[0:8]
    sums = (jnp.where(section <= 1, a + b, c + d)) * (1.0 / rows_total)
    row = lax.broadcasted_iota(jnp.int32, sums.shape, 0)
    lane = lax.broadcasted_iota(jnp.int32, sums.shape, 1)
    averaged = jnp.zeros_like(sums)
    running = None
    for t in range(8):
        here = row == order[t]
        marginal = jnp.sum(jnp.where(here, sums, 0.0), axis=0, keepdims=True)
        running = marginal if t == 0 else 0.5 * running + 0.5 * marginal
        averaged = jnp.where(here, running, averaged)
    smoothed = jnp.where(lane < BITS, 0.05 + 0.9 * averaged, 0.5)
    term = smoothed * jnp.log(smoothed) + (1.0 - smoothed) * jnp.log(1.0 - smoothed)
    term = jnp.where(lane < BITS, term, jnp.where(lane == BITS, sums, 0.0))
    result = jnp.sum(term, axis=1, keepdims=True)
    loss[...] = jnp.sum(jnp.where(row == lane, result, 0.0), axis=0, keepdims=True)

    @pl.when(section == 0)
    def _():
        unpack(error.at[0], cross, 8)
        unpack(error.at[1], cross, 16)

    @pl.when(section == 1)
    def _():
        unpack(error.at[0], far, 24)
        unpack(error.at[1], cross, 8)

    @pl.when(section == 2)
    def _():
        unpack(error.at[0], mine, 16)
        error[1] = own[0]

    @pl.when(section == 3)
    def _():
        error[0] = own[1]
        error[1] = own[2]


PAIR = ((0, 1), (1, 0), (2, 3), (3, 2))
CROSS = ((0, 3), (3, 0), (1, 2), (2, 1))
FAR = ((0, 2), (2, 0), (1, 3), (3, 1))


def shifted(x, axis, by):
    n = lax.axis_size(axis)
    return lax.ppermute(x, axis, [(i, (i + by) % n) for i in range(n)])


def split_shift(x, axis):
    n = lax.axis_size(axis)
    pairs = []
    for i in range(n):
        pairs.append((2 * i, 2 * ((i + 1) % n)))
        pairs.append((2 * i + 1, 2 * ((i - 1) % n) + 1))
    return lax.ppermute(x, (axis, "dp_2"), pairs)


def plane_sum(x):
    n = lax.axis_size(DP)
    return jnp.sum(lax.all_to_all(jnp.broadcast_to(x[None], (n, *x.shape)), DP, 0, 0), axis=0)


def on_device(pool, index, order, taps, out_weight, gain, quant_weight, quant_bias, post_weight):
    bf16, f32 = jnp.bfloat16, jnp.float32
    taps = taps.reshape(3 * C, C)
    out_weight = out_weight.reshape(C, C)
    dma = pltpu.SemaphoreType.DMA
    index = index.T
    chunk = (CLIPS, ROWS, C)
    kinds = [((2, 3 * C, C), bf16), ((2, C, C), bf16), ((2, 8, C), f32)]

    pool, taps, out_weight = (
        pltpu.with_memory_space_constraint(x, pltpu.HBM) for x in (pool, taps, out_weight)
    )
    (piece,) = call(
        prep_body, [HB, HB, VM], [((PIECE, 128), bf16)], [dma((5,))], name="prep"
    )(taps, out_weight, gain)
    mine = lax.ppermute(piece, "section", PAIR)
    v_a, *weights, qw, qb, post = call(
        functools.partial(start_body, (0, 1)),
        [HB, SM, HB, HB, VM, VM, VM, VM],
        [((2, *chunk), bf16), *kinds, ((C, 128), bf16), ((8, 128), f32), ((32, C), bf16)],
        [dma((10,))],
        name="start",
        blocks=2,
    )(pool, index, taps, out_weight, gain, quant_weight.T, quant_bias.reshape(1, BITS), post_weight)
    mine, v_a, index = lax.optimization_barrier((mine, v_a, index))
    up = shifted(mine, "dp_0", 1)
    down = shifted(mine, "dp_0", -1)
    side = split_shift(mine, "dp_1")
    mine_s = shifted(mine, "dp_2", 1)
    (v_b,) = call(
        functools.partial(load_body, (2, 3, 4)),
        [HB, SM, VM, VM, VM],
        [((3, *chunk), bf16)],
        [dma((12,))],
        name="load",
        blocks=3,
    )(pool, index, *weights)
    up, down, side, mine_s, v_b = lax.optimization_barrier((up, down, side, mine_s, v_b))
    swapped = [mine_s] + [shifted(x, "dp_2", 1) for x in (up, down, side)]
    weights = call(
        join_body,
        [VM] + [ANY] * 7 + [VM] * 3,
        kinds,
        [dma((24,))],
        name="join",
        aliases={8: 0, 9: 1, 10: 2},
    )(mine, up, down, side, *swapped, *weights)

    def encode(steps, v, before, last):
        n = len(steps)
        return call(
            functools.partial(encode_body, steps, last),
            [VM] * 7,
            [((n, 32, CLIPS * ROWS), bf16), ((8 if last else 32, 128), f32)],
            [pltpu.VMEM(chunk, bf16), pltpu.VMEM((32, 128), f32)],
            name="encode_%d" % steps[0],
            blocks=2 * n,
        )(v, *weights, qw, qb, before)

    def ship(codes):
        return lax.ppermute(codes, "section", [(0, 3), (1, 2)])

    codes, stats = encode((0, 1), v_a, jnp.zeros((32, 128), f32), False)
    codes_a = ship(codes)
    codes, stats = encode((2, 3, 4), v_b, stats, True)
    codes_b = ship(codes)
    codes_a, stats = lax.optimization_barrier((codes_a, stats))
    (e01,) = call(
        functools.partial(decode_body, (0, 1)),
        [VM] * 6,
        [((2, 8, 128), f32)],
        [pltpu.VMEM(chunk, bf16)],
        name="decode_0",
        blocks=4,
    )(v_a, *weights, post, codes_a)
    packed, own = call(
        functools.partial(decode_last_body, (2, 3, 4)),
        [VM] * 7,
        [((24, 128), f32), ((3, CLIPS, ROWS), f32)],
        [pltpu.VMEM(chunk, bf16)],
        name="decode_2",
        blocks=6,
    )(v_b, *weights, post, codes_b, e01)
    stats, packed, own = lax.optimization_barrier((stats, packed, own))
    total = lax.cond(lax.axis_index("section") <= 1, plane_sum, lambda x: 0.0 * x, stats)
    packed = jnp.concatenate([total, packed], axis=0)
    rest = [lax.ppermute(packed, "section", pairs) for pairs in (CROSS, FAR, PAIR)]
    rows_total = float(index.shape[0] * lax.axis_size(DP) * ROWS)
    error, loss = call(
        functools.partial(final_body, rows_total),
        [SM] + [VM] * 5,
        [((2, CLIPS, ROWS), f32), ((1, 128), f32)],
        name="final",
    )(order, packed, rest[2], rest[0], rest[1], own)
    return error, loss[0, : order.shape[0]]


def solution(mesh):
    torus = Mesh(
        mesh.devices.reshape(mesh.shape["section"], 4, 4, 2), ("section", "dp_0", "dp_1", "dp_2")
    )
    return jax.shard_map(
        on_device,
        mesh=torus,
        in_specs=(
            P(DP, None, None),
            P(None, DP),
            P(),
            P("section", None, None, None),
            P("section", None, None),
            P("section", None),
            P(),
            P(),
            P(),
        ),
        out_specs=(P("section", DP, None), P()),
        check_vma=False,
    )
```

```python
import functools

import jax
import jax.numpy as jnp
from jax import lax
from jax.experimental import pallas as pl
from jax.experimental.pallas import tpu as pltpu
from jax.sharding import Mesh
from jax.sharding import PartitionSpec as P


DP = ("dp_0", "dp_1", "dp_2")
EPS = 1e-06
C = 512
BITS = 18
FRAME = 64
ROWS = 256
CLIPS = 4
FRAMES = ROWS // FRAME
CHUNKS = ((4, 0, 1, 6, 7), (None, 2, 3, 5, None), (4, 2, 3, 5, None), (None, 0, 1, 6, 7))
STEPS = len(CHUNKS[0])
CODE_ROWS = 24
HALF = 1024
PIECE = HALF + 16
VM = pl.BlockSpec(memory_space=pltpu.VMEM)
SM = pl.BlockSpec(memory_space=pltpu.SMEM)
HB = pl.BlockSpec(memory_space=pltpu.HBM)
ANY = pl.BlockSpec(memory_space=pl.ANY)


def call(body, ins, outs, scratch=(), limit=24, aliases={}, blocks=0):
    return pl.pallas_call(
        body,
        in_specs=list(ins),
        out_specs=[VM] * len(outs),
        out_shape=[jax.ShapeDtypeStruct(shape, kind) for shape, kind in outs],
        scratch_shapes=list(scratch),
        compiler_params=pltpu.CompilerParams(vmem_limit_bytes=limit * 2**20),
        input_output_aliases=aliases,
        cost_estimate=pl.CostEstimate(
            flops=blocks * CLIPS * ROWS * C * C * 8, transcendentals=0, bytes_accessed=0
        ),
    )


def run_block(src, dst, taps, out_weight, half_gain):
    frames = [
        src[:, f * FRAME : (f + 1) * FRAME, :].reshape(CLIPS * FRAME, C) for f in range(FRAMES)
    ]
    normed = []
    for v in frames:
        w = v.astype(jnp.float32)
        mean = jnp.mean(w * w, axis=-1, keepdims=True)
        normed.append((w * lax.rsqrt(mean + EPS) * half_gain).astype(jnp.bfloat16))
    first = jnp.dot(normed[0], taps(C), preferred_element_type=jnp.float32)
    second = jnp.dot(
        jnp.concatenate([normed[1], normed[0]], axis=1),
        taps(2 * C),
        preferred_element_type=jnp.float32,
    )
    rest = jnp.concatenate(
        [
            jnp.concatenate([normed[f], normed[f - 1], normed[f - 2]], axis=1)
            for f in range(2, FRAMES)
        ],
        axis=0,
    )
    third = jnp.dot(rest, taps(3 * C), preferred_element_type=jnp.float32)
    h = jnp.concatenate([first, second, third], axis=0)
    activated = (h + h * jnp.tanh(h)).astype(jnp.bfloat16)
    update = jnp.dot(activated, out_weight(), preferred_element_type=jnp.float32)
    for f in range(FRAMES):
        part = update[f * CLIPS * FRAME : (f + 1) * CLIPS * FRAME]
        dst[:, f * FRAME : (f + 1) * FRAME, :] = (
            (frames[f].astype(jnp.float32) + part)
            .astype(jnp.bfloat16)
            .reshape(CLIPS, FRAME, C)
        )


def prep_body(taps, out_weight, gain_hbm, piece, gain, sems):
    colour = lax.rem(lax.axis_index("dp_0") + 2 * lax.axis_index("dp_1"), 4)
    at = pl.ds(pl.multiple_of(colour * 128, 128), 128)
    core = lax.axis_index("dp_2")
    gain_copy = pltpu.make_async_copy(gain_hbm, gain, sems.at[5])
    gain_copy.start()

    @pl.when(core == 0)
    def _():
        copy = pltpu.make_async_copy(
            taps.at[pl.ds(0, HALF), at], piece.at[pl.ds(0, HALF)], sems.at[0]
        )
        copy.start()
        copy.wait()

    @pl.when(core == 1)
    def _():
        copies = [
            pltpu.make_async_copy(
                taps.at[pl.ds(HALF, 512), at], piece.at[pl.ds(0, 512)], sems.at[0]
            )
        ]
        for j in range(4):
            copies.append(
                pltpu.make_async_copy(
                    out_weight.at[at, pl.ds(128 * j, 128)],
                    piece.at[pl.ds(512 + 128 * j, 128)],
                    sems.at[1 + j],
                )
            )
        for copy in copies:
            copy.start()
        for copy in copies:
            copy.wait()

    gain_copy.wait()
    wide = gain[...].astype(jnp.float32)
    rows = [wide[:, 128 * j : 128 * (j + 1)] for j in range(4)]
    rows.append(jnp.zeros((12, 128), jnp.float32))
    piece[HALF:, :] = jnp.concatenate(rows, axis=0).astype(jnp.bfloat16)


def batch_of(t):
    section = lax.axis_index("section")
    batch = jnp.int32(0)
    for k in range(4):
        if CHUNKS[k][t] is not None:
            batch = jnp.where(section == k, CHUNKS[k][t], batch)
    return batch


def has_chunk(t, sections):
    section = lax.axis_index("section")
    found = [section == k for k in sections if CHUNKS[k][t] is not None]
    return functools.reduce(jnp.logical_or, found)


def start_body(
    steps, pool, index_hbm, taps, out_weight, gain_hbm, qwt_hbm, qbias_hbm, postw_hbm,
    v, all_taps, all_out, all_gain, qw, qb, post,
    index, gain, qwt, qbias, postw, sems,
):
    own = lax.rem(lax.axis_index("section"), 2)
    pairs = [
        (index_hbm, index),
        (taps, all_taps.at[own]),
        (out_weight, all_out.at[own]),
        (gain_hbm, gain),
        (qwt_hbm, qwt),
        (qbias_hbm, qbias),
        (postw_hbm, postw),
    ]
    small = [pltpu.make_async_copy(a, b, sems.at[k]) for k, (a, b) in enumerate(pairs)]
    for copy in small:
        copy.start()
    small[0].wait()
    copies = []
    for t in range(STEPS):
        batch = batch_of(t)
        for c in range(CLIPS):
            copy = pltpu.make_async_copy(
                pool.at[index[c, batch]], v.at[t, c], sems.at[len(pairs) + t * CLIPS + c]
            )
            copy.start()
            copies.append(copy)
    for copy in small[1:]:
        copy.wait()
    all_gain[own] = jnp.broadcast_to(0.5 * gain[...].astype(jnp.float32), (8, C))
    wide = jnp.concatenate(
        [qwt[...].astype(jnp.float32), jnp.zeros((128 - BITS, C), jnp.float32)], axis=0
    )
    qw[...] = wide.T.astype(jnp.bfloat16)
    qb[...] = jnp.zeros((8, 128), jnp.float32)
    qb[0:1, 0:BITS] = qbias[...]
    post[...] = jnp.zeros((CODE_ROWS, C), jnp.bfloat16)
    post[0:BITS, :] = postw[...]
    for copy in copies[: steps * CLIPS]:
        copy.wait()
    first_block(0, steps, v, all_taps, all_out, all_gain)
    for copy in copies[steps * CLIPS :]:
        copy.wait()


def first_block(begin, end, v, all_taps, all_out, all_gain):
    @pl.when(lax.axis_index("section") == 0)
    def _():
        def step(t, _):
            block_at(0, v.at[t], all_taps, all_out, all_gain)
            return 0

        lax.fori_loop(begin, end, step, 0)


def more_body(begin, end, before, all_taps, all_out, all_gain, v):
    first_block(begin, end, v, all_taps, all_out, all_gain)


def join_body(*refs):
    pieces, (all_taps, all_out, all_gain), sems = refs[:8], refs[11:14], refs[14]
    section = lax.axis_index("section")
    core = lax.axis_index("dp_2")
    other = 1 - lax.rem(section, 2)

    def place(lower, upper):
        copies = []
        for j in range(4):
            lanes = pl.ds(128 * j, 128)
            copies.append(
                pltpu.make_async_copy(
                    lower[j].at[pl.ds(0, HALF)],
                    all_taps.at[other, pl.ds(0, HALF), lanes],
                    sems.at[j],
                )
            )
            copies.append(
                pltpu.make_async_copy(
                    upper[j].at[pl.ds(0, 512)],
                    all_taps.at[other, pl.ds(HALF, 512), lanes],
                    sems.at[4 + j],
                )
            )
            for k in range(4):
                copies.append(
                    pltpu.make_async_copy(
                        upper[j].at[pl.ds(512 + 128 * k, 128)],
                        all_out.at[other, pl.ds(128 * j, 128), pl.ds(128 * k, 128)],
                        sems.at[8 + 4 * j + k],
                    )
                )
        for copy in copies:
            copy.start()
        for copy in copies:
            copy.wait()

    @pl.when(core == 0)
    def _():
        place(pieces[:4], pieces[4:])

    @pl.when(core == 1)
    def _():
        place(pieces[4:], pieces[:4])

    rows = pieces[0][HALF:, :].astype(jnp.float32)
    row = jnp.concatenate([rows[k : k + 1, :] for k in range(4)], axis=1)
    all_gain[other] = jnp.broadcast_to(0.5 * row, (8, C))


def block_at(b, buf, all_taps, all_out, all_gain):
    run_block(
        buf,
        buf,
        lambda k: all_taps[b, :k, :],
        lambda: all_out[b],
        all_gain[b, 0:1, :],
    )


def encode_body(steps, last, v, all_taps, all_out, all_gain, qw, qb, *rest):
    section = lax.axis_index("section")
    codes, stats, buf, sums = rest[-4:]
    sums[...] = rest[0][...] if len(rest) > 4 else jnp.zeros_like(sums)
    row = lax.broadcasted_iota(jnp.int32, (CODE_ROWS, CLIPS * ROWS), 0)
    top = lax.broadcasted_iota(jnp.int32, (CODE_ROWS, 128), 0)
    lane = lax.broadcasted_iota(jnp.int32, (CODE_ROWS, 128), 1)

    def chunk(i, t):
        buf[...] = v[t]

        def step(b, _):
            block_at(b, buf, all_taps, all_out, all_gain)
            return 0

        lax.fori_loop(1 - section, 2, step, 0)
        logits = jnp.dot(
            buf[...].reshape(CLIPS * ROWS, C), qw[...], preferred_element_type=jnp.float32
        )
        z = (4.0 * (logits + qb[0:1, :])).T[:CODE_ROWS]
        size = jnp.abs(z)
        e = jnp.exp(-size)
        r = 1.0 / (1.0 + e)
        p = jnp.where(z >= 0, r, e * r)
        entropy = jnp.log1p(e) + size * (e * r)
        valid = row < BITS
        codes[i] = jnp.where(valid, 2.0 * p - 1.0, 0.0).astype(jnp.bfloat16)
        bit_sums = jnp.sum(jnp.where(valid, p, 0.0), axis=1, keepdims=True)
        total = jnp.sum(
            jnp.sum(jnp.where(valid, entropy, 0.0), axis=1, keepdims=True), axis=0, keepdims=True
        )
        column = jnp.where(top == BITS, total, bit_sums)
        sums[...] += jnp.where(lane == batch_of(t), column, 0.0)

    for i, t in enumerate(steps):
        pl.when(has_chunk(t, (0, 1)))(functools.partial(chunk, i, t))

    if last:
        full = jnp.concatenate([sums[...], jnp.zeros((128 - CODE_ROWS, 128), jnp.float32)], axis=0)
        stats[...] = full.T[:8]
    else:
        stats[...] = sums[...]


def decode_body(steps, v, all_taps, all_out, all_gain, post, codes, errors, buf):
    def chunk(i, t):
        quantized = lax.dot_general(
            codes[i], post[...], (((0,), (0,)), ((), ())), preferred_element_type=jnp.float32
        )
        buf[...] = quantized.astype(jnp.bfloat16).reshape(CLIPS, ROWS, C)

        def step(b, _):
            block_at(b, buf, all_taps, all_out, all_gain)
            return 0

        lax.fori_loop(0, 2, step, 0)
        for c in range(CLIPS):
            differ = buf[c].astype(jnp.float32) - v[t, c].astype(jnp.float32)
            square = differ * differ
            part = (
                square[:, :128] + square[:, 128:256] + square[:, 256:384] + square[:, 384:]
            )
            mean = jnp.sum(part.T, axis=0, keepdims=True) * (1.0 / C)
            errors[i, 2 * c : 2 * c + 1, :] = mean[:, :128]
            errors[i, 2 * c + 1 : 2 * c + 2, :] = mean[:, 128:]

    for i, t in enumerate(steps):
        pl.when(has_chunk(t, (2, 3)))(functools.partial(chunk, i, t))


def unpack(target, source):
    for c in range(CLIPS):
        row = source[2 * c : 2 * c + 2, :]
        target[c : c + 1, :] = jnp.concatenate([row[0:1], row[1:2]], axis=1)


def final_body(rows_total, order, mine, next_, cross, far, e0, e34, error, loss):
    section = lax.axis_index("section")
    a, b, c, d = mine[0:8], next_[0:8], cross[0:8], far[0:8]
    sums = (jnp.where(section <= 1, a + b, c + d)) * (1.0 / rows_total)
    row = lax.broadcasted_iota(jnp.int32, sums.shape, 0)
    lane = lax.broadcasted_iota(jnp.int32, sums.shape, 1)
    averaged = jnp.zeros_like(sums)
    running = None
    for t in range(8):
        here = row == order[t]
        marginal = jnp.sum(jnp.where(here, sums, 0.0), axis=0, keepdims=True)
        running = marginal if t == 0 else 0.5 * running + 0.5 * marginal
        averaged = jnp.where(here, running, averaged)
    smoothed = jnp.where(lane < BITS, 0.05 + 0.9 * averaged, 0.5)
    term = smoothed * jnp.log(smoothed) + (1.0 - smoothed) * jnp.log(1.0 - smoothed)
    term = jnp.where(lane < BITS, term, jnp.where(lane == BITS, sums, 0.0))
    result = jnp.sum(term, axis=1, keepdims=True)
    loss[...] = jnp.sum(jnp.where(row == lane, result, 0.0), axis=0, keepdims=True)

    @pl.when(section <= 1)
    def _():
        unpack(error.at[0], cross.at[pl.ds(8, 8)])
        unpack(error.at[1], cross.at[pl.ds(16, 8)])

    @pl.when(section == 2)
    def _():
        unpack(error.at[0], e0.at[0])
        unpack(error.at[1], e34.at[0])

    @pl.when(section == 3)
    def _():
        unpack(error.at[0], e34.at[0])
        unpack(error.at[1], e34.at[1])


PAIR = ((0, 1), (1, 0), (2, 3), (3, 2))
CROSS = ((0, 3), (3, 0), (1, 2), (2, 1))
FAR = ((0, 2), (2, 0), (1, 3), (3, 1))


def shifted(x, axis, by):
    n = lax.axis_size(axis)
    return lax.ppermute(x, axis, [(i, (i + by) % n) for i in range(n)])


def split_shift(x, axis):
    n = lax.axis_size(axis)
    pairs = []
    for i in range(n):
        pairs.append((2 * i, 2 * ((i + 1) % n)))
        pairs.append((2 * i + 1, 2 * ((i - 1) % n) + 1))
    return lax.ppermute(x, (axis, "dp_2"), pairs)


def plane_sum(x):
    n = lax.axis_size(DP)
    return jnp.sum(lax.all_to_all(jnp.broadcast_to(x[None], (n, *x.shape)), DP, 0, 0), axis=0)


def on_device(pool, index, order, taps, out_weight, gain, quant_weight, quant_bias, post_weight):
    bf16, f32 = jnp.bfloat16, jnp.float32
    taps = taps.reshape(3 * C, C)
    out_weight = out_weight.reshape(C, C)
    dma = pltpu.SemaphoreType.DMA
    index = index.T
    encoder = (lax.axis_index("section") <= 1).astype(jnp.int32)
    gain, encoder = lax.optimization_barrier((gain, encoder))
    chunk = (CLIPS, ROWS, C)
    kinds = [((2, 3 * C, C), bf16), ((2, C, C), bf16), ((2, 8, C), f32)]

    pool, taps, out_weight = (
        pltpu.with_memory_space_constraint(x, pltpu.HBM) for x in (pool, taps, out_weight)
    )
    gain, qwt, post_weight, index = (
        pltpu.with_memory_space_constraint(x, pltpu.HBM)
        for x in (gain, quant_weight.T, post_weight, index)
    )
    qbias = pltpu.with_memory_space_constraint(quant_bias.reshape(1, BITS), pltpu.HBM)
    (piece,) = call(
        prep_body, [HB] * 3, [((PIECE, 128), bf16)], [pltpu.VMEM((1, C), bf16), dma((6,))]
    )(taps, out_weight, gain)
    mine = lax.ppermute(piece, "section", PAIR)
    v_kind = ((STEPS, *chunk), bf16)
    v, *weights, qw, qb, post = call(
        functools.partial(start_body, 2),
        [HB] * 8,
        [v_kind, *kinds, ((C, 128), bf16), ((8, 128), f32), ((CODE_ROWS, C), bf16)],
        [
            pltpu.SMEM(index.shape, jnp.int32),
            pltpu.VMEM((1, C), bf16),
            pltpu.VMEM((BITS, C), bf16),
            pltpu.VMEM((1, BITS), f32),
            pltpu.VMEM((BITS, C), bf16),
            dma((7 + STEPS * CLIPS,)),
        ],
        blocks=2,
    )(pool, index, taps, out_weight, gain, qwt, qbias, post_weight)
    mine, v = lax.optimization_barrier((mine, v))
    up = shifted(mine, "dp_0", 1)
    down = shifted(mine, "dp_0", -1)
    side = split_shift(mine, "dp_1")
    mine_s = shifted(mine, "dp_2", 1)
    (v,) = call(
        functools.partial(more_body, 2, STEPS), [VM] * 4, [v_kind], blocks=3, aliases={0: 0}
    )(v, *weights)
    up, down, side, mine_s, v = lax.optimization_barrier((up, down, side, mine_s, v))
    swapped = [mine_s] + [shifted(x, "dp_2", 1) for x in (up, down, side)]
    weights = call(
        join_body, [VM] + [ANY] * 7 + [VM] * 3, kinds, [dma((24,))], aliases={8: 0, 9: 1, 10: 2}
    )(mine, up, down, side, *swapped, *weights)

    def encode(steps, before, last):
        n = len(steps)
        return call(
            functools.partial(encode_body, steps, last),
            [VM] * (6 + len(before)),
            [((n, CODE_ROWS, CLIPS * ROWS), bf16), ((8 if last else CODE_ROWS, 128), f32)],
            [pltpu.VMEM(chunk, bf16), pltpu.VMEM((CODE_ROWS, 128), f32)],
            blocks=2 * n,
        )(v, *weights, qw, qb, *before)

    def decode(steps, codes):
        n = len(steps)
        return call(
            functools.partial(decode_body, steps),
            [VM] * 6,
            [((n, 8, 128), f32)],
            [pltpu.VMEM(chunk, bf16)],
            blocks=2 * n,
        )(v, *weights, post, codes)[0]

    to_cross = ((0, 3), (1, 2))
    codes, stats = encode((0,), (), False)
    codes_a = lax.ppermute(codes, "section", ((0, 2),))
    codes, stats = encode((1, 2), (stats,), False)
    codes_b = lax.ppermute(codes, "section", to_cross)
    codes, stats = encode((3, 4), (stats,), True)
    codes_c = lax.ppermute(codes, "section", to_cross)
    codes_a, stats = lax.optimization_barrier((codes_a, stats))
    e0 = decode((0,), codes_a)
    codes_b, e0 = lax.optimization_barrier((codes_b, e0))
    e12 = decode((1, 2), codes_b)
    codes_c, e12 = lax.optimization_barrier((codes_c, e12))
    e34 = decode((3, 4), codes_c)
    stats, e12, e34, encoder = lax.optimization_barrier((stats, e12, e34, encoder))
    total = lax.cond(encoder == 1, plane_sum, lambda x: 0.0 * x, stats)
    packed = jnp.concatenate([total, e12[0], e12[1]], axis=0)
    near, cross, far = (lax.ppermute(packed, "section", pairs) for pairs in (PAIR, CROSS, FAR))
    rows_total = float(CLIPS * lax.axis_size(DP) * ROWS)
    error, loss = call(
        functools.partial(final_body, rows_total),
        [SM] + [VM] * 6,
        [((2, CLIPS, ROWS), f32), ((1, 128), f32)],
    )(order, packed, near, cross, far, e0, e34)
    return error, loss[0, : order.shape[0]]


def solution(mesh):
    torus = Mesh(
        mesh.devices.reshape(mesh.shape["section"], 4, 4, 2), ("section", "dp_0", "dp_1", "dp_2")
    )
    return jax.shard_map(
        on_device,
        mesh=torus,
        in_specs=(
            P(DP, None, None),
            P(None, DP),
            P(),
            P("section", None, None, None),
            P("section", None, None),
            P("section", None),
            P(),
            P(),
            P(),
        ),
        out_specs=(P("section", DP, None), P()),
        check_vma=False,
    )
```

```python
import functools

import jax
import jax.numpy as jnp
from jax import lax
from jax.experimental import pallas as pl
from jax.experimental.pallas import tpu as pltpu
from jax.sharding import Mesh
from jax.sharding import PartitionSpec as P


DP = ("dp_0", "dp_1", "dp_2")
EPS = 1e-06
C = 512
BITS = 18
FRAME = 64
ROWS = 256
CLIPS = 4
FRAMES = ROWS // FRAME
CHUNKS = ((4, 0, 1, 6, 7), (None, 2, 3, 5, None), (4, 2, 3, 5, None), (None, 0, 1, 6, 7))
STEPS = len(CHUNKS[0])
CODE_ROWS = 24
HALF = 1024
PIECE = HALF + 16
VM = pl.BlockSpec(memory_space=pltpu.VMEM)
SM = pl.BlockSpec(memory_space=pltpu.SMEM)
HB = pl.BlockSpec(memory_space=pltpu.HBM)
ANY = pl.BlockSpec(memory_space=pl.ANY)


def call(body, ins, outs, scratch=(), limit=24, aliases={}, blocks=0):
    return pl.pallas_call(
        body,
        in_specs=list(ins),
        out_specs=[VM] * len(outs),
        out_shape=[jax.ShapeDtypeStruct(shape, kind) for shape, kind in outs],
        scratch_shapes=list(scratch),
        compiler_params=pltpu.CompilerParams(vmem_limit_bytes=limit * 2**20),
        input_output_aliases=aliases,
        cost_estimate=pl.CostEstimate(
            flops=blocks * CLIPS * ROWS * C * C * 8, transcendentals=0, bytes_accessed=0
        ),
    )


def run_block(src, dst, taps, out_weight, half_gain):
    frames = [
        src[:, f * FRAME : (f + 1) * FRAME, :].reshape(CLIPS * FRAME, C) for f in range(FRAMES)
    ]
    normed = []
    for v in frames:
        w = v.astype(jnp.float32)
        mean = jnp.mean(w * w, axis=-1, keepdims=True)
        normed.append((w * lax.rsqrt(mean + EPS) * half_gain).astype(jnp.bfloat16))
    first = jnp.dot(normed[0], taps(C), preferred_element_type=jnp.float32)
    second = jnp.dot(
        jnp.concatenate([normed[1], normed[0]], axis=1),
        taps(2 * C),
        preferred_element_type=jnp.float32,
    )
    rest = jnp.concatenate(
        [
            jnp.concatenate([normed[f], normed[f - 1], normed[f - 2]], axis=1)
            for f in range(2, FRAMES)
        ],
        axis=0,
    )
    third = jnp.dot(rest, taps(3 * C), preferred_element_type=jnp.float32)
    h = jnp.concatenate([first, second, third], axis=0)
    activated = (h + h * jnp.tanh(h)).astype(jnp.bfloat16)
    update = jnp.dot(activated, out_weight(), preferred_element_type=jnp.float32)
    for f in range(FRAMES):
        part = update[f * CLIPS * FRAME : (f + 1) * CLIPS * FRAME]
        dst[:, f * FRAME : (f + 1) * FRAME, :] = (
            (frames[f].astype(jnp.float32) + part)
            .astype(jnp.bfloat16)
            .reshape(CLIPS, FRAME, C)
        )


def prep_body(taps, out_weight, gain_hbm, piece, second, gain, sems):
    core = lax.axis_index("dp_2")
    gain_copy = pltpu.make_async_copy(gain_hbm, gain, sems.at[10])
    gain_copy.start()

    def copies(target, on, at):
        colour = lax.rem(lax.axis_index("dp_0") + 2 * lax.axis_index("dp_1") + on, 4)
        lanes = pl.ds(pl.multiple_of(colour * 128, 128), 128)
        lower = [
            pltpu.make_async_copy(
                taps.at[pl.ds(0, HALF), lanes], target.at[pl.ds(0, HALF)], sems.at[at]
            )
        ]
        upper = [
            pltpu.make_async_copy(
                taps.at[pl.ds(HALF, 512), lanes], target.at[pl.ds(0, 512)], sems.at[at]
            )
        ]
        for j in range(4):
            upper.append(
                pltpu.make_async_copy(
                    out_weight.at[lanes, pl.ds(128 * j, 128)],
                    target.at[pl.ds(512 + 128 * j, 128)],
                    sems.at[at + 1 + j],
                )
            )
        return lower, upper

    sets = [copies(piece, 0, 0), copies(second, 2, 5)]
    for side in range(2):

        @pl.when(core == side)
        def _(side=side):
            chosen = sets[0][side] + sets[1][side]
            for copy in chosen:
                copy.start()
            for copy in chosen:
                copy.wait()

    gain_copy.wait()
    wide = gain[...].astype(jnp.float32)
    rows = [wide[:, 128 * j : 128 * (j + 1)] for j in range(4)]
    rows.append(jnp.zeros((12, 128), jnp.float32))
    piece[HALF:, :] = jnp.concatenate(rows, axis=0).astype(jnp.bfloat16)


def batch_of(t):
    section = lax.axis_index("section")
    batch = jnp.int32(0)
    for k in range(4):
        if CHUNKS[k][t] is not None:
            batch = jnp.where(section == k, CHUNKS[k][t], batch)
    return batch


def has_chunk(t, sections):
    section = lax.axis_index("section")
    found = [section == k for k in sections if CHUNKS[k][t] is not None]
    return functools.reduce(jnp.logical_or, found)


def start_body(
    steps, pool, index_hbm, taps, out_weight, gain_hbm, qwt_hbm, qbias_hbm, postw_hbm,
    v, all_taps, all_out, all_gain, qw, qb, post,
    index, gain, qwt, qbias, postw, sems,
):
    own = lax.rem(lax.axis_index("section"), 2)
    pairs = [
        (index_hbm, index),
        (taps, all_taps.at[own]),
        (out_weight, all_out.at[own]),
        (gain_hbm, gain),
        (qwt_hbm, qwt),
        (qbias_hbm, qbias),
        (postw_hbm, postw),
    ]
    small = [pltpu.make_async_copy(a, b, sems.at[k]) for k, (a, b) in enumerate(pairs)]
    for copy in small:
        copy.start()
    small[0].wait()
    copies = []
    for t in range(STEPS):
        batch = batch_of(t)
        for c in range(CLIPS):
            copy = pltpu.make_async_copy(
                pool.at[index[c, batch]], v.at[t, c], sems.at[len(pairs) + t * CLIPS + c]
            )
            copy.start()
            copies.append(copy)
    for copy in small[1:]:
        copy.wait()
    all_gain[own] = jnp.broadcast_to(0.5 * gain[...].astype(jnp.float32), (8, C))
    wide = jnp.concatenate(
        [qwt[...].astype(jnp.float32), jnp.zeros((128 - BITS, C), jnp.float32)], axis=0
    )
    qw[...] = wide.T.astype(jnp.bfloat16)
    qb[...] = jnp.zeros((8, 128), jnp.float32)
    qb[0:1, 0:BITS] = qbias[...]
    post[...] = jnp.zeros((CODE_ROWS, C), jnp.bfloat16)
    post[0:BITS, :] = postw[...]
    for copy in copies[: steps * CLIPS]:
        copy.wait()
    first_block(0, steps, v, all_taps, all_out, all_gain)
    for copy in copies[steps * CLIPS :]:
        copy.wait()


def first_block(begin, end, v, all_taps, all_out, all_gain):
    @pl.when(lax.axis_index("section") == 0)
    def _():
        def step(t, _):
            block_at(0, v.at[t], all_taps, all_out, all_gain)
            return 0

        lax.fori_loop(begin, end, step, 0)


def more_body(begin, end, before, all_taps, all_out, all_gain, v):
    first_block(begin, end, v, all_taps, all_out, all_gain)


def join_body(*refs):
    pieces, (all_taps, all_out, all_gain), sems = refs[:8], refs[11:14], refs[14]
    section = lax.axis_index("section")
    core = lax.axis_index("dp_2")
    other = 1 - lax.rem(section, 2)

    def place(lower, upper):
        copies = []
        for j in range(4):
            lanes = pl.ds(128 * j, 128)
            copies.append(
                pltpu.make_async_copy(
                    lower[j].at[pl.ds(0, HALF)],
                    all_taps.at[other, pl.ds(0, HALF), lanes],
                    sems.at[j],
                )
            )
            copies.append(
                pltpu.make_async_copy(
                    upper[j].at[pl.ds(0, 512)],
                    all_taps.at[other, pl.ds(HALF, 512), lanes],
                    sems.at[4 + j],
                )
            )
            for k in range(4):
                copies.append(
                    pltpu.make_async_copy(
                        upper[j].at[pl.ds(512 + 128 * k, 128)],
                        all_out.at[other, pl.ds(128 * j, 128), pl.ds(128 * k, 128)],
                        sems.at[8 + 4 * j + k],
                    )
                )
        for copy in copies:
            copy.start()
        for copy in copies:
            copy.wait()

    @pl.when(core == 0)
    def _():
        place(pieces[:4], pieces[4:])

    @pl.when(core == 1)
    def _():
        place(pieces[4:], pieces[:4])

    rows = pieces[0][HALF:, :].astype(jnp.float32)
    row = jnp.concatenate([rows[k : k + 1, :] for k in range(4)], axis=1)
    all_gain[other] = jnp.broadcast_to(0.5 * row, (8, C))


def block_at(b, buf, all_taps, all_out, all_gain):
    run_block(
        buf,
        buf,
        lambda k: all_taps[b, :k, :],
        lambda: all_out[b],
        all_gain[b, 0:1, :],
    )


def encode_body(steps, last, v, all_taps, all_out, all_gain, qw, qb, *rest):
    section = lax.axis_index("section")
    codes, stats, buf, sums = rest[-4:]
    sums[...] = rest[0][...] if len(rest) > 4 else jnp.zeros_like(sums)
    row = lax.broadcasted_iota(jnp.int32, (CODE_ROWS, CLIPS * ROWS), 0)
    top = lax.broadcasted_iota(jnp.int32, (CODE_ROWS, 128), 0)
    lane = lax.broadcasted_iota(jnp.int32, (CODE_ROWS, 128), 1)

    def chunk(i, t):
        buf[...] = v[t]

        def step(b, _):
            block_at(b, buf, all_taps, all_out, all_gain)
            return 0

        lax.fori_loop(1 - section, 2, step, 0)
        logits = jnp.dot(
            buf[...].reshape(CLIPS * ROWS, C), qw[...], preferred_element_type=jnp.float32
        )
        z = (4.0 * (logits + qb[0:1, :])).T[:CODE_ROWS]
        size = jnp.abs(z)
        e = jnp.exp(-size)
        r = 1.0 / (1.0 + e)
        p = jnp.where(z >= 0, r, e * r)
        entropy = jnp.log1p(e) + size * (e * r)
        valid = row < BITS
        codes[i] = jnp.where(valid, 2.0 * p - 1.0, 0.0).astype(jnp.bfloat16)
        bit_sums = jnp.sum(jnp.where(valid, p, 0.0), axis=1, keepdims=True)
        total = jnp.sum(
            jnp.sum(jnp.where(valid, entropy, 0.0), axis=1, keepdims=True), axis=0, keepdims=True
        )
        column = jnp.where(top == BITS, total, bit_sums)
        sums[...] += jnp.where(lane == batch_of(t), column, 0.0)

    for i, t in enumerate(steps):
        pl.when(has_chunk(t, (0, 1)))(functools.partial(chunk, i, t))

    if last:
        full = jnp.concatenate([sums[...], jnp.zeros((128 - CODE_ROWS, 128), jnp.float32)], axis=0)
        stats[...] = full.T[:8]
    else:
        stats[...] = sums[...]


def decode_body(steps, v, all_taps, all_out, all_gain, post, codes, errors, buf):
    def chunk(i, t):
        quantized = lax.dot_general(
            codes[i], post[...], (((0,), (0,)), ((), ())), preferred_element_type=jnp.float32
        )
        buf[...] = quantized.astype(jnp.bfloat16).reshape(CLIPS, ROWS, C)

        def step(b, _):
            block_at(b, buf, all_taps, all_out, all_gain)
            return 0

        lax.fori_loop(0, 2, step, 0)
        for c in range(CLIPS):
            differ = buf[c].astype(jnp.float32) - v[t, c].astype(jnp.float32)
            square = differ * differ
            part = (
                square[:, :128] + square[:, 128:256] + square[:, 256:384] + square[:, 384:]
            )
            mean = jnp.sum(part.T, axis=0, keepdims=True) * (1.0 / C)
            errors[i, 2 * c : 2 * c + 1, :] = mean[:, :128]
            errors[i, 2 * c + 1 : 2 * c + 2, :] = mean[:, 128:]

    for i, t in enumerate(steps):
        pl.when(has_chunk(t, (2, 3)))(functools.partial(chunk, i, t))


def unpack(target, source):
    for c in range(CLIPS):
        row = source[2 * c : 2 * c + 2, :]
        target[c : c + 1, :] = jnp.concatenate([row[0:1], row[1:2]], axis=1)


def final_body(rows_total, order, mine, next_, cross, far, e0, e34, error, loss):
    section = lax.axis_index("section")
    a, b, c, d = mine[0:8], next_[0:8], cross[0:8], far[0:8]
    sums = (jnp.where(section <= 1, a + b, c + d)) * (1.0 / rows_total)
    row = lax.broadcasted_iota(jnp.int32, sums.shape, 0)
    lane = lax.broadcasted_iota(jnp.int32, sums.shape, 1)
    averaged = jnp.zeros_like(sums)
    running = None
    for t in range(8):
        here = row == order[t]
        marginal = jnp.sum(jnp.where(here, sums, 0.0), axis=0, keepdims=True)
        running = marginal if t == 0 else 0.5 * running + 0.5 * marginal
        averaged = jnp.where(here, running, averaged)
    smoothed = jnp.where(lane < BITS, 0.05 + 0.9 * averaged, 0.5)
    term = smoothed * jnp.log(smoothed) + (1.0 - smoothed) * jnp.log(1.0 - smoothed)
    term = jnp.where(lane < BITS, term, jnp.where(lane == BITS, sums, 0.0))
    result = jnp.sum(term, axis=1, keepdims=True)
    flat = jnp.sum(jnp.where(row == lane, result, 0.0), axis=0)
    loss[...] = flat[:8]

    @pl.when(section <= 1)
    def _():
        unpack(error.at[0], cross.at[pl.ds(8, 8)])
        unpack(error.at[1], cross.at[pl.ds(16, 8)])

    @pl.when(section == 2)
    def _():
        unpack(error.at[0], e0.at[0])
        unpack(error.at[1], e34.at[0])

    @pl.when(section == 3)
    def _():
        unpack(error.at[0], e34.at[0])
        unpack(error.at[1], e34.at[1])


PAIR = ((0, 1), (1, 0), (2, 3), (3, 2))
CROSS = ((0, 3), (3, 0), (1, 2), (2, 1))
FAR = ((0, 2), (2, 0), (1, 3), (3, 1))


def shifted(x, axis, by):
    n = lax.axis_size(axis)
    return lax.ppermute(x, axis, [(i, (i + by) % n) for i in range(n)])


def plane_sum(x):
    n = lax.axis_size(DP)
    return jnp.sum(lax.all_to_all(jnp.broadcast_to(x[None], (n, *x.shape)), DP, 0, 0), axis=0)


def on_device(pool, index, order, taps, out_weight, gain, quant_weight, quant_bias, post_weight):
    bf16, f32 = jnp.bfloat16, jnp.float32
    taps = taps.reshape(3 * C, C)
    out_weight = out_weight.reshape(C, C)
    dma = pltpu.SemaphoreType.DMA
    index = index.T
    encoder = (lax.axis_index("section") <= 1).astype(jnp.int32)
    gain, encoder = lax.optimization_barrier((gain, encoder))
    chunk = (CLIPS, ROWS, C)
    kinds = [((2, 3 * C, C), bf16), ((2, C, C), bf16), ((2, 8, C), f32)]

    pool, taps, out_weight = (
        pltpu.with_memory_space_constraint(x, pltpu.HBM) for x in (pool, taps, out_weight)
    )
    gain, qwt, post_weight, index = (
        pltpu.with_memory_space_constraint(x, pltpu.HBM)
        for x in (gain, quant_weight.T, post_weight, index)
    )
    qbias = pltpu.with_memory_space_constraint(quant_bias.reshape(1, BITS), pltpu.HBM)
    piece, second = call(
        prep_body,
        [HB] * 3,
        [((PIECE, 128), bf16), ((HALF, 128), bf16)],
        [pltpu.VMEM((1, C), bf16), dma((11,))],
    )(taps, out_weight, gain)
    mine = lax.ppermute(piece, "section", PAIR)
    second = lax.ppermute(second, "section", PAIR)
    v_kind = ((STEPS, *chunk), bf16)
    v, *weights, qw, qb, post = call(
        functools.partial(start_body, 2),
        [HB] * 8,
        [v_kind, *kinds, ((C, 128), bf16), ((8, 128), f32), ((CODE_ROWS, C), bf16)],
        [
            pltpu.SMEM(index.shape, jnp.int32),
            pltpu.VMEM((1, C), bf16),
            pltpu.VMEM((BITS, C), bf16),
            pltpu.VMEM((1, BITS), f32),
            pltpu.VMEM((BITS, C), bf16),
            dma((7 + STEPS * CLIPS,)),
        ],
        blocks=2,
    )(pool, index, taps, out_weight, gain, qwt, qbias, post_weight)
    mine, v = lax.optimization_barrier((mine, v))
    up = shifted(mine, "dp_0", 1)
    down = shifted(mine, "dp_0", -1)
    mine_s = shifted(mine, "dp_2", 1)
    (v,) = call(
        functools.partial(more_body, 2, STEPS), [VM] * 4, [v_kind], blocks=3, aliases={0: 0}
    )(v, *weights)
    up, down, second, mine_s, v = lax.optimization_barrier((up, down, second, mine_s, v))
    swapped = [mine_s] + [shifted(x, "dp_2", 1) for x in (second, up, down)]
    weights = call(
        join_body, [VM] + [ANY] * 7 + [VM] * 3, kinds, [dma((24,))], aliases={8: 0, 9: 1, 10: 2}
    )(mine, second, up, down, *swapped, *weights)

    def encode(steps, before, last):
        n = len(steps)
        return call(
            functools.partial(encode_body, steps, last),
            [VM] * (6 + len(before)),
            [((n, CODE_ROWS, CLIPS * ROWS), bf16), ((8 if last else CODE_ROWS, 128), f32)],
            [pltpu.VMEM(chunk, bf16), pltpu.VMEM((CODE_ROWS, 128), f32)],
            blocks=2 * n,
        )(v, *weights, qw, qb, *before)

    def decode(steps, codes):
        n = len(steps)
        return call(
            functools.partial(decode_body, steps),
            [VM] * 6,
            [((n, 8, 128), f32)],
            [pltpu.VMEM(chunk, bf16)],
            blocks=2 * n,
        )(v, *weights, post, codes)[0]

    to_cross = ((0, 3), (1, 2))
    codes, stats = encode((0,), (), False)
    codes_a = lax.ppermute(codes, "section", ((0, 2),))
    codes, stats = encode((1, 2), (stats,), False)
    codes_b = lax.ppermute(codes, "section", to_cross)
    codes, stats = encode((3, 4), (stats,), True)
    codes_c = lax.ppermute(codes, "section", to_cross)
    codes_a, stats = lax.optimization_barrier((codes_a, stats))
    e0 = decode((0,), codes_a)
    codes_b, e0 = lax.optimization_barrier((codes_b, e0))
    e12 = decode((1, 2), codes_b)
    codes_c, e12 = lax.optimization_barrier((codes_c, e12))
    e34 = decode((3, 4), codes_c)
    stats, e12, e34, encoder = lax.optimization_barrier((stats, e12, e34, encoder))
    total = lax.cond(encoder == 1, plane_sum, lambda x: 0.0 * x, stats)
    packed = jnp.concatenate([total, e12[0], e12[1]], axis=0)
    near, cross, far = (lax.ppermute(packed, "section", pairs) for pairs in (PAIR, CROSS, FAR))
    rows_total = float(CLIPS * lax.axis_size(DP) * ROWS)
    error, loss = call(
        functools.partial(final_body, rows_total),
        [SM] + [VM] * 6,
        [((2, CLIPS, ROWS), f32), ((8,), f32)],
    )(order, packed, near, cross, far, e0, e34)
    return error, loss


def solution(mesh):
    torus = Mesh(
        mesh.devices.reshape(mesh.shape["section"], 4, 4, 2), ("section", "dp_0", "dp_1", "dp_2")
    )
    return jax.shard_map(
        on_device,
        mesh=torus,
        in_specs=(
            P(DP, None, None),
            P(None, DP),
            P(),
            P("section", None, None, None),
            P("section", None, None),
            P("section", None),
            P(),
            P(),
            P(),
        ),
        out_specs=(P("section", DP, None), P()),
        check_vma=False,
    )
```

```python
import functools

import jax
import jax.numpy as jnp
from jax import lax
from jax.experimental import pallas as pl
from jax.experimental.pallas import tpu as pltpu
from jax.sharding import Mesh
from jax.sharding import PartitionSpec as P


DP = ("dp_0", "dp_1", "dp_2")
EPS = 1e-06
C = 512
BITS = 18
FRAME = 64
ROWS = 256
CLIPS = 4
FRAMES = ROWS // FRAME
CHUNKS = ((4, 0, 1, 6, 7), (None, 2, 3, 5, None), (4, 2, 3, 5, None), (None, 0, 1, 6, 7))
STEPS = len(CHUNKS[0])
CODE_ROWS = 24
HALF = 1024
PIECE = HALF + 16
VM = pl.BlockSpec(memory_space=pltpu.VMEM)
SM = pl.BlockSpec(memory_space=pltpu.SMEM)
HB = pl.BlockSpec(memory_space=pltpu.HBM)
ANY = pl.BlockSpec(memory_space=pl.ANY)


def call(body, ins, outs, scratch=(), limit=24, aliases={}, blocks=0):
    return pl.pallas_call(
        body,
        in_specs=list(ins),
        out_specs=[VM] * len(outs),
        out_shape=[jax.ShapeDtypeStruct(shape, kind) for shape, kind in outs],
        scratch_shapes=list(scratch),
        compiler_params=pltpu.CompilerParams(vmem_limit_bytes=limit * 2**20),
        input_output_aliases=aliases,
        cost_estimate=pl.CostEstimate(
            flops=blocks * CLIPS * ROWS * C * C * 8, transcendentals=0, bytes_accessed=0
        ),
    )


def run_block(src, dst, taps, out_weight, half_gain):
    frames = [
        src[:, f * FRAME : (f + 1) * FRAME, :].reshape(CLIPS * FRAME, C) for f in range(FRAMES)
    ]
    normed = []
    for v in frames:
        w = v.astype(jnp.float32)
        mean = jnp.mean(w * w, axis=-1, keepdims=True)
        normed.append((w * lax.rsqrt(mean + EPS) * half_gain).astype(jnp.bfloat16))
    first = jnp.dot(normed[0], taps(C), preferred_element_type=jnp.float32)
    second = jnp.dot(
        jnp.concatenate([normed[1], normed[0]], axis=1),
        taps(2 * C),
        preferred_element_type=jnp.float32,
    )
    rest = jnp.concatenate(
        [
            jnp.concatenate([normed[f], normed[f - 1], normed[f - 2]], axis=1)
            for f in range(2, FRAMES)
        ],
        axis=0,
    )
    third = jnp.dot(rest, taps(3 * C), preferred_element_type=jnp.float32)
    h = jnp.concatenate([first, second, third], axis=0)
    activated = (h + h * jnp.tanh(h)).astype(jnp.bfloat16)
    update = jnp.dot(activated, out_weight(), preferred_element_type=jnp.float32)
    for f in range(FRAMES):
        part = update[f * CLIPS * FRAME : (f + 1) * CLIPS * FRAME]
        dst[:, f * FRAME : (f + 1) * FRAME, :] = (
            (frames[f].astype(jnp.float32) + part)
            .astype(jnp.bfloat16)
            .reshape(CLIPS, FRAME, C)
        )


def prep_body(taps, out_weight, gain_hbm, piece, second, gain, sems):
    core = lax.axis_index("dp_2")
    gain_copy = pltpu.make_async_copy(gain_hbm, gain, sems.at[10])
    gain_copy.start()

    def copies(target, on, at):
        colour = lax.rem(lax.axis_index("dp_0") + lax.axis_index("dp_1") + on, 4)
        lanes = pl.ds(pl.multiple_of(colour * 128, 128), 128)
        lower = [
            pltpu.make_async_copy(
                taps.at[pl.ds(0, HALF), lanes], target.at[pl.ds(0, HALF)], sems.at[at]
            )
        ]
        upper = [
            pltpu.make_async_copy(
                taps.at[pl.ds(HALF, 512), lanes], target.at[pl.ds(0, 512)], sems.at[at]
            )
        ]
        for j in range(4):
            upper.append(
                pltpu.make_async_copy(
                    out_weight.at[lanes, pl.ds(128 * j, 128)],
                    target.at[pl.ds(512 + 128 * j, 128)],
                    sems.at[at + 1 + j],
                )
            )
        return lower, upper

    sets = [copies(piece, 0, 0), copies(second, 2, 5)]
    for side in range(2):

        @pl.when(core == side)
        def _(side=side):
            chosen = sets[0][side] + sets[1][side]
            for copy in chosen:
                copy.start()
            for copy in chosen:
                copy.wait()

    gain_copy.wait()
    wide = gain[...].astype(jnp.float32)
    rows = [wide[:, 128 * j : 128 * (j + 1)] for j in range(4)]
    rows.append(jnp.zeros((12, 128), jnp.float32))
    piece[HALF:, :] = jnp.concatenate(rows, axis=0).astype(jnp.bfloat16)


def batch_of(t):
    section = lax.axis_index("section")
    batch = jnp.int32(0)
    for k in range(4):
        if CHUNKS[k][t] is not None:
            batch = jnp.where(section == k, CHUNKS[k][t], batch)
    return batch


def has_chunk(t, sections):
    section = lax.axis_index("section")
    found = [section == k for k in sections if CHUNKS[k][t] is not None]
    return functools.reduce(jnp.logical_or, found)


def start_body(
    steps, pool, index_hbm, taps, out_weight, gain_hbm, qwt_hbm, qbias_hbm, postw_hbm,
    v, all_taps, all_out, all_gain, qw, qb, post,
    index, gain, qwt, qbias, postw, sems,
):
    own = lax.rem(lax.axis_index("section"), 2)
    pairs = [
        (index_hbm, index),
        (taps, all_taps.at[own]),
        (out_weight, all_out.at[own]),
        (gain_hbm, gain),
        (qwt_hbm, qwt),
        (qbias_hbm, qbias),
        (postw_hbm, postw),
    ]
    small = [pltpu.make_async_copy(a, b, sems.at[k]) for k, (a, b) in enumerate(pairs)]
    for copy in small:
        copy.start()
    small[0].wait()
    copies = []
    for t in range(STEPS):
        batch = batch_of(t)
        for c in range(CLIPS):
            copy = pltpu.make_async_copy(
                pool.at[index[c, batch]], v.at[t, c], sems.at[len(pairs) + t * CLIPS + c]
            )
            copy.start()
            copies.append(copy)
    for copy in small[1:]:
        copy.wait()
    all_gain[own] = jnp.broadcast_to(0.5 * gain[...].astype(jnp.float32), (8, C))
    wide = jnp.concatenate(
        [qwt[...].astype(jnp.float32), jnp.zeros((128 - BITS, C), jnp.float32)], axis=0
    )
    qw[...] = wide.T.astype(jnp.bfloat16)
    qb[...] = jnp.zeros((8, 128), jnp.float32)
    qb[0:1, 0:BITS] = qbias[...]
    post[...] = jnp.zeros((CODE_ROWS, C), jnp.bfloat16)
    post[0:BITS, :] = postw[...]
    for copy in copies[: steps * CLIPS]:
        copy.wait()
    first_block(0, steps, v, all_taps, all_out, all_gain)
    for copy in copies[steps * CLIPS :]:
        copy.wait()


def first_block(begin, end, v, all_taps, all_out, all_gain):
    @pl.when(lax.axis_index("section") == 0)
    def _():
        def step(t, _):
            block_at(0, v.at[t], all_taps, all_out, all_gain)
            return 0

        lax.fori_loop(begin, end, step, 0)


def more_body(begin, end, before, all_taps, all_out, all_gain, v):
    first_block(begin, end, v, all_taps, all_out, all_gain)


def join_body(*refs):
    pieces, (all_taps, all_out, all_gain), sems = refs[:8], refs[11:14], refs[14]
    section = lax.axis_index("section")
    core = lax.axis_index("dp_2")
    other = 1 - lax.rem(section, 2)

    def place(lower, upper):
        copies = []
        for j in range(4):
            lanes = pl.ds(128 * j, 128)
            copies.append(
                pltpu.make_async_copy(
                    lower[j].at[pl.ds(0, HALF)],
                    all_taps.at[other, pl.ds(0, HALF), lanes],
                    sems.at[j],
                )
            )
            copies.append(
                pltpu.make_async_copy(
                    upper[j].at[pl.ds(0, 512)],
                    all_taps.at[other, pl.ds(HALF, 512), lanes],
                    sems.at[4 + j],
                )
            )
            for k in range(4):
                copies.append(
                    pltpu.make_async_copy(
                        upper[j].at[pl.ds(512 + 128 * k, 128)],
                        all_out.at[other, pl.ds(128 * j, 128), pl.ds(128 * k, 128)],
                        sems.at[8 + 4 * j + k],
                    )
                )
        for copy in copies:
            copy.start()
        for copy in copies:
            copy.wait()

    @pl.when(core == 0)
    def _():
        place(pieces[:4], pieces[4:])

    @pl.when(core == 1)
    def _():
        place(pieces[4:], pieces[:4])

    rows = pieces[0][HALF:, :].astype(jnp.float32)
    row = jnp.concatenate([rows[k : k + 1, :] for k in range(4)], axis=1)
    all_gain[other] = jnp.broadcast_to(0.5 * row, (8, C))


def block_at(b, buf, all_taps, all_out, all_gain):
    run_block(
        buf,
        buf,
        lambda k: all_taps[b, :k, :],
        lambda: all_out[b],
        all_gain[b, 0:1, :],
    )


def encode_body(steps, last, v, all_taps, all_out, all_gain, qw, qb, *rest):
    section = lax.axis_index("section")
    codes, stats, buf, sums = rest[-4:]
    sums[...] = rest[0][...] if len(rest) > 4 else jnp.zeros_like(sums)
    row = lax.broadcasted_iota(jnp.int32, (CODE_ROWS, CLIPS * ROWS), 0)
    top = lax.broadcasted_iota(jnp.int32, (CODE_ROWS, 128), 0)
    lane = lax.broadcasted_iota(jnp.int32, (CODE_ROWS, 128), 1)

    def chunk(i, t):
        buf[...] = v[t]

        def step(b, _):
            block_at(b, buf, all_taps, all_out, all_gain)
            return 0

        lax.fori_loop(1 - section, 2, step, 0)
        logits = jnp.dot(
            buf[...].reshape(CLIPS * ROWS, C), qw[...], preferred_element_type=jnp.float32
        )
        z = (4.0 * (logits + qb[0:1, :])).T[:CODE_ROWS]
        size = jnp.abs(z)
        e = jnp.exp(-size)
        r = 1.0 / (1.0 + e)
        p = jnp.where(z >= 0, r, e * r)
        entropy = jnp.log1p(e) + size * (e * r)
        valid = row < BITS
        codes[i] = jnp.where(valid, 2.0 * p - 1.0, 0.0).astype(jnp.bfloat16)
        bit_sums = jnp.sum(jnp.where(valid, p, 0.0), axis=1, keepdims=True)
        total = jnp.sum(
            jnp.sum(jnp.where(valid, entropy, 0.0), axis=1, keepdims=True), axis=0, keepdims=True
        )
        column = jnp.where(top == BITS, total, bit_sums)
        sums[...] += jnp.where(lane == batch_of(t), column, 0.0)

    for i, t in enumerate(steps):
        pl.when(has_chunk(t, (0, 1)))(functools.partial(chunk, i, t))

    if last:
        full = jnp.concatenate([sums[...], jnp.zeros((128 - CODE_ROWS, 128), jnp.float32)], axis=0)
        stats[...] = full.T[:8]
    else:
        stats[...] = sums[...]


def decode_body(steps, v, all_taps, all_out, all_gain, post, codes, errors, buf):
    def chunk(i, t):
        quantized = lax.dot_general(
            codes[i], post[...], (((0,), (0,)), ((), ())), preferred_element_type=jnp.float32
        )
        buf[...] = quantized.astype(jnp.bfloat16).reshape(CLIPS, ROWS, C)

        def step(b, _):
            block_at(b, buf, all_taps, all_out, all_gain)
            return 0

        lax.fori_loop(0, 2, step, 0)
        for c in range(CLIPS):
            differ = buf[c].astype(jnp.float32) - v[t, c].astype(jnp.float32)
            square = differ * differ
            part = (
                square[:, :128] + square[:, 128:256] + square[:, 256:384] + square[:, 384:]
            )
            mean = jnp.sum(part.T, axis=0, keepdims=True) * (1.0 / C)
            errors[i, 2 * c : 2 * c + 1, :] = mean[:, :128]
            errors[i, 2 * c + 1 : 2 * c + 2, :] = mean[:, 128:]

    for i, t in enumerate(steps):
        pl.when(has_chunk(t, (2, 3)))(functools.partial(chunk, i, t))


def unpack(target, source):
    for c in range(CLIPS):
        row = source[2 * c : 2 * c + 2, :]
        target[c : c + 1, :] = jnp.concatenate([row[0:1], row[1:2]], axis=1)


def final_body(rows_total, order, mine, next_, cross, far, e0, e34, error, loss):
    section = lax.axis_index("section")
    a, b, c, d = mine[0:8], next_[0:8], cross[0:8], far[0:8]
    sums = (jnp.where(section <= 1, a + b, c + d)) * (1.0 / rows_total)
    row = lax.broadcasted_iota(jnp.int32, sums.shape, 0)
    lane = lax.broadcasted_iota(jnp.int32, sums.shape, 1)
    averaged = jnp.zeros_like(sums)
    running = None
    for t in range(8):
        here = row == order[t]
        marginal = jnp.sum(jnp.where(here, sums, 0.0), axis=0, keepdims=True)
        running = marginal if t == 0 else 0.5 * running + 0.5 * marginal
        averaged = jnp.where(here, running, averaged)
    smoothed = jnp.where(lane < BITS, 0.05 + 0.9 * averaged, 0.5)
    term = smoothed * jnp.log(smoothed) + (1.0 - smoothed) * jnp.log(1.0 - smoothed)
    term = jnp.where(lane < BITS, term, jnp.where(lane == BITS, sums, 0.0))
    result = jnp.sum(term, axis=1, keepdims=True)
    flat = jnp.sum(jnp.where(row == lane, result, 0.0), axis=0)
    loss[...] = flat[:8]

    @pl.when(section <= 1)
    def _():
        unpack(error.at[0], cross.at[pl.ds(8, 8)])
        unpack(error.at[1], cross.at[pl.ds(16, 8)])

    @pl.when(section == 2)
    def _():
        unpack(error.at[0], e0.at[0])
        unpack(error.at[1], e34.at[0])

    @pl.when(section == 3)
    def _():
        unpack(error.at[0], e34.at[0])
        unpack(error.at[1], e34.at[1])


PAIR = ((0, 1), (1, 0), (2, 3), (3, 2))
CROSS = ((0, 3), (3, 0), (1, 2), (2, 1))
FAR = ((0, 2), (2, 0), (1, 3), (3, 1))


def shifted(x, axis, by):
    n = lax.axis_size(axis)
    return lax.ppermute(x, axis, [(i, (i + by) % n) for i in range(n)])


def around(x, by):
    n, m = lax.axis_size("dp_0"), lax.axis_size("dp_1")
    pairs = []
    for i in range(n):
        for j in range(m):
            along_0 = (((i + by) % n) * m + j) * 2
            along_1 = (i * m + (j + by) % m) * 2
            targets = (along_0, along_1) if by == 1 else (along_1, along_0)
            pairs.append(((i * m + j) * 2, targets[0]))
            pairs.append(((i * m + j) * 2 + 1, targets[1] + 1))
    return lax.ppermute(x, DP, pairs)


def plane_sum(x):
    n = lax.axis_size(DP)
    return jnp.sum(lax.all_to_all(jnp.broadcast_to(x[None], (n, *x.shape)), DP, 0, 0), axis=0)


def on_device(pool, index, order, taps, out_weight, gain, quant_weight, quant_bias, post_weight):
    bf16, f32 = jnp.bfloat16, jnp.float32
    taps = taps.reshape(3 * C, C)
    out_weight = out_weight.reshape(C, C)
    dma = pltpu.SemaphoreType.DMA
    index = index.T
    encoder = (lax.axis_index("section") <= 1).astype(jnp.int32)
    gain, encoder = lax.optimization_barrier((gain, encoder))
    chunk = (CLIPS, ROWS, C)
    kinds = [((2, 3 * C, C), bf16), ((2, C, C), bf16), ((2, 8, C), f32)]

    pool, taps, out_weight = (
        pltpu.with_memory_space_constraint(x, pltpu.HBM) for x in (pool, taps, out_weight)
    )
    gain, qwt, post_weight, index = (
        pltpu.with_memory_space_constraint(x, pltpu.HBM)
        for x in (gain, quant_weight.T, post_weight, index)
    )
    qbias = pltpu.with_memory_space_constraint(quant_bias.reshape(1, BITS), pltpu.HBM)
    piece, second = call(
        prep_body,
        [HB] * 3,
        [((PIECE, 128), bf16), ((HALF, 128), bf16)],
        [pltpu.VMEM((1, C), bf16), dma((11,))],
    )(taps, out_weight, gain)
    mine = lax.ppermute(piece, "section", PAIR)
    second = lax.ppermute(second, "section", PAIR)
    v_kind = ((STEPS, *chunk), bf16)
    v, *weights, qw, qb, post = call(
        functools.partial(start_body, 2),
        [HB] * 8,
        [v_kind, *kinds, ((C, 128), bf16), ((8, 128), f32), ((CODE_ROWS, C), bf16)],
        [
            pltpu.SMEM(index.shape, jnp.int32),
            pltpu.VMEM((1, C), bf16),
            pltpu.VMEM((BITS, C), bf16),
            pltpu.VMEM((1, BITS), f32),
            pltpu.VMEM((BITS, C), bf16),
            dma((7 + STEPS * CLIPS,)),
        ],
        blocks=2,
    )(pool, index, taps, out_weight, gain, qwt, qbias, post_weight)
    mine, v = lax.optimization_barrier((mine, v))
    up = around(mine, 1)
    down = around(mine, -1)
    mine_s = shifted(mine, "dp_2", 1)
    (v,) = call(
        functools.partial(more_body, 2, STEPS), [VM] * 4, [v_kind], blocks=3, aliases={0: 0}
    )(v, *weights)
    up, down, second, mine_s, v = lax.optimization_barrier((up, down, second, mine_s, v))
    swapped = [mine_s] + [shifted(x, "dp_2", 1) for x in (second, up, down)]
    weights = call(
        join_body, [VM] + [ANY] * 7 + [VM] * 3, kinds, [dma((24,))], aliases={8: 0, 9: 1, 10: 2}
    )(mine, second, up, down, *swapped, *weights)

    def encode(steps, before, last):
        n = len(steps)
        return call(
            functools.partial(encode_body, steps, last),
            [VM] * (6 + len(before)),
            [((n, CODE_ROWS, CLIPS * ROWS), bf16), ((8 if last else CODE_ROWS, 128), f32)],
            [pltpu.VMEM(chunk, bf16), pltpu.VMEM((CODE_ROWS, 128), f32)],
            blocks=2 * n,
        )(v, *weights, qw, qb, *before)

    def decode(steps, codes):
        n = len(steps)
        return call(
            functools.partial(decode_body, steps),
            [VM] * 6,
            [((n, 8, 128), f32)],
            [pltpu.VMEM(chunk, bf16)],
            blocks=2 * n,
        )(v, *weights, post, codes)[0]

    codes, stats = encode((0,), (), False)
    codes_a = lax.ppermute(codes, "section", FAR)
    codes, stats = encode((1, 2), (stats,), False)
    codes_b = lax.ppermute(codes, "section", CROSS)
    codes, stats = encode((3, 4), (stats,), True)
    codes_c = lax.ppermute(codes, "section", ((0, 3), (1, 2)))
    codes_a, stats = lax.optimization_barrier((codes_a, stats))
    e0 = decode((0,), codes_a)
    codes_b, e0 = lax.optimization_barrier((codes_b, e0))
    e12 = decode((1, 2), codes_b)
    codes_c, e12 = lax.optimization_barrier((codes_c, e12))
    e34 = decode((3, 4), codes_c)
    stats, e12, e34, encoder = lax.optimization_barrier((stats, e12, e34, encoder))
    total = lax.cond(encoder == 1, plane_sum, lambda x: 0.0 * x, stats)
    packed = jnp.concatenate([total, e12[0], e12[1]], axis=0)
    near, cross, far = (lax.ppermute(packed, "section", pairs) for pairs in (PAIR, CROSS, FAR))
    rows_total = float(CLIPS * lax.axis_size(DP) * ROWS)
    error, loss = call(
        functools.partial(final_body, rows_total),
        [SM] + [VM] * 6,
        [((2, CLIPS, ROWS), f32), ((8,), f32)],
    )(order, packed, near, cross, far, e0, e34)
    return error, loss


def solution(mesh):
    torus = Mesh(
        mesh.devices.reshape(mesh.shape["section"], 4, 4, 2), ("section", "dp_0", "dp_1", "dp_2")
    )
    return jax.shard_map(
        on_device,
        mesh=torus,
        in_specs=(
            P(DP, None, None),
            P(None, DP),
            P(),
            P("section", None, None, None),
            P("section", None, None),
            P("section", None),
            P(),
            P(),
            P(),
        ),
        out_specs=(P("section", DP, None), P()),
        check_vma=False,
    )
```

```python
import functools

import jax
import jax.numpy as jnp
from jax import lax
from jax.experimental import pallas as pl
from jax.experimental.pallas import tpu as pltpu
from jax.sharding import Mesh
from jax.sharding import PartitionSpec as P


DP = ("dp_0", "dp_1", "dp_2")
EPS = 1e-06
C = 512
BITS = 18
FRAME = 64
ROWS = 256
CLIPS = 4
FRAMES = ROWS // FRAME
CHUNKS = ((4, 0, 1, 6, 7), (None, 2, 3, 5, None), (4, 2, 3, 5, None), (None, 0, 1, 6, 7))
STEPS = len(CHUNKS[0])
CODE_ROWS = 24
HALF = 1024
PIECE = HALF + 16
VM = pl.BlockSpec(memory_space=pltpu.VMEM)
SM = pl.BlockSpec(memory_space=pltpu.SMEM)
HB = pl.BlockSpec(memory_space=pltpu.HBM)
ANY = pl.BlockSpec(memory_space=pl.ANY)


def call(body, ins, outs, scratch=(), limit=24, aliases={}, blocks=0):
    return pl.pallas_call(
        body,
        in_specs=list(ins),
        out_specs=[VM] * len(outs),
        out_shape=[jax.ShapeDtypeStruct(shape, kind) for shape, kind in outs],
        scratch_shapes=list(scratch),
        compiler_params=pltpu.CompilerParams(vmem_limit_bytes=limit * 2**20),
        input_output_aliases=aliases,
        cost_estimate=pl.CostEstimate(
            flops=blocks * CLIPS * ROWS * C * C * 8, transcendentals=0, bytes_accessed=0
        ),
    )


def run_block(src, dst, taps, out_weight, half_gain):
    frames = [
        src[:, f * FRAME : (f + 1) * FRAME, :].reshape(CLIPS * FRAME, C) for f in range(FRAMES)
    ]
    normed = []
    for v in frames:
        w = v.astype(jnp.float32)
        mean = jnp.mean(w * w, axis=-1, keepdims=True)
        normed.append((w * lax.rsqrt(mean + EPS) * half_gain).astype(jnp.bfloat16))
    first = jnp.dot(normed[0], taps(C), preferred_element_type=jnp.float32)
    second = jnp.dot(
        jnp.concatenate([normed[1], normed[0]], axis=1),
        taps(2 * C),
        preferred_element_type=jnp.float32,
    )
    rest = jnp.concatenate(
        [
            jnp.concatenate([normed[f], normed[f - 1], normed[f - 2]], axis=1)
            for f in range(2, FRAMES)
        ],
        axis=0,
    )
    third = jnp.dot(rest, taps(3 * C), preferred_element_type=jnp.float32)
    h = jnp.concatenate([first, second, third], axis=0)
    activated = (h + h * jnp.tanh(h)).astype(jnp.bfloat16)
    update = jnp.dot(activated, out_weight(), preferred_element_type=jnp.float32)
    for f in range(FRAMES):
        part = update[f * CLIPS * FRAME : (f + 1) * CLIPS * FRAME]
        dst[:, f * FRAME : (f + 1) * FRAME, :] = (
            (frames[f].astype(jnp.float32) + part)
            .astype(jnp.bfloat16)
            .reshape(CLIPS, FRAME, C)
        )


def prep_body(taps, out_weight, gain_hbm, piece, second, gain, sems):
    core = lax.axis_index("dp_2")
    gain_copy = pltpu.make_async_copy(gain_hbm, gain, sems.at[10])
    gain_copy.start()

    own = 2 * lax.rem(lax.axis_index("dp_0"), 2) + lax.rem(lax.axis_index("dp_1"), 2)

    def copies(target, colour, at):
        lanes = pl.ds(pl.multiple_of(colour * 128, 128), 128)
        lower = [
            pltpu.make_async_copy(
                taps.at[pl.ds(0, HALF), lanes], target.at[pl.ds(0, HALF)], sems.at[at]
            )
        ]
        upper = [
            pltpu.make_async_copy(
                taps.at[pl.ds(HALF, 512), lanes], target.at[pl.ds(0, 512)], sems.at[at]
            )
        ]
        for j in range(4):
            upper.append(
                pltpu.make_async_copy(
                    out_weight.at[lanes, pl.ds(128 * j, 128)],
                    target.at[pl.ds(512 + 128 * j, 128)],
                    sems.at[at + 1 + j],
                )
            )
        return lower, upper

    sets = [copies(piece, own, 0), copies(second, 3 - own, 5)]
    for side in range(2):

        @pl.when(core == side)
        def _(side=side):
            chosen = sets[0][side] + sets[1][side]
            for copy in chosen:
                copy.start()
            for copy in chosen:
                copy.wait()

    gain_copy.wait()
    wide = gain[...].astype(jnp.float32)
    rows = [wide[:, 128 * j : 128 * (j + 1)] for j in range(4)]
    rows.append(jnp.zeros((12, 128), jnp.float32))
    piece[HALF:, :] = jnp.concatenate(rows, axis=0).astype(jnp.bfloat16)


def batch_of(t):
    section = lax.axis_index("section")
    batch = jnp.int32(0)
    for k in range(4):
        if CHUNKS[k][t] is not None:
            batch = jnp.where(section == k, CHUNKS[k][t], batch)
    return batch


def has_chunk(t, sections):
    section = lax.axis_index("section")
    found = [section == k for k in sections if CHUNKS[k][t] is not None]
    return functools.reduce(jnp.logical_or, found)


def start_body(
    steps, pool, index_hbm, taps, out_weight, gain_hbm, qwt_hbm, qbias_hbm, postw_hbm,
    v, all_taps, all_out, all_gain, qw, qb, post,
    index, gain, qwt, qbias, postw, sems,
):
    own = lax.rem(lax.axis_index("section"), 2)
    pairs = [
        (index_hbm, index),
        (taps, all_taps.at[own]),
        (out_weight, all_out.at[own]),
        (gain_hbm, gain),
        (qwt_hbm, qwt),
        (qbias_hbm, qbias),
        (postw_hbm, postw),
    ]
    small = [pltpu.make_async_copy(a, b, sems.at[k]) for k, (a, b) in enumerate(pairs)]
    for copy in small:
        copy.start()
    small[0].wait()
    copies = []
    for t in range(STEPS):
        batch = batch_of(t)
        for c in range(CLIPS):
            copy = pltpu.make_async_copy(
                pool.at[index[c, batch]], v.at[t, c], sems.at[len(pairs) + t * CLIPS + c]
            )
            copy.start()
            copies.append(copy)
    for copy in small[1:]:
        copy.wait()
    all_gain[own] = jnp.broadcast_to(0.5 * gain[...].astype(jnp.float32), (8, C))
    wide = jnp.concatenate(
        [qwt[...].astype(jnp.float32), jnp.zeros((128 - BITS, C), jnp.float32)], axis=0
    )
    qw[...] = wide.T.astype(jnp.bfloat16)
    qb[...] = jnp.zeros((8, 128), jnp.float32)
    qb[0:1, 0:BITS] = qbias[...]
    post[...] = jnp.zeros((CODE_ROWS, C), jnp.bfloat16)
    post[0:BITS, :] = postw[...]
    for copy in copies[: steps * CLIPS]:
        copy.wait()
    first_block(0, steps, v, all_taps, all_out, all_gain)
    for copy in copies[steps * CLIPS :]:
        copy.wait()


def first_block(begin, end, v, all_taps, all_out, all_gain):
    @pl.when(lax.axis_index("section") == 0)
    def _():
        def step(t, _):
            block_at(0, v.at[t], all_taps, all_out, all_gain)
            return 0

        lax.fori_loop(begin, end, step, 0)


def more_body(begin, end, before, all_taps, all_out, all_gain, v):
    first_block(begin, end, v, all_taps, all_out, all_gain)


def join_body(*refs):
    pieces, (all_taps, all_out, all_gain), sems = refs[:8], refs[11:14], refs[14]
    section = lax.axis_index("section")
    core = lax.axis_index("dp_2")
    other = 1 - lax.rem(section, 2)

    def place(lower, upper):
        copies = []
        for j in range(4):
            lanes = pl.ds(128 * j, 128)
            copies.append(
                pltpu.make_async_copy(
                    lower[j].at[pl.ds(0, HALF)],
                    all_taps.at[other, pl.ds(0, HALF), lanes],
                    sems.at[j],
                )
            )
            copies.append(
                pltpu.make_async_copy(
                    upper[j].at[pl.ds(0, 512)],
                    all_taps.at[other, pl.ds(HALF, 512), lanes],
                    sems.at[4 + j],
                )
            )
            for k in range(4):
                copies.append(
                    pltpu.make_async_copy(
                        upper[j].at[pl.ds(512 + 128 * k, 128)],
                        all_out.at[other, pl.ds(128 * j, 128), pl.ds(128 * k, 128)],
                        sems.at[8 + 4 * j + k],
                    )
                )
        for copy in copies:
            copy.start()
        for copy in copies:
            copy.wait()

    @pl.when(core == 0)
    def _():
        place(pieces[:4], pieces[4:])

    @pl.when(core == 1)
    def _():
        place(pieces[4:], pieces[:4])

    rows = pieces[0][HALF:, :].astype(jnp.float32)
    row = jnp.concatenate([rows[k : k + 1, :] for k in range(4)], axis=1)
    all_gain[other] = jnp.broadcast_to(0.5 * row, (8, C))


def block_at(b, buf, all_taps, all_out, all_gain):
    run_block(
        buf,
        buf,
        lambda k: all_taps[b, :k, :],
        lambda: all_out[b],
        all_gain[b, 0:1, :],
    )


def encode_body(steps, last, v, all_taps, all_out, all_gain, qw, qb, *rest):
    section = lax.axis_index("section")
    codes, stats, buf, sums = rest[-4:]
    sums[...] = rest[0][...] if len(rest) > 4 else jnp.zeros_like(sums)
    row = lax.broadcasted_iota(jnp.int32, (CODE_ROWS, CLIPS * ROWS), 0)
    top = lax.broadcasted_iota(jnp.int32, (CODE_ROWS, 128), 0)
    lane = lax.broadcasted_iota(jnp.int32, (CODE_ROWS, 128), 1)

    def chunk(i, t):
        buf[...] = v[t]

        def step(b, _):
            block_at(b, buf, all_taps, all_out, all_gain)
            return 0

        lax.fori_loop(1 - section, 2, step, 0)
        logits = jnp.dot(
            buf[...].reshape(CLIPS * ROWS, C), qw[...], preferred_element_type=jnp.float32
        )
        z = (4.0 * (logits + qb[0:1, :])).T[:CODE_ROWS]
        size = jnp.abs(z)
        e = jnp.exp(-size)
        r = 1.0 / (1.0 + e)
        p = jnp.where(z >= 0, r, e * r)
        entropy = jnp.log1p(e) + size * (e * r)
        valid = row < BITS
        codes[i] = jnp.where(valid, 2.0 * p - 1.0, 0.0).astype(jnp.bfloat16)
        bit_sums = jnp.sum(jnp.where(valid, p, 0.0), axis=1, keepdims=True)
        total = jnp.sum(
            jnp.sum(jnp.where(valid, entropy, 0.0), axis=1, keepdims=True), axis=0, keepdims=True
        )
        column = jnp.where(top == BITS, total, bit_sums)
        sums[...] += jnp.where(lane == batch_of(t), column, 0.0)

    for i, t in enumerate(steps):
        pl.when(has_chunk(t, (0, 1)))(functools.partial(chunk, i, t))

    if last:
        full = jnp.concatenate([sums[...], jnp.zeros((128 - CODE_ROWS, 128), jnp.float32)], axis=0)
        stats[...] = full.T[:8]
    else:
        stats[...] = sums[...]


def decode_body(steps, v, all_taps, all_out, all_gain, post, codes, errors, buf):
    def chunk(i, t):
        quantized = lax.dot_general(
            codes[i], post[...], (((0,), (0,)), ((), ())), preferred_element_type=jnp.float32
        )
        buf[...] = quantized.astype(jnp.bfloat16).reshape(CLIPS, ROWS, C)

        def step(b, _):
            block_at(b, buf, all_taps, all_out, all_gain)
            return 0

        lax.fori_loop(0, 2, step, 0)
        for c in range(CLIPS):
            differ = buf[c].astype(jnp.float32) - v[t, c].astype(jnp.float32)
            square = differ * differ
            part = (
                square[:, :128] + square[:, 128:256] + square[:, 256:384] + square[:, 384:]
            )
            mean = jnp.sum(part.T, axis=0, keepdims=True) * (1.0 / C)
            errors[i, 2 * c : 2 * c + 1, :] = mean[:, :128]
            errors[i, 2 * c + 1 : 2 * c + 2, :] = mean[:, 128:]

    for i, t in enumerate(steps):
        pl.when(has_chunk(t, (2, 3)))(functools.partial(chunk, i, t))


def unpack(target, source):
    for c in range(CLIPS):
        row = source[2 * c : 2 * c + 2, :]
        target[c : c + 1, :] = jnp.concatenate([row[0:1], row[1:2]], axis=1)


def final_body(rows_total, order, mine, next_, cross, far, e0, e34, error, loss):
    section = lax.axis_index("section")
    a, b, c, d = mine[0:8], next_[0:8], cross[0:8], far[0:8]
    sums = (jnp.where(section <= 1, a + b, c + d)) * (1.0 / rows_total)
    row = lax.broadcasted_iota(jnp.int32, sums.shape, 0)
    lane = lax.broadcasted_iota(jnp.int32, sums.shape, 1)
    averaged = jnp.zeros_like(sums)
    running = None
    for t in range(8):
        here = row == order[t]
        marginal = jnp.sum(jnp.where(here, sums, 0.0), axis=0, keepdims=True)
        running = marginal if t == 0 else 0.5 * running + 0.5 * marginal
        averaged = jnp.where(here, running, averaged)
    smoothed = jnp.where(lane < BITS, 0.05 + 0.9 * averaged, 0.5)
    term = smoothed * jnp.log(smoothed) + (1.0 - smoothed) * jnp.log(1.0 - smoothed)
    term = jnp.where(lane < BITS, term, jnp.where(lane == BITS, sums, 0.0))
    result = jnp.sum(term, axis=1, keepdims=True)
    flat = jnp.sum(jnp.where(row == lane, result, 0.0), axis=0)
    loss[...] = flat[:8]

    @pl.when(section <= 1)
    def _():
        unpack(error.at[0], cross.at[pl.ds(8, 8)])
        unpack(error.at[1], cross.at[pl.ds(16, 8)])

    @pl.when(section == 2)
    def _():
        unpack(error.at[0], e0.at[0])
        unpack(error.at[1], e34.at[0])

    @pl.when(section == 3)
    def _():
        unpack(error.at[0], e34.at[0])
        unpack(error.at[1], e34.at[1])


PAIR = ((0, 1), (1, 0), (2, 3), (3, 2))
CROSS = ((0, 3), (3, 0), (1, 2), (2, 1))
FAR = ((0, 2), (2, 0), (1, 3), (3, 1))


def shifted(x, axis, by):
    n = lax.axis_size(axis)
    return lax.ppermute(x, axis, [(i, (i + by) % n) for i in range(n)])


def within_corner(x, first):
    n, m = lax.axis_size("dp_0"), lax.axis_size("dp_1")
    pairs = []
    for i in range(n):
        for j in range(m):
            for core in range(2):
                to = (i ^ 1, j) if (core == 0) == first else (i, j ^ 1)
                pairs.append(((i * m + j) * 2 + core, (to[0] * m + to[1]) * 2 + core))
    return lax.ppermute(x, DP, pairs)


def plane_sum(x):
    n = lax.axis_size(DP)
    return jnp.sum(lax.all_to_all(jnp.broadcast_to(x[None], (n, *x.shape)), DP, 0, 0), axis=0)


def on_device(pool, index, order, taps, out_weight, gain, quant_weight, quant_bias, post_weight):
    bf16, f32 = jnp.bfloat16, jnp.float32
    taps = taps.reshape(3 * C, C)
    out_weight = out_weight.reshape(C, C)
    dma = pltpu.SemaphoreType.DMA
    index = index.T
    encoder = (lax.axis_index("section") <= 1).astype(jnp.int32)
    gain, encoder = lax.optimization_barrier((gain, encoder))
    chunk = (CLIPS, ROWS, C)
    kinds = [((2, 3 * C, C), bf16), ((2, C, C), bf16), ((2, 8, C), f32)]

    pool, taps, out_weight = (
        pltpu.with_memory_space_constraint(x, pltpu.HBM) for x in (pool, taps, out_weight)
    )
    gain, qwt, post_weight, index = (
        pltpu.with_memory_space_constraint(x, pltpu.HBM)
        for x in (gain, quant_weight.T, post_weight, index)
    )
    qbias = pltpu.with_memory_space_constraint(quant_bias.reshape(1, BITS), pltpu.HBM)
    piece, second = call(
        prep_body,
        [HB] * 3,
        [((PIECE, 128), bf16), ((HALF, 128), bf16)],
        [pltpu.VMEM((1, C), bf16), dma((11,))],
    )(taps, out_weight, gain)
    mine = lax.ppermute(piece, "section", PAIR)
    second = lax.ppermute(second, "section", PAIR)
    v_kind = ((STEPS, *chunk), bf16)
    v, *weights, qw, qb, post = call(
        functools.partial(start_body, 2),
        [HB] * 8,
        [v_kind, *kinds, ((C, 128), bf16), ((8, 128), f32), ((CODE_ROWS, C), bf16)],
        [
            pltpu.SMEM(index.shape, jnp.int32),
            pltpu.VMEM((1, C), bf16),
            pltpu.VMEM((BITS, C), bf16),
            pltpu.VMEM((1, BITS), f32),
            pltpu.VMEM((BITS, C), bf16),
            dma((7 + STEPS * CLIPS,)),
        ],
        blocks=2,
    )(pool, index, taps, out_weight, gain, qwt, qbias, post_weight)
    mine, v = lax.optimization_barrier((mine, v))
    up = within_corner(mine, True)
    down = within_corner(mine, False)
    mine_s = shifted(mine, "dp_2", 1)
    (v,) = call(
        functools.partial(more_body, 2, STEPS), [VM] * 4, [v_kind], blocks=3, aliases={0: 0}
    )(v, *weights)
    up, down, second, mine_s, v = lax.optimization_barrier((up, down, second, mine_s, v))
    swapped = [mine_s] + [shifted(x, "dp_2", 1) for x in (second, down, up)]
    weights = call(
        join_body, [VM] + [ANY] * 7 + [VM] * 3, kinds, [dma((24,))], aliases={8: 0, 9: 1, 10: 2}
    )(mine, second, up, down, *swapped, *weights)

    def encode(steps, before, last):
        n = len(steps)
        return call(
            functools.partial(encode_body, steps, last),
            [VM] * (6 + len(before)),
            [((n, CODE_ROWS, CLIPS * ROWS), bf16), ((8 if last else CODE_ROWS, 128), f32)],
            [pltpu.VMEM(chunk, bf16), pltpu.VMEM((CODE_ROWS, 128), f32)],
            blocks=2 * n,
        )(v, *weights, qw, qb, *before)

    def decode(steps, codes):
        n = len(steps)
        return call(
            functools.partial(decode_body, steps),
            [VM] * 6,
            [((n, 8, 128), f32)],
            [pltpu.VMEM(chunk, bf16)],
            blocks=2 * n,
        )(v, *weights, post, codes)[0]

    codes, stats = encode((0,), (), False)
    codes_a = lax.ppermute(codes, "section", FAR)
    codes, stats = encode((1, 2), (stats,), False)
    e0 = decode((0,), codes_a)
    codes, e0 = lax.optimization_barrier((codes, e0))
    codes_b = lax.ppermute(codes, "section", CROSS)
    codes, stats = encode((3, 4), (stats,), True)
    codes_c = lax.ppermute(codes, "section", ((0, 3), (1, 2)))
    codes_b, stats = lax.optimization_barrier((codes_b, stats))
    e12 = decode((1, 2), codes_b)
    codes_c, e12 = lax.optimization_barrier((codes_c, e12))
    e34 = decode((3, 4), codes_c)
    stats, e12, e34, encoder = lax.optimization_barrier((stats, e12, e34, encoder))
    total = lax.cond(encoder == 1, plane_sum, lambda x: 0.0 * x, stats)
    packed = jnp.concatenate([total, e12[0], e12[1]], axis=0)
    near, cross, far = (lax.ppermute(packed, "section", pairs) for pairs in (PAIR, CROSS, FAR))
    rows_total = float(CLIPS * lax.axis_size(DP) * ROWS)
    error, loss = call(
        functools.partial(final_body, rows_total),
        [SM] + [VM] * 6,
        [((2, CLIPS, ROWS), f32), ((8,), f32)],
    )(order, packed, near, cross, far, e0, e34)
    return error, loss


def solution(mesh):
    torus = Mesh(
        mesh.devices.reshape(mesh.shape["section"], 4, 4, 2), ("section", "dp_0", "dp_1", "dp_2")
    )
    return jax.shard_map(
        on_device,
        mesh=torus,
        in_specs=(
            P(DP, None, None),
            P(None, DP),
            P(),
            P("section", None, None, None),
            P("section", None, None),
            P("section", None),
            P(),
            P(),
            P(),
        ),
        out_specs=(P("section", DP, None), P()),
        check_vma=False,
    )
```

```python
import functools

import jax
import jax.numpy as jnp
from jax import lax
from jax.experimental import pallas as pl
from jax.experimental.pallas import tpu as pltpu
from jax.sharding import Mesh
from jax.sharding import PartitionSpec as P


DP = ("dp_0", "dp_1", "dp_2")
EPS = 1e-06
C = 512
BITS = 18
FRAME = 64
ROWS = 256
CLIPS = 4
FRAMES = ROWS // FRAME
CHUNKS = ((4, 0, 1, 6, 7), (None, 2, 3, 5, None), (4, 2, 3, 5, None), (None, 0, 1, 6, 7))
STEPS = len(CHUNKS[0])
CODE_ROWS = 24
HALF = 1024
PIECE = HALF + 16
VM = pl.BlockSpec(memory_space=pltpu.VMEM)
SM = pl.BlockSpec(memory_space=pltpu.SMEM)
HB = pl.BlockSpec(memory_space=pltpu.HBM)
ANY = pl.BlockSpec(memory_space=pl.ANY)


def call(body, ins, outs, scratch=(), limit=24, aliases={}, blocks=0):
    return pl.pallas_call(
        body,
        in_specs=list(ins),
        out_specs=[VM] * len(outs),
        out_shape=[jax.ShapeDtypeStruct(shape, kind) for shape, kind in outs],
        scratch_shapes=list(scratch),
        compiler_params=pltpu.CompilerParams(vmem_limit_bytes=limit * 2**20),
        input_output_aliases=aliases,
        cost_estimate=pl.CostEstimate(
            flops=blocks * CLIPS * ROWS * C * C * 8, transcendentals=0, bytes_accessed=0
        ),
    )


def run_block(src, dst, taps, out_weight, half_gain):
    frames = [
        src[:, f * FRAME : (f + 1) * FRAME, :].reshape(CLIPS * FRAME, C) for f in range(FRAMES)
    ]
    normed = []
    for v in frames:
        w = v.astype(jnp.float32)
        mean = jnp.mean(w * w, axis=-1, keepdims=True)
        normed.append((w * lax.rsqrt(mean + EPS) * half_gain).astype(jnp.bfloat16))
    first = jnp.dot(normed[0], taps(C), preferred_element_type=jnp.float32)
    second = jnp.dot(
        jnp.concatenate([normed[1], normed[0]], axis=1),
        taps(2 * C),
        preferred_element_type=jnp.float32,
    )
    rest = jnp.concatenate(
        [
            jnp.concatenate([normed[f], normed[f - 1], normed[f - 2]], axis=1)
            for f in range(2, FRAMES)
        ],
        axis=0,
    )
    third = jnp.dot(rest, taps(3 * C), preferred_element_type=jnp.float32)
    h = jnp.concatenate([first, second, third], axis=0)
    activated = (h + h * jnp.tanh(h)).astype(jnp.bfloat16)
    update = jnp.dot(activated, out_weight(), preferred_element_type=jnp.float32)
    for f in range(FRAMES):
        part = update[f * CLIPS * FRAME : (f + 1) * CLIPS * FRAME]
        dst[:, f * FRAME : (f + 1) * FRAME, :] = (
            (frames[f].astype(jnp.float32) + part)
            .astype(jnp.bfloat16)
            .reshape(CLIPS, FRAME, C)
        )


def prep_body(taps, out_weight, gain_hbm, piece, second, gain, sems):
    core = lax.axis_index("dp_2")
    gain_copy = pltpu.make_async_copy(gain_hbm, gain, sems.at[10])
    gain_copy.start()

    own = 2 * lax.rem(lax.axis_index("dp_0"), 2) + lax.rem(lax.axis_index("dp_1"), 2)

    def copies(target, colour, at):
        lanes = pl.ds(pl.multiple_of(colour * 128, 128), 128)
        lower = [
            pltpu.make_async_copy(
                taps.at[pl.ds(0, HALF), lanes], target.at[pl.ds(0, HALF)], sems.at[at]
            )
        ]
        upper = [
            pltpu.make_async_copy(
                taps.at[pl.ds(HALF, 512), lanes], target.at[pl.ds(0, 512)], sems.at[at]
            )
        ]
        for j in range(4):
            upper.append(
                pltpu.make_async_copy(
                    out_weight.at[lanes, pl.ds(128 * j, 128)],
                    target.at[pl.ds(512 + 128 * j, 128)],
                    sems.at[at + 1 + j],
                )
            )
        return lower, upper

    sets = [copies(piece, own, 0), copies(second, 3 - own, 5)]
    for side in range(2):

        @pl.when(core == side)
        def _(side=side):
            chosen = sets[0][side] + sets[1][side]
            for copy in chosen:
                copy.start()
            for copy in chosen:
                copy.wait()

    gain_copy.wait()
    wide = gain[...].astype(jnp.float32)
    rows = [wide[:, 128 * j : 128 * (j + 1)] for j in range(4)]
    rows.append(jnp.zeros((12, 128), jnp.float32))
    piece[HALF:, :] = jnp.concatenate(rows, axis=0).astype(jnp.bfloat16)


def batch_of(t):
    section = lax.axis_index("section")
    batch = jnp.int32(0)
    for k in range(4):
        if CHUNKS[k][t] is not None:
            batch = jnp.where(section == k, CHUNKS[k][t], batch)
    return batch


def has_chunk(t, sections):
    section = lax.axis_index("section")
    found = [section == k for k in sections if CHUNKS[k][t] is not None]
    return functools.reduce(jnp.logical_or, found)


def start_body(
    steps, pool, index_hbm, taps, out_weight, gain_hbm, qwt_hbm, qbias_hbm, postw_hbm,
    v, all_taps, all_out, all_gain, qw, qb, post,
    index, gain, qwt, qbias, postw, sems,
):
    own = lax.rem(lax.axis_index("section"), 2)
    pairs = [
        (index_hbm, index),
        (taps, all_taps.at[own]),
        (out_weight, all_out.at[own]),
        (gain_hbm, gain),
        (qwt_hbm, qwt),
        (qbias_hbm, qbias),
        (postw_hbm, postw),
    ]
    small = [pltpu.make_async_copy(a, b, sems.at[k]) for k, (a, b) in enumerate(pairs)]
    for copy in small:
        copy.start()
    small[0].wait()
    copies = []
    for t in range(STEPS):
        batch = batch_of(t)
        for c in range(CLIPS):
            copy = pltpu.make_async_copy(
                pool.at[index[c, batch]], v.at[t, c], sems.at[len(pairs) + t * CLIPS + c]
            )
            copy.start()
            copies.append(copy)
    for copy in small[1:]:
        copy.wait()
    all_gain[own] = jnp.broadcast_to(0.5 * gain[...].astype(jnp.float32), (8, C))
    wide = jnp.concatenate(
        [qwt[...].astype(jnp.float32), jnp.zeros((128 - BITS, C), jnp.float32)], axis=0
    )
    qw[...] = wide.T.astype(jnp.bfloat16)
    qb[...] = jnp.zeros((8, 128), jnp.float32)
    qb[0:1, 0:BITS] = qbias[...]
    post[...] = jnp.zeros((CODE_ROWS, C), jnp.bfloat16)
    post[0:BITS, :] = postw[...]
    for copy in copies[: steps * CLIPS]:
        copy.wait()
    first_block(0, steps, v, all_taps, all_out, all_gain)
    for copy in copies[steps * CLIPS :]:
        copy.wait()


def first_block(begin, end, v, all_taps, all_out, all_gain):
    @pl.when(lax.axis_index("section") == 0)
    def _():
        def step(t, _):
            block_at(0, v.at[t], all_taps, all_out, all_gain)
            return 0

        lax.fori_loop(begin, end, step, 0)


def more_body(begin, end, before, all_taps, all_out, all_gain, v):
    first_block(begin, end, v, all_taps, all_out, all_gain)


def join_body(*refs):
    pieces, (all_taps, all_out, all_gain), sems = refs[:8], refs[11:14], refs[14]
    section = lax.axis_index("section")
    core = lax.axis_index("dp_2")
    other = 1 - lax.rem(section, 2)

    def place(lower, upper):
        copies = []
        for j in range(4):
            lanes = pl.ds(128 * j, 128)
            copies.append(
                pltpu.make_async_copy(
                    lower[j].at[pl.ds(0, HALF)],
                    all_taps.at[other, pl.ds(0, HALF), lanes],
                    sems.at[j],
                )
            )
            copies.append(
                pltpu.make_async_copy(
                    upper[j].at[pl.ds(0, 512)],
                    all_taps.at[other, pl.ds(HALF, 512), lanes],
                    sems.at[4 + j],
                )
            )
            for k in range(4):
                copies.append(
                    pltpu.make_async_copy(
                        upper[j].at[pl.ds(512 + 128 * k, 128)],
                        all_out.at[other, pl.ds(128 * j, 128), pl.ds(128 * k, 128)],
                        sems.at[8 + 4 * j + k],
                    )
                )
        for copy in copies:
            copy.start()
        for copy in copies:
            copy.wait()

    @pl.when(core == 0)
    def _():
        place(pieces[:4], pieces[4:])

    @pl.when(core == 1)
    def _():
        place(pieces[4:], pieces[:4])

    rows = pieces[0][HALF:, :].astype(jnp.float32)
    row = jnp.concatenate([rows[k : k + 1, :] for k in range(4)], axis=1)
    all_gain[other] = jnp.broadcast_to(0.5 * row, (8, C))


def block_at(b, buf, all_taps, all_out, all_gain):
    run_block(
        buf,
        buf,
        lambda k: all_taps[b, :k, :],
        lambda: all_out[b],
        all_gain[b, 0:1, :],
    )


def encode_body(steps, last, v, all_taps, all_out, all_gain, qw, qb, *rest):
    section = lax.axis_index("section")
    codes, stats, buf, sums = rest[-4:]
    sums[...] = rest[0][...] if len(rest) > 4 else jnp.zeros_like(sums)
    row = lax.broadcasted_iota(jnp.int32, (CODE_ROWS, CLIPS * ROWS), 0)
    top = lax.broadcasted_iota(jnp.int32, (CODE_ROWS, 128), 0)
    lane = lax.broadcasted_iota(jnp.int32, (CODE_ROWS, 128), 1)

    def chunk(i, t):
        buf[...] = v[t]

        def step(b, _):
            block_at(b, buf, all_taps, all_out, all_gain)
            return 0

        lax.fori_loop(1 - section, 2, step, 0)
        logits = jnp.dot(
            buf[...].reshape(CLIPS * ROWS, C), qw[...], preferred_element_type=jnp.float32
        )
        z = (4.0 * (logits + qb[0:1, :])).T[:CODE_ROWS]
        size = jnp.abs(z)
        e = jnp.exp(-size)
        r = 1.0 / (1.0 + e)
        p = jnp.where(z >= 0, r, e * r)
        entropy = jnp.log1p(e) + size * (e * r)
        valid = row < BITS
        codes[i] = jnp.where(valid, 2.0 * p - 1.0, 0.0).astype(jnp.bfloat16)
        bit_sums = jnp.sum(jnp.where(valid, p, 0.0), axis=1, keepdims=True)
        total = jnp.sum(
            jnp.sum(jnp.where(valid, entropy, 0.0), axis=1, keepdims=True), axis=0, keepdims=True
        )
        column = jnp.where(top == BITS, total, bit_sums)
        sums[...] += jnp.where(lane == batch_of(t), column, 0.0)

    for i, t in enumerate(steps):
        pl.when(has_chunk(t, (0, 1)))(functools.partial(chunk, i, t))

    if last:
        full = jnp.concatenate([sums[...], jnp.zeros((128 - CODE_ROWS, 128), jnp.float32)], axis=0)
        stats[...] = full.T[:8]
    else:
        stats[...] = sums[...]


def decode_body(steps, v, all_taps, all_out, all_gain, post, codes, errors, buf):
    def chunk(i, t):
        quantized = lax.dot_general(
            codes[i], post[...], (((0,), (0,)), ((), ())), preferred_element_type=jnp.float32
        )
        buf[...] = quantized.astype(jnp.bfloat16).reshape(CLIPS, ROWS, C)

        def step(b, _):
            block_at(b, buf, all_taps, all_out, all_gain)
            return 0

        lax.fori_loop(0, 2, step, 0)
        for c in range(CLIPS):
            differ = buf[c].astype(jnp.float32) - v[t, c].astype(jnp.float32)
            square = differ * differ
            part = (
                square[:, :128] + square[:, 128:256] + square[:, 256:384] + square[:, 384:]
            )
            mean = jnp.sum(part.T, axis=0, keepdims=True) * (1.0 / C)
            errors[i, 2 * c : 2 * c + 1, :] = mean[:, :128]
            errors[i, 2 * c + 1 : 2 * c + 2, :] = mean[:, 128:]

    for i, t in enumerate(steps):
        pl.when(has_chunk(t, (2, 3)))(functools.partial(chunk, i, t))


def unpack(target, source):
    for c in range(CLIPS):
        row = source[2 * c : 2 * c + 2, :]
        target[c : c + 1, :] = jnp.concatenate([row[0:1], row[1:2]], axis=1)


def final_body(rows_total, order, mine, cross, e0, e34, error, loss):
    section = lax.axis_index("section")
    sums = jnp.where(section <= 1, mine[0:8], cross[0:8]) * (1.0 / rows_total)
    row = lax.broadcasted_iota(jnp.int32, sums.shape, 0)
    lane = lax.broadcasted_iota(jnp.int32, sums.shape, 1)
    averaged = jnp.zeros_like(sums)
    running = None
    for t in range(8):
        here = row == order[t]
        marginal = jnp.sum(jnp.where(here, sums, 0.0), axis=0, keepdims=True)
        running = marginal if t == 0 else 0.5 * running + 0.5 * marginal
        averaged = jnp.where(here, running, averaged)
    smoothed = jnp.where(lane < BITS, 0.05 + 0.9 * averaged, 0.5)
    term = smoothed * jnp.log(smoothed) + (1.0 - smoothed) * jnp.log(1.0 - smoothed)
    term = jnp.where(lane < BITS, term, jnp.where(lane == BITS, sums, 0.0))
    result = jnp.sum(term, axis=1, keepdims=True)
    flat = jnp.sum(jnp.where(row == lane, result, 0.0), axis=0)
    loss[...] = flat[:8]

    @pl.when(section <= 1)
    def _():
        unpack(error.at[0], cross.at[pl.ds(8, 8)])
        unpack(error.at[1], cross.at[pl.ds(16, 8)])

    @pl.when(section == 2)
    def _():
        unpack(error.at[0], e0.at[0])
        unpack(error.at[1], e34.at[0])

    @pl.when(section == 3)
    def _():
        unpack(error.at[0], e34.at[0])
        unpack(error.at[1], e34.at[1])


PAIR = ((0, 1), (1, 0), (2, 3), (3, 2))
CROSS = ((0, 3), (3, 0), (1, 2), (2, 1))
FAR = ((0, 2), (2, 0), (1, 3), (3, 1))


def shifted(x, axis, by):
    n = lax.axis_size(axis)
    return lax.ppermute(x, axis, [(i, (i + by) % n) for i in range(n)])


def within_corner(x, first):
    n, m = lax.axis_size("dp_0"), lax.axis_size("dp_1")
    pairs = []
    for i in range(n):
        for j in range(m):
            for core in range(2):
                to = (i ^ 1, j) if (core == 0) == first else (i, j ^ 1)
                pairs.append(((i * m + j) * 2 + core, (to[0] * m + to[1]) * 2 + core))
    return lax.ppermute(x, DP, pairs)


def encoder_sum(x):
    n = lax.axis_size(DP)
    x = x + lax.ppermute(x, "section", PAIR)
    return jnp.sum(lax.all_to_all(jnp.broadcast_to(x[None], (n, *x.shape)), DP, 0, 0), axis=0)


def on_device(pool, index, order, taps, out_weight, gain, quant_weight, quant_bias, post_weight):
    bf16, f32 = jnp.bfloat16, jnp.float32
    taps = taps.reshape(3 * C, C)
    out_weight = out_weight.reshape(C, C)
    dma = pltpu.SemaphoreType.DMA
    index = index.T
    encoder = (lax.axis_index("section") <= 1).astype(jnp.int32)
    gain, encoder = lax.optimization_barrier((gain, encoder))
    chunk = (CLIPS, ROWS, C)
    kinds = [((2, 3 * C, C), bf16), ((2, C, C), bf16), ((2, 8, C), f32)]

    pool, taps, out_weight = (
        pltpu.with_memory_space_constraint(x, pltpu.HBM) for x in (pool, taps, out_weight)
    )
    gain, qwt, post_weight, index = (
        pltpu.with_memory_space_constraint(x, pltpu.HBM)
        for x in (gain, quant_weight.T, post_weight, index)
    )
    qbias = pltpu.with_memory_space_constraint(quant_bias.reshape(1, BITS), pltpu.HBM)
    piece, second = call(
        prep_body,
        [HB] * 3,
        [((PIECE, 128), bf16), ((HALF, 128), bf16)],
        [pltpu.VMEM((1, C), bf16), dma((11,))],
    )(taps, out_weight, gain)
    mine = lax.ppermute(piece, "section", PAIR)
    second = lax.ppermute(second, "section", PAIR)
    v_kind = ((STEPS, *chunk), bf16)
    v, *weights, qw, qb, post = call(
        functools.partial(start_body, 2),
        [HB] * 8,
        [v_kind, *kinds, ((C, 128), bf16), ((8, 128), f32), ((CODE_ROWS, C), bf16)],
        [
            pltpu.SMEM(index.shape, jnp.int32),
            pltpu.VMEM((1, C), bf16),
            pltpu.VMEM((BITS, C), bf16),
            pltpu.VMEM((1, BITS), f32),
            pltpu.VMEM((BITS, C), bf16),
            dma((7 + STEPS * CLIPS,)),
        ],
        blocks=2,
    )(pool, index, taps, out_weight, gain, qwt, qbias, post_weight)
    mine, v = lax.optimization_barrier((mine, v))
    up = within_corner(mine, True)
    down = within_corner(mine, False)
    mine_s = shifted(mine, "dp_2", 1)
    (v,) = call(
        functools.partial(more_body, 2, STEPS), [VM] * 4, [v_kind], blocks=3, aliases={0: 0}
    )(v, *weights)
    up, down, second, mine_s, v = lax.optimization_barrier((up, down, second, mine_s, v))
    swapped = [mine_s] + [shifted(x, "dp_2", 1) for x in (second, down, up)]
    weights = call(
        join_body, [VM] + [ANY] * 7 + [VM] * 3, kinds, [dma((24,))], aliases={8: 0, 9: 1, 10: 2}
    )(mine, second, up, down, *swapped, *weights)

    def encode(steps, before, last):
        n = len(steps)
        return call(
            functools.partial(encode_body, steps, last),
            [VM] * (6 + len(before)),
            [((n, CODE_ROWS, CLIPS * ROWS), bf16), ((8 if last else CODE_ROWS, 128), f32)],
            [pltpu.VMEM(chunk, bf16), pltpu.VMEM((CODE_ROWS, 128), f32)],
            blocks=2 * n,
        )(v, *weights, qw, qb, *before)

    def decode(steps, codes):
        n = len(steps)
        return call(
            functools.partial(decode_body, steps),
            [VM] * 6,
            [((n, 8, 128), f32)],
            [pltpu.VMEM(chunk, bf16)],
            blocks=2 * n,
        )(v, *weights, post, codes)[0]

    codes, stats = encode((0,), (), False)
    codes_a = lax.ppermute(codes, "section", FAR)
    codes, stats = encode((1, 2), (stats,), False)
    e0 = decode((0,), codes_a)
    codes, e0 = lax.optimization_barrier((codes, e0))
    codes_b = lax.ppermute(codes, "section", CROSS)
    codes, stats = encode((3, 4), (stats,), True)
    codes_c = lax.ppermute(codes, "section", ((0, 3), (1, 2)))
    codes_b, stats = lax.optimization_barrier((codes_b, stats))
    e12 = decode((1, 2), codes_b)
    codes_c, e12 = lax.optimization_barrier((codes_c, e12))
    e34 = decode((3, 4), codes_c)
    stats, e12, e34, encoder = lax.optimization_barrier((stats, e12, e34, encoder))
    total = lax.cond(encoder == 1, encoder_sum, lambda x: 0.0 * x, stats)
    packed = jnp.concatenate([total, e12[0], e12[1]], axis=0)
    cross = lax.ppermute(packed, "section", CROSS)
    rows_total = float(CLIPS * lax.axis_size(DP) * ROWS)
    error, loss = call(
        functools.partial(final_body, rows_total),
        [SM] + [VM] * 4,
        [((2, CLIPS, ROWS), f32), ((8,), f32)],
    )(order, packed, cross, e0, e34)
    return error, loss


def solution(mesh):
    torus = Mesh(
        mesh.devices.reshape(mesh.shape["section"], 4, 4, 2), ("section", "dp_0", "dp_1", "dp_2")
    )
    return jax.shard_map(
        on_device,
        mesh=torus,
        in_specs=(
            P(DP, None, None),
            P(None, DP),
            P(),
            P("section", None, None, None),
            P("section", None, None),
            P("section", None),
            P(),
            P(),
            P(),
        ),
        out_specs=(P("section", DP, None), P()),
        check_vma=False,
    )
```

```python
import functools

import jax
import jax.numpy as jnp
from jax import lax
from jax.experimental import pallas as pl
from jax.experimental.pallas import tpu as pltpu
from jax.sharding import Mesh
from jax.sharding import PartitionSpec as P


DP = ("dp_0", "dp_1", "dp_2")
EPS = 1e-06
C = 512
BITS = 18
FRAME = 64
ROWS = 256
CLIPS = 4
FRAMES = ROWS // FRAME
CHUNKS = ((4, 0, 1, 6, 7), (None, 2, 3, 5, None), (4, 2, 3, 5, None), (None, 0, 1, 6, 7))
STEPS = len(CHUNKS[0])
CODE_ROWS = 24
HALF = 1024
PIECE = HALF + 16
VM = pl.BlockSpec(memory_space=pltpu.VMEM)
SM = pl.BlockSpec(memory_space=pltpu.SMEM)
HB = pl.BlockSpec(memory_space=pltpu.HBM)
ANY = pl.BlockSpec(memory_space=pl.ANY)


def call(body, ins, outs, scratch=(), limit=24, aliases={}, blocks=0):
    return pl.pallas_call(
        body,
        in_specs=list(ins),
        out_specs=[VM] * len(outs),
        out_shape=[jax.ShapeDtypeStruct(shape, kind) for shape, kind in outs],
        scratch_shapes=list(scratch),
        compiler_params=pltpu.CompilerParams(vmem_limit_bytes=limit * 2**20),
        input_output_aliases=aliases,
        cost_estimate=pl.CostEstimate(
            flops=blocks * CLIPS * ROWS * C * C * 8, transcendentals=0, bytes_accessed=0
        ),
    )


def run_block(src, dst, taps, out_weight, half_gain):
    frames = [
        src[:, f * FRAME : (f + 1) * FRAME, :].reshape(CLIPS * FRAME, C) for f in range(FRAMES)
    ]
    normed = []
    for v in frames:
        w = v.astype(jnp.float32)
        mean = jnp.mean(w * w, axis=-1, keepdims=True)
        normed.append((w * lax.rsqrt(mean + EPS) * half_gain).astype(jnp.bfloat16))
    first = jnp.dot(normed[0], taps(C), preferred_element_type=jnp.float32)
    second = jnp.dot(
        jnp.concatenate([normed[1], normed[0]], axis=1),
        taps(2 * C),
        preferred_element_type=jnp.float32,
    )
    rest = jnp.concatenate(
        [
            jnp.concatenate([normed[f], normed[f - 1], normed[f - 2]], axis=1)
            for f in range(2, FRAMES)
        ],
        axis=0,
    )
    third = jnp.dot(rest, taps(3 * C), preferred_element_type=jnp.float32)
    h = jnp.concatenate([first, second, third], axis=0)
    activated = (h + h * jnp.tanh(h)).astype(jnp.bfloat16)
    update = jnp.dot(activated, out_weight(), preferred_element_type=jnp.float32)
    for f in range(FRAMES):
        part = update[f * CLIPS * FRAME : (f + 1) * CLIPS * FRAME]
        dst[:, f * FRAME : (f + 1) * FRAME, :] = (
            (frames[f].astype(jnp.float32) + part)
            .astype(jnp.bfloat16)
            .reshape(CLIPS, FRAME, C)
        )


def prep_body(taps, out_weight, gain_hbm, piece, second, gain, sems):
    core = lax.axis_index("dp_2")
    gain_copy = pltpu.make_async_copy(gain_hbm, gain, sems.at[10])
    gain_copy.start()

    own = 2 * lax.rem(lax.axis_index("dp_0"), 2) + lax.rem(lax.axis_index("dp_1"), 2)

    def copies(target, colour, at):
        lanes = pl.ds(pl.multiple_of(colour * 128, 128), 128)
        lower = [
            pltpu.make_async_copy(
                taps.at[pl.ds(0, HALF), lanes], target.at[pl.ds(0, HALF)], sems.at[at]
            )
        ]
        upper = [
            pltpu.make_async_copy(
                taps.at[pl.ds(HALF, 512), lanes], target.at[pl.ds(0, 512)], sems.at[at]
            )
        ]
        for j in range(4):
            upper.append(
                pltpu.make_async_copy(
                    out_weight.at[lanes, pl.ds(128 * j, 128)],
                    target.at[pl.ds(512 + 128 * j, 128)],
                    sems.at[at + 1 + j],
                )
            )
        return lower, upper

    sets = [copies(piece, own, 0), copies(second, 3 - own, 5)]
    for side in range(2):

        @pl.when(core == side)
        def _(side=side):
            chosen = sets[0][side] + sets[1][side]
            for copy in chosen:
                copy.start()
            for copy in chosen:
                copy.wait()

    gain_copy.wait()
    wide = gain[...].astype(jnp.float32)
    rows = [wide[:, 128 * j : 128 * (j + 1)] for j in range(4)]
    rows.append(jnp.zeros((12, 128), jnp.float32))
    piece[HALF:, :] = jnp.concatenate(rows, axis=0).astype(jnp.bfloat16)


def batch_of(t):
    section = lax.axis_index("section")
    batch = jnp.int32(0)
    for k in range(4):
        if CHUNKS[k][t] is not None:
            batch = jnp.where(section == k, CHUNKS[k][t], batch)
    return batch


def has_chunk(t, sections):
    section = lax.axis_index("section")
    found = [section == k for k in sections if CHUNKS[k][t] is not None]
    return functools.reduce(jnp.logical_or, found)


def start_body(
    steps, pool, index_hbm, taps, out_weight, gain_hbm, qwt_hbm, qbias_hbm, postw_hbm,
    v, all_taps, all_out, all_gain, qw, qb, post,
    index, gain, qwt, qbias, postw, sems,
):
    own = lax.rem(lax.axis_index("section"), 2)
    pairs = [
        (index_hbm, index),
        (taps, all_taps.at[own]),
        (out_weight, all_out.at[own]),
        (gain_hbm, gain),
        (qwt_hbm, qwt),
        (qbias_hbm, qbias),
        (postw_hbm, postw),
    ]
    small = [pltpu.make_async_copy(a, b, sems.at[k]) for k, (a, b) in enumerate(pairs)]
    for copy in small:
        copy.start()
    small[0].wait()
    copies = []
    for t in range(STEPS):
        batch = batch_of(t)
        for c in range(CLIPS):
            copy = pltpu.make_async_copy(
                pool.at[index[c, batch]], v.at[t, c], sems.at[len(pairs) + t * CLIPS + c]
            )
            copy.start()
            copies.append(copy)
    for copy in small[1:]:
        copy.wait()
    all_gain[own] = jnp.broadcast_to(0.5 * gain[...].astype(jnp.float32), (8, C))
    wide = jnp.concatenate(
        [qwt[...].astype(jnp.float32), jnp.zeros((128 - BITS, C), jnp.float32)], axis=0
    )
    qw[...] = wide.T.astype(jnp.bfloat16)
    qb[...] = jnp.zeros((8, 128), jnp.float32)
    qb[0:1, 0:BITS] = qbias[...]
    post[...] = jnp.zeros((CODE_ROWS, C), jnp.bfloat16)
    post[0:BITS, :] = postw[...]
    for copy in copies[: steps * CLIPS]:
        copy.wait()
    first_block(0, steps, v, all_taps, all_out, all_gain)
    for copy in copies[steps * CLIPS :]:
        copy.wait()


def first_block(begin, end, v, all_taps, all_out, all_gain):
    @pl.when(lax.axis_index("section") == 0)
    def _():
        def step(t, _):
            block_at(0, v.at[t], all_taps, all_out, all_gain)
            return 0

        lax.fori_loop(begin, end, step, 0)


def more_body(begin, end, before, all_taps, all_out, all_gain, v):
    first_block(begin, end, v, all_taps, all_out, all_gain)


def join_body(*refs):
    pieces, (all_taps, all_out, all_gain), sems = refs[:8], refs[11:14], refs[14]
    section = lax.axis_index("section")
    core = lax.axis_index("dp_2")
    other = 1 - lax.rem(section, 2)

    def place(lower, upper):
        copies = []
        for j in range(4):
            lanes = pl.ds(128 * j, 128)
            copies.append(
                pltpu.make_async_copy(
                    lower[j].at[pl.ds(0, HALF)],
                    all_taps.at[other, pl.ds(0, HALF), lanes],
                    sems.at[j],
                )
            )
            copies.append(
                pltpu.make_async_copy(
                    upper[j].at[pl.ds(0, 512)],
                    all_taps.at[other, pl.ds(HALF, 512), lanes],
                    sems.at[4 + j],
                )
            )
            for k in range(4):
                copies.append(
                    pltpu.make_async_copy(
                        upper[j].at[pl.ds(512 + 128 * k, 128)],
                        all_out.at[other, pl.ds(128 * j, 128), pl.ds(128 * k, 128)],
                        sems.at[8 + 4 * j + k],
                    )
                )
        for copy in copies:
            copy.start()
        for copy in copies:
            copy.wait()

    @pl.when(core == 0)
    def _():
        place(pieces[:4], pieces[4:])

    @pl.when(core == 1)
    def _():
        place(pieces[4:], pieces[:4])

    rows = pieces[0][HALF:, :].astype(jnp.float32)
    row = jnp.concatenate([rows[k : k + 1, :] for k in range(4)], axis=1)
    all_gain[other] = jnp.broadcast_to(0.5 * row, (8, C))


def block_at(b, buf, all_taps, all_out, all_gain):
    run_block(
        buf,
        buf,
        lambda k: all_taps[b, :k, :],
        lambda: all_out[b],
        all_gain[b, 0:1, :],
    )


def encode_body(steps, last, v_in, all_taps, all_out, all_gain, qw, qb, *rest):
    section = lax.axis_index("section")
    v, codes, stats, sums = rest[-4:]
    sums[...] = rest[0][...] if len(rest) > 4 else jnp.zeros_like(sums)
    n = len(steps)
    span = CLIPS * ROWS

    def blocks(t):
        def step(b, _):
            block_at(b, v.at[t], all_taps, all_out, all_gain)
            return 0

        lax.fori_loop(1 - section, 2, step, 0)

    def quantize():
        row = lax.broadcasted_iota(jnp.int32, (CODE_ROWS, n * span), 0)
        top = lax.broadcasted_iota(jnp.int32, (CODE_ROWS, 128), 0)
        lane = lax.broadcasted_iota(jnp.int32, (CODE_ROWS, 128), 1)
        rows = v[steps[0] : steps[0] + n].reshape(n * span, C)
        logits = jnp.dot(rows, qw[...], preferred_element_type=jnp.float32)
        z = (4.0 * (logits + qb[0:1, :])).T[:CODE_ROWS]
        size = jnp.abs(z)
        e = jnp.exp(-size)
        r = 1.0 / (1.0 + e)
        valid = row < BITS
        p = jnp.where(valid, jnp.where(z >= 0, r, e * r), 0.0)
        entropy = jnp.where(valid, jnp.log1p(e) + size * (e * r), 0.0)
        code = jnp.where(valid, 2.0 * p - 1.0, 0.0).astype(jnp.bfloat16)
        added = jnp.zeros((CODE_ROWS, 128), jnp.float32)
        for i, t in enumerate(steps):
            at = slice(i * span, (i + 1) * span)
            codes[i] = code[:, at]
            bit_sums = jnp.sum(p[:, at], axis=1, keepdims=True)
            total = jnp.sum(
                jnp.sum(entropy[:, at], axis=0, keepdims=True), axis=1, keepdims=True
            )
            column = jnp.where(top == BITS, total, bit_sums)
            batch = jnp.where(has_chunk(t, (0, 1)), batch_of(t), -1)
            added = added + jnp.where(lane == batch, column, 0.0)
        sums[...] += added

    for t in steps:
        pl.when(has_chunk(t, (0, 1)))(functools.partial(blocks, t))
    active = functools.reduce(jnp.logical_or, [has_chunk(t, (0, 1)) for t in steps])
    pl.when(active)(quantize)

    if last:
        full = jnp.concatenate([sums[...], jnp.zeros((128 - CODE_ROWS, 128), jnp.float32)], axis=0)
        stats[...] = full.T[:8]
    else:
        stats[...] = sums[...]


def decode_body(steps, v, all_taps, all_out, all_gain, post, codes, errors, buf):
    def chunk(i, t):
        quantized = lax.dot_general(
            codes[i], post[...], (((0,), (0,)), ((), ())), preferred_element_type=jnp.float32
        )
        buf[...] = quantized.astype(jnp.bfloat16).reshape(CLIPS, ROWS, C)

        def step(b, _):
            block_at(b, buf, all_taps, all_out, all_gain)
            return 0

        lax.fori_loop(0, 2, step, 0)
        for c in range(CLIPS):
            differ = buf[c].astype(jnp.float32) - v[t, c].astype(jnp.float32)
            square = differ * differ
            part = (
                square[:, :128] + square[:, 128:256] + square[:, 256:384] + square[:, 384:]
            )
            mean = jnp.sum(part.T, axis=0, keepdims=True) * (1.0 / C)
            errors[i, 2 * c : 2 * c + 1, :] = mean[:, :128]
            errors[i, 2 * c + 1 : 2 * c + 2, :] = mean[:, 128:]

    for i, t in enumerate(steps):
        pl.when(has_chunk(t, (2, 3)))(functools.partial(chunk, i, t))


def unpack(target, source):
    for c in range(CLIPS):
        row = source[2 * c : 2 * c + 2, :]
        target[c : c + 1, :] = jnp.concatenate([row[0:1], row[1:2]], axis=1)


def final_body(rows_total, order, mine, cross, e0, e34, error, loss):
    section = lax.axis_index("section")
    sums = jnp.where(section <= 1, mine[0:8], cross[0:8]) * (1.0 / rows_total)
    row = lax.broadcasted_iota(jnp.int32, sums.shape, 0)
    lane = lax.broadcasted_iota(jnp.int32, sums.shape, 1)
    averaged = jnp.zeros_like(sums)
    running = None
    for t in range(8):
        here = row == order[t]
        marginal = jnp.sum(jnp.where(here, sums, 0.0), axis=0, keepdims=True)
        running = marginal if t == 0 else 0.5 * running + 0.5 * marginal
        averaged = jnp.where(here, running, averaged)
    smoothed = jnp.where(lane < BITS, 0.05 + 0.9 * averaged, 0.5)
    term = smoothed * jnp.log(smoothed) + (1.0 - smoothed) * jnp.log(1.0 - smoothed)
    term = jnp.where(lane < BITS, term, jnp.where(lane == BITS, sums, 0.0))
    result = jnp.sum(term, axis=1, keepdims=True)
    flat = jnp.sum(jnp.where(row == lane, result, 0.0), axis=0)
    loss[...] = flat[:8]

    @pl.when(section <= 1)
    def _():
        unpack(error.at[0], cross.at[pl.ds(8, 8)])
        unpack(error.at[1], cross.at[pl.ds(16, 8)])

    @pl.when(section == 2)
    def _():
        unpack(error.at[0], e0.at[0])
        unpack(error.at[1], e34.at[0])

    @pl.when(section == 3)
    def _():
        unpack(error.at[0], e34.at[0])
        unpack(error.at[1], e34.at[1])


PAIR = ((0, 1), (1, 0), (2, 3), (3, 2))
CROSS = ((0, 3), (3, 0), (1, 2), (2, 1))
FAR = ((0, 2), (2, 0), (1, 3), (3, 1))


def shifted(x, axis, by):
    n = lax.axis_size(axis)
    return lax.ppermute(x, axis, [(i, (i + by) % n) for i in range(n)])


def within_corner(x, first):
    n, m = lax.axis_size("dp_0"), lax.axis_size("dp_1")
    pairs = []
    for i in range(n):
        for j in range(m):
            for core in range(2):
                to = (i ^ 1, j) if (core == 0) == first else (i, j ^ 1)
                pairs.append(((i * m + j) * 2 + core, (to[0] * m + to[1]) * 2 + core))
    return lax.ppermute(x, DP, pairs)


def encoder_sum(x):
    n = lax.axis_size(DP)
    x = x + lax.ppermute(x, "section", PAIR)
    return jnp.sum(lax.all_to_all(jnp.broadcast_to(x[None], (n, *x.shape)), DP, 0, 0), axis=0)


def on_device(pool, index, order, taps, out_weight, gain, quant_weight, quant_bias, post_weight):
    bf16, f32 = jnp.bfloat16, jnp.float32
    taps = taps.reshape(3 * C, C)
    out_weight = out_weight.reshape(C, C)
    dma = pltpu.SemaphoreType.DMA
    index = index.T
    encoder = (lax.axis_index("section") <= 1).astype(jnp.int32)
    gain, encoder = lax.optimization_barrier((gain, encoder))
    chunk = (CLIPS, ROWS, C)
    kinds = [((2, 3 * C, C), bf16), ((2, C, C), bf16), ((2, 8, C), f32)]

    pool, taps, out_weight = (
        pltpu.with_memory_space_constraint(x, pltpu.HBM) for x in (pool, taps, out_weight)
    )
    gain, qwt, post_weight, index = (
        pltpu.with_memory_space_constraint(x, pltpu.HBM)
        for x in (gain, quant_weight.T, post_weight, index)
    )
    qbias = pltpu.with_memory_space_constraint(quant_bias.reshape(1, BITS), pltpu.HBM)
    piece, second = call(
        prep_body,
        [HB] * 3,
        [((PIECE, 128), bf16), ((HALF, 128), bf16)],
        [pltpu.VMEM((1, C), bf16), dma((11,))],
    )(taps, out_weight, gain)
    mine = lax.ppermute(piece, "section", PAIR)
    second = lax.ppermute(second, "section", PAIR)
    v_kind = ((STEPS, *chunk), bf16)
    v, *weights, qw, qb, post = call(
        functools.partial(start_body, 2),
        [HB] * 8,
        [v_kind, *kinds, ((C, 128), bf16), ((8, 128), f32), ((CODE_ROWS, C), bf16)],
        [
            pltpu.SMEM(index.shape, jnp.int32),
            pltpu.VMEM((1, C), bf16),
            pltpu.VMEM((BITS, C), bf16),
            pltpu.VMEM((1, BITS), f32),
            pltpu.VMEM((BITS, C), bf16),
            dma((7 + STEPS * CLIPS,)),
        ],
        blocks=2,
    )(pool, index, taps, out_weight, gain, qwt, qbias, post_weight)
    mine, v = lax.optimization_barrier((mine, v))
    up = within_corner(mine, True)
    down = within_corner(mine, False)
    mine_s = shifted(mine, "dp_2", 1)
    (v,) = call(
        functools.partial(more_body, 2, STEPS), [VM] * 4, [v_kind], blocks=3, aliases={0: 0}
    )(v, *weights)
    up, down, second, mine_s, v = lax.optimization_barrier((up, down, second, mine_s, v))
    swapped = [mine_s] + [shifted(x, "dp_2", 1) for x in (second, down, up)]
    weights = call(
        join_body, [VM] + [ANY] * 7 + [VM] * 3, kinds, [dma((24,))], aliases={8: 0, 9: 1, 10: 2}
    )(mine, second, up, down, *swapped, *weights)

    def encode(steps, v, before, last):
        n = len(steps)
        return call(
            functools.partial(encode_body, steps, last),
            [VM] * (6 + len(before)),
            [
                v_kind,
                ((n, CODE_ROWS, CLIPS * ROWS), bf16),
                ((8 if last else CODE_ROWS, 128), f32),
            ],
            [pltpu.VMEM((CODE_ROWS, 128), f32)],
            blocks=2 * n,
            aliases={0: 0},
        )(v, *weights, qw, qb, *before)

    def decode(steps, v, codes):
        n = len(steps)
        return call(
            functools.partial(decode_body, steps),
            [VM] * 6,
            [((n, 8, 128), f32)],
            [pltpu.VMEM(chunk, bf16)],
            blocks=2 * n,
        )(v, *weights, post, codes)[0]

    v, codes, stats = encode((0,), v, (), False)
    codes_a = lax.ppermute(codes, "section", FAR)
    v, codes, stats = encode((1, 2), v, (stats,), False)
    e0 = decode((0,), v, codes_a)
    codes, e0, v = lax.optimization_barrier((codes, e0, v))
    codes_b = lax.ppermute(codes, "section", CROSS)
    v, codes, stats = encode((3, 4), v, (stats,), True)
    codes_c = lax.ppermute(codes, "section", ((0, 3), (1, 2)))
    codes_b, stats = lax.optimization_barrier((codes_b, stats))
    e12 = decode((1, 2), v, codes_b)
    codes_c, e12 = lax.optimization_barrier((codes_c, e12))
    e34 = decode((3, 4), v, codes_c)
    stats, e12, e34, encoder = lax.optimization_barrier((stats, e12, e34, encoder))
    total = lax.cond(encoder == 1, encoder_sum, lambda x: 0.0 * x, stats)
    packed = jnp.concatenate([total, e12[0], e12[1]], axis=0)
    cross = lax.ppermute(packed, "section", CROSS)
    rows_total = float(CLIPS * lax.axis_size(DP) * ROWS)
    error, loss = call(
        functools.partial(final_body, rows_total),
        [SM] + [VM] * 4,
        [((2, CLIPS, ROWS), f32), ((8,), f32)],
    )(order, packed, cross, e0, e34)
    return error, loss


def solution(mesh):
    torus = Mesh(
        mesh.devices.reshape(mesh.shape["section"], 4, 4, 2), ("section", "dp_0", "dp_1", "dp_2")
    )
    return jax.shard_map(
        on_device,
        mesh=torus,
        in_specs=(
            P(DP, None, None),
            P(None, DP),
            P(),
            P("section", None, None, None),
            P("section", None, None),
            P("section", None),
            P(),
            P(),
            P(),
        ),
        out_specs=(P("section", DP, None), P()),
        check_vma=False,
    )
```

```python
import functools

import jax
import jax.numpy as jnp
from jax import lax
from jax.experimental import pallas as pl
from jax.experimental.pallas import tpu as pltpu
from jax.sharding import Mesh
from jax.sharding import PartitionSpec as P


DP = ("dp_0", "dp_1", "dp_2")
EPS = 1e-06
C = 512
BITS = 18
FRAME = 64
ROWS = 256
CLIPS = 4
FRAMES = ROWS // FRAME
CHUNKS = ((4, 0, 1, 6, 7), (None, 2, 3, 5, None), (4, 2, 3, 5, None), (None, 0, 1, 6, 7))
STEPS = len(CHUNKS[0])
CODE_ROWS = 24
HALF = 1024
PIECE = HALF + 16
VM = pl.BlockSpec(memory_space=pltpu.VMEM)
SM = pl.BlockSpec(memory_space=pltpu.SMEM)
HB = pl.BlockSpec(memory_space=pltpu.HBM)
ANY = pl.BlockSpec(memory_space=pl.ANY)


def call(body, ins, outs, scratch=(), limit=24, aliases={}, blocks=0):
    return pl.pallas_call(
        body,
        in_specs=list(ins),
        out_specs=[VM] * len(outs),
        out_shape=[jax.ShapeDtypeStruct(shape, kind) for shape, kind in outs],
        scratch_shapes=list(scratch),
        compiler_params=pltpu.CompilerParams(vmem_limit_bytes=limit * 2**20),
        input_output_aliases=aliases,
        cost_estimate=pl.CostEstimate(
            flops=blocks * CLIPS * ROWS * C * C * 8, transcendentals=0, bytes_accessed=0
        ),
    )


def run_block(src, dst, taps, out_weight, half_gain):
    frames = [
        src[:, f * FRAME : (f + 1) * FRAME, :].reshape(CLIPS * FRAME, C) for f in range(FRAMES)
    ]
    normed = []
    for v in frames:
        w = v.astype(jnp.float32)
        mean = jnp.mean(w * w, axis=-1, keepdims=True)
        normed.append((w * lax.rsqrt(mean + EPS) * half_gain).astype(jnp.bfloat16))
    first = jnp.dot(normed[0], taps(C), preferred_element_type=jnp.float32)
    second = jnp.dot(
        jnp.concatenate([normed[1], normed[0]], axis=1),
        taps(2 * C),
        preferred_element_type=jnp.float32,
    )
    rest = jnp.concatenate(
        [
            jnp.concatenate([normed[f], normed[f - 1], normed[f - 2]], axis=1)
            for f in range(2, FRAMES)
        ],
        axis=0,
    )
    third = jnp.dot(rest, taps(3 * C), preferred_element_type=jnp.float32)
    h = jnp.concatenate([first, second, third], axis=0)
    activated = (h + h * jnp.tanh(h)).astype(jnp.bfloat16)
    update = jnp.dot(activated, out_weight(), preferred_element_type=jnp.float32)
    for f in range(FRAMES):
        part = update[f * CLIPS * FRAME : (f + 1) * CLIPS * FRAME]
        dst[:, f * FRAME : (f + 1) * FRAME, :] = (
            (frames[f].astype(jnp.float32) + part)
            .astype(jnp.bfloat16)
            .reshape(CLIPS, FRAME, C)
        )


def prep_body(taps, out_weight, gain_hbm, piece, second, gain, sems):
    core = lax.axis_index("dp_2")
    gain_copy = pltpu.make_async_copy(gain_hbm, gain, sems.at[10])
    gain_copy.start()

    own = 2 * lax.rem(lax.axis_index("dp_0"), 2) + lax.rem(lax.axis_index("dp_1"), 2)

    def copies(target, colour, at):
        lanes = pl.ds(pl.multiple_of(colour * 128, 128), 128)
        lower = [
            pltpu.make_async_copy(
                taps.at[pl.ds(0, HALF), lanes], target.at[pl.ds(0, HALF)], sems.at[at]
            )
        ]
        upper = [
            pltpu.make_async_copy(
                taps.at[pl.ds(HALF, 512), lanes], target.at[pl.ds(0, 512)], sems.at[at]
            )
        ]
        for j in range(4):
            upper.append(
                pltpu.make_async_copy(
                    out_weight.at[lanes, pl.ds(128 * j, 128)],
                    target.at[pl.ds(512 + 128 * j, 128)],
                    sems.at[at + 1 + j],
                )
            )
        return lower, upper

    sets = [copies(piece, own, 0), copies(second, 3 - own, 5)]
    for side in range(2):

        @pl.when(core == side)
        def _(side=side):
            chosen = sets[0][side] + sets[1][side]
            for copy in chosen:
                copy.start()
            for copy in chosen:
                copy.wait()

    gain_copy.wait()
    wide = gain[...].astype(jnp.float32)
    rows = [wide[:, 128 * j : 128 * (j + 1)] for j in range(4)]
    rows.append(jnp.zeros((12, 128), jnp.float32))
    piece[HALF:, :] = jnp.concatenate(rows, axis=0).astype(jnp.bfloat16)


def batch_of(t):
    section = lax.axis_index("section")
    batch = jnp.int32(0)
    for k in range(4):
        if CHUNKS[k][t] is not None:
            batch = jnp.where(section == k, CHUNKS[k][t], batch)
    return batch


def has_chunk(t, sections):
    section = lax.axis_index("section")
    found = [section == k for k in sections if CHUNKS[k][t] is not None]
    return functools.reduce(jnp.logical_or, found)


def start_body(
    steps, pool, index_hbm, taps, out_weight, gain_hbm, qwt_hbm, qbias_hbm, postw_hbm,
    v, all_taps, all_out, all_gain, qw, qb, post,
    index, gain, qwt, qbias, postw, sems,
):
    own = lax.rem(lax.axis_index("section"), 2)
    pairs = [
        (index_hbm, index),
        (taps, all_taps.at[own]),
        (out_weight, all_out.at[own]),
        (gain_hbm, gain),
        (qwt_hbm, qwt),
        (qbias_hbm, qbias),
        (postw_hbm, postw),
    ]
    small = [pltpu.make_async_copy(a, b, sems.at[k]) for k, (a, b) in enumerate(pairs)]
    for copy in small:
        copy.start()
    small[0].wait()
    copies = []
    for t in range(STEPS):
        batch = batch_of(t)
        for c in range(CLIPS):
            copy = pltpu.make_async_copy(
                pool.at[index[c, batch]], v.at[t, c], sems.at[len(pairs) + t * CLIPS + c]
            )
            copy.start()
            copies.append(copy)
    for copy in small[1:]:
        copy.wait()
    all_gain[own] = jnp.broadcast_to(0.5 * gain[...].astype(jnp.float32), (8, C))
    wide = jnp.concatenate(
        [qwt[...].astype(jnp.float32), jnp.zeros((128 - BITS, C), jnp.float32)], axis=0
    )
    qw[...] = wide.T.astype(jnp.bfloat16)
    qb[...] = jnp.zeros((8, 128), jnp.float32)
    qb[0:1, 0:BITS] = qbias[...]
    post[...] = jnp.zeros((CODE_ROWS, C), jnp.bfloat16)
    post[0:BITS, :] = postw[...]
    for copy in copies[: steps * CLIPS]:
        copy.wait()
    first_block(0, steps, v, all_taps, all_out, all_gain)
    for copy in copies[steps * CLIPS :]:
        copy.wait()


def first_block(begin, end, v, all_taps, all_out, all_gain):
    @pl.when(lax.axis_index("section") == 0)
    def _():
        def step(t, _):
            block_at(0, v.at[t], all_taps, all_out, all_gain)
            return 0

        lax.fori_loop(begin, end, step, 0)


def more_body(begin, end, before, all_taps, all_out, all_gain, v):
    first_block(begin, end, v, all_taps, all_out, all_gain)


def join_body(*refs):
    pieces, (all_taps, all_out, all_gain), sems = refs[:8], refs[11:14], refs[14]
    section = lax.axis_index("section")
    core = lax.axis_index("dp_2")
    other = 1 - lax.rem(section, 2)

    def place(lower, upper):
        copies = []
        for j in range(4):
            lanes = pl.ds(128 * j, 128)
            copies.append(
                pltpu.make_async_copy(
                    lower[j].at[pl.ds(0, HALF)],
                    all_taps.at[other, pl.ds(0, HALF), lanes],
                    sems.at[j],
                )
            )
            copies.append(
                pltpu.make_async_copy(
                    upper[j].at[pl.ds(0, 512)],
                    all_taps.at[other, pl.ds(HALF, 512), lanes],
                    sems.at[4 + j],
                )
            )
            for k in range(4):
                copies.append(
                    pltpu.make_async_copy(
                        upper[j].at[pl.ds(512 + 128 * k, 128)],
                        all_out.at[other, pl.ds(128 * j, 128), pl.ds(128 * k, 128)],
                        sems.at[8 + 4 * j + k],
                    )
                )
        for copy in copies:
            copy.start()
        for copy in copies:
            copy.wait()

    @pl.when(core == 0)
    def _():
        place(pieces[:4], pieces[4:])

    @pl.when(core == 1)
    def _():
        place(pieces[4:], pieces[:4])

    rows = pieces[0][HALF:, :].astype(jnp.float32)
    row = jnp.concatenate([rows[k : k + 1, :] for k in range(4)], axis=1)
    all_gain[other] = jnp.broadcast_to(0.5 * row, (8, C))


def block_at(b, buf, all_taps, all_out, all_gain):
    run_block(
        buf,
        buf,
        lambda k: all_taps[b, :k, :],
        lambda: all_out[b],
        all_gain[b, 0:1, :],
    )


def encode_body(steps, last, v_in, all_taps, all_out, all_gain, qw, qb, *rest):
    section = lax.axis_index("section")
    v, codes, stats, sums = rest[-4:]
    sums[...] = rest[0][...] if len(rest) > 4 else jnp.zeros_like(sums)
    n = len(steps)
    span = CLIPS * ROWS

    def blocks(t):
        def step(b, _):
            block_at(b, v.at[t], all_taps, all_out, all_gain)
            return 0

        lax.fori_loop(1 - section, 2, step, 0)

    def quantize():
        row = lax.broadcasted_iota(jnp.int32, (CODE_ROWS, n * span), 0)
        top = lax.broadcasted_iota(jnp.int32, (CODE_ROWS, 128), 0)
        lane = lax.broadcasted_iota(jnp.int32, (CODE_ROWS, 128), 1)
        rows = v[steps[0] : steps[0] + n].reshape(n * span, C)
        logits = jnp.dot(rows, qw[...], preferred_element_type=jnp.float32)
        z = (4.0 * (logits + qb[0:1, :])).T[:CODE_ROWS]
        size = jnp.abs(z)
        e = jnp.exp(-size)
        r = 1.0 / (1.0 + e)
        valid = row < BITS
        p = jnp.where(valid, jnp.where(z >= 0, r, e * r), 0.0)
        entropy = jnp.where(valid, jnp.log1p(e) + size * (e * r), 0.0)
        code = jnp.where(valid, 2.0 * p - 1.0, 0.0).astype(jnp.bfloat16)
        added = jnp.zeros((CODE_ROWS, 128), jnp.float32)
        for i, t in enumerate(steps):
            at = slice(i * span, (i + 1) * span)
            codes[i] = code[:, at]
            bit_sums = jnp.sum(p[:, at], axis=1, keepdims=True)
            total = jnp.sum(
                jnp.sum(entropy[:, at], axis=0, keepdims=True), axis=1, keepdims=True
            )
            column = jnp.where(top == BITS, total, bit_sums)
            batch = jnp.where(has_chunk(t, (0, 1)), batch_of(t), -1)
            added = added + jnp.where(lane == batch, column, 0.0)
        sums[...] += added

    for t in steps:
        pl.when(has_chunk(t, (0, 1)))(functools.partial(blocks, t))
    active = functools.reduce(jnp.logical_or, [has_chunk(t, (0, 1)) for t in steps])
    pl.when(active)(quantize)

    if last:
        full = jnp.concatenate([sums[...], jnp.zeros((128 - CODE_ROWS, 128), jnp.float32)], axis=0)
        stats[...] = full.T[:8]
    else:
        stats[...] = sums[...]


def decode_body(steps, v, all_taps, all_out, all_gain, post, codes, errors, buf):
    def chunk(i, t):
        quantized = lax.dot_general(
            codes[i], post[...], (((0,), (0,)), ((), ())), preferred_element_type=jnp.float32
        )
        buf[...] = quantized.astype(jnp.bfloat16).reshape(CLIPS, ROWS, C)

        def step(b, _):
            block_at(b, buf, all_taps, all_out, all_gain)
            return 0

        lax.fori_loop(0, 2, step, 0)
        for c in range(CLIPS):
            differ = buf[c].astype(jnp.float32) - v[t, c].astype(jnp.float32)
            square = differ * differ
            part = (
                square[:, :128] + square[:, 128:256] + square[:, 256:384] + square[:, 384:]
            )
            mean = jnp.sum(part.T, axis=0, keepdims=True) * (1.0 / C)
            errors[i, 2 * c : 2 * c + 1, :] = mean[:, :128]
            errors[i, 2 * c + 1 : 2 * c + 2, :] = mean[:, 128:]

    for i, t in enumerate(steps):
        pl.when(has_chunk(t, (2, 3)))(functools.partial(chunk, i, t))


def unpack(target, source):
    for c in range(CLIPS):
        row = source[2 * c : 2 * c + 2, :]
        target[c : c + 1, :] = jnp.concatenate([row[0:1], row[1:2]], axis=1)


def final_body(rows_total, order, mine, cross, given, e0, e34, error, loss):
    section = lax.axis_index("section")
    sums = jnp.where(section <= 1, mine[...], cross[...]) * (1.0 / rows_total)
    row = lax.broadcasted_iota(jnp.int32, sums.shape, 0)
    lane = lax.broadcasted_iota(jnp.int32, sums.shape, 1)
    averaged = jnp.zeros_like(sums)
    running = None
    for t in range(8):
        here = row == order[t]
        marginal = jnp.sum(jnp.where(here, sums, 0.0), axis=0, keepdims=True)
        running = marginal if t == 0 else 0.5 * running + 0.5 * marginal
        averaged = jnp.where(here, running, averaged)
    smoothed = jnp.where(lane < BITS, 0.05 + 0.9 * averaged, 0.5)
    term = smoothed * jnp.log(smoothed) + (1.0 - smoothed) * jnp.log(1.0 - smoothed)
    term = jnp.where(lane < BITS, term, jnp.where(lane == BITS, sums, 0.0))
    result = jnp.sum(term, axis=1, keepdims=True)
    flat = jnp.sum(jnp.where(row == lane, result, 0.0), axis=0)
    loss[...] = flat[:8]

    @pl.when(section <= 1)
    def _():
        unpack(error.at[0], given.at[0])
        unpack(error.at[1], given.at[1])

    @pl.when(section == 2)
    def _():
        unpack(error.at[0], e0.at[0])
        unpack(error.at[1], e34.at[0])

    @pl.when(section == 3)
    def _():
        unpack(error.at[0], e34.at[0])
        unpack(error.at[1], e34.at[1])


PAIR = ((0, 1), (1, 0), (2, 3), (3, 2))
CROSS = ((0, 3), (3, 0), (1, 2), (2, 1))


def shifted(x, axis, by):
    n = lax.axis_size(axis)
    return lax.ppermute(x, axis, [(i, (i + by) % n) for i in range(n)])


def within_corner(x, first):
    n, m = lax.axis_size("dp_0"), lax.axis_size("dp_1")
    pairs = []
    for i in range(n):
        for j in range(m):
            for core in range(2):
                to = (i ^ 1, j) if (core == 0) == first else (i, j ^ 1)
                pairs.append(((i * m + j) * 2 + core, (to[0] * m + to[1]) * 2 + core))
    return lax.ppermute(x, DP, pairs)


def encoder_sum(x):
    n = lax.axis_size(DP)
    x = x + lax.ppermute(x, "section", PAIR)
    return jnp.sum(lax.all_to_all(jnp.broadcast_to(x[None], (n, *x.shape)), DP, 0, 0), axis=0)


def on_device(pool, index, order, taps, out_weight, gain, quant_weight, quant_bias, post_weight):
    bf16, f32 = jnp.bfloat16, jnp.float32
    taps = taps.reshape(3 * C, C)
    out_weight = out_weight.reshape(C, C)
    dma = pltpu.SemaphoreType.DMA
    index = index.T
    encoder = (lax.axis_index("section") <= 1).astype(jnp.int32)
    gain, encoder = lax.optimization_barrier((gain, encoder))
    chunk = (CLIPS, ROWS, C)
    kinds = [((2, 3 * C, C), bf16), ((2, C, C), bf16), ((2, 8, C), f32)]

    pool, taps, out_weight = (
        pltpu.with_memory_space_constraint(x, pltpu.HBM) for x in (pool, taps, out_weight)
    )
    gain, qwt, post_weight, index = (
        pltpu.with_memory_space_constraint(x, pltpu.HBM)
        for x in (gain, quant_weight.T, post_weight, index)
    )
    qbias = pltpu.with_memory_space_constraint(quant_bias.reshape(1, BITS), pltpu.HBM)
    piece, second = call(
        prep_body,
        [HB] * 3,
        [((PIECE, 128), bf16), ((HALF, 128), bf16)],
        [pltpu.VMEM((1, C), bf16), dma((11,))],
    )(taps, out_weight, gain)
    mine = lax.ppermute(piece, "section", PAIR)
    second = lax.ppermute(second, "section", PAIR)
    v_kind = ((STEPS, *chunk), bf16)
    v, *weights, qw, qb, post = call(
        functools.partial(start_body, 2),
        [HB] * 8,
        [v_kind, *kinds, ((C, 128), bf16), ((8, 128), f32), ((CODE_ROWS, C), bf16)],
        [
            pltpu.SMEM(index.shape, jnp.int32),
            pltpu.VMEM((1, C), bf16),
            pltpu.VMEM((BITS, C), bf16),
            pltpu.VMEM((1, BITS), f32),
            pltpu.VMEM((BITS, C), bf16),
            dma((7 + STEPS * CLIPS,)),
        ],
        blocks=2,
    )(pool, index, taps, out_weight, gain, qwt, qbias, post_weight)
    mine, v = lax.optimization_barrier((mine, v))
    up = within_corner(mine, True)
    down = within_corner(mine, False)
    mine_s = shifted(mine, "dp_2", 1)
    (v,) = call(
        functools.partial(more_body, 2, STEPS), [VM] * 4, [v_kind], blocks=3, aliases={0: 0}
    )(v, *weights)
    up, down, second, mine_s, v = lax.optimization_barrier((up, down, second, mine_s, v))
    swapped = [mine_s] + [shifted(x, "dp_2", 1) for x in (second, down, up)]
    weights = call(
        join_body, [VM] + [ANY] * 7 + [VM] * 3, kinds, [dma((24,))], aliases={8: 0, 9: 1, 10: 2}
    )(mine, second, up, down, *swapped, *weights)

    def encode(steps, v, before, last):
        n = len(steps)
        return call(
            functools.partial(encode_body, steps, last),
            [VM] * (6 + len(before)),
            [
                v_kind,
                ((n, CODE_ROWS, CLIPS * ROWS), bf16),
                ((8 if last else CODE_ROWS, 128), f32),
            ],
            [pltpu.VMEM((CODE_ROWS, 128), f32)],
            blocks=2 * n,
            aliases={0: 0},
        )(v, *weights, qw, qb, *before)

    def decode(steps, v, codes):
        n = len(steps)
        return call(
            functools.partial(decode_body, steps),
            [VM] * 6,
            [((n, 8, 128), f32)],
            [pltpu.VMEM(chunk, bf16)],
            blocks=2 * n,
        )(v, *weights, post, codes)[0]

    v, codes, stats = encode((0,), v, (), False)
    codes_a = lax.ppermute(codes, "section", ((0, 2),))
    v, codes, stats = encode((1, 2), v, (stats,), False)
    codes_b = lax.ppermute(codes, "section", CROSS)
    v, codes, stats = encode((3, 4), v, (stats,), True)
    codes_c = lax.ppermute(codes, "section", ((0, 3), (1, 2)))
    codes_a, stats = lax.optimization_barrier((codes_a, stats))
    e0 = decode((0,), v, codes_a)
    codes_b, e0 = lax.optimization_barrier((codes_b, e0))
    e12 = decode((1, 2), v, codes_b)
    given = lax.ppermute(e12, "section", ((3, 0), (2, 1)))
    e34 = decode((3, 4), v, codes_c)
    stats, e34, encoder = lax.optimization_barrier((stats, e34, encoder))
    total = lax.cond(encoder == 1, encoder_sum, lambda x: 0.0 * x, stats)
    cross = lax.ppermute(total, "section", ((0, 3), (1, 2)))
    rows_total = float(CLIPS * lax.axis_size(DP) * ROWS)
    error, loss = call(
        functools.partial(final_body, rows_total),
        [SM] + [VM] * 5,
        [((2, CLIPS, ROWS), f32), ((8,), f32)],
    )(order, total, cross, given, e0, e34)
    return error, loss


def solution(mesh):
    torus = Mesh(
        mesh.devices.reshape(mesh.shape["section"], 4, 4, 2), ("section", "dp_0", "dp_1", "dp_2")
    )
    return jax.shard_map(
        on_device,
        mesh=torus,
        in_specs=(
            P(DP, None, None),
            P(None, DP),
            P(),
            P("section", None, None, None),
            P("section", None, None),
            P("section", None),
            P(),
            P(),
            P(),
        ),
        out_specs=(P("section", DP, None), P()),
        check_vma=False,
    )
```

```python
import functools

import jax
import jax.numpy as jnp
from jax import lax
from jax.experimental import pallas as pl
from jax.experimental.pallas import tpu as pltpu
from jax.sharding import Mesh
from jax.sharding import PartitionSpec as P


DP = ("dp_0", "dp_1", "dp_2")
EPS = 1e-06
C = 512
BITS = 18
FRAME = 64
ROWS = 256
CLIPS = 4
FRAMES = ROWS // FRAME
CHUNKS = ((4, 0, 1, 6, 7), (None, 2, 3, 5, None), (4, 2, 3, 5, None), (None, 0, 1, 6, 7))
STEPS = len(CHUNKS[0])
CODE_ROWS = 24
HALF = 1024
PIECE = HALF + 16
VM = pl.BlockSpec(memory_space=pltpu.VMEM)
SM = pl.BlockSpec(memory_space=pltpu.SMEM)
HB = pl.BlockSpec(memory_space=pltpu.HBM)
ANY = pl.BlockSpec(memory_space=pl.ANY)


def call(body, ins, outs, scratch=(), limit=24, aliases={}, blocks=0):
    return pl.pallas_call(
        body,
        in_specs=list(ins),
        out_specs=[VM] * len(outs),
        out_shape=[jax.ShapeDtypeStruct(shape, kind) for shape, kind in outs],
        scratch_shapes=list(scratch),
        compiler_params=pltpu.CompilerParams(vmem_limit_bytes=limit * 2**20),
        input_output_aliases=aliases,
        cost_estimate=pl.CostEstimate(
            flops=blocks * CLIPS * ROWS * C * C * 8, transcendentals=0, bytes_accessed=0
        ),
    )


def run_block(src, dst, taps, out_weight, half_gain):
    frames = [
        src[:, f * FRAME : (f + 1) * FRAME, :].reshape(CLIPS * FRAME, C) for f in range(FRAMES)
    ]
    normed = []
    for v in frames:
        w = v.astype(jnp.float32)
        mean = jnp.mean(w * w, axis=-1, keepdims=True)
        normed.append((w * lax.rsqrt(mean + EPS) * half_gain).astype(jnp.bfloat16))
    first = jnp.dot(normed[0], taps(C), preferred_element_type=jnp.float32)
    second = jnp.dot(
        jnp.concatenate([normed[1], normed[0]], axis=1),
        taps(2 * C),
        preferred_element_type=jnp.float32,
    )
    rest = jnp.concatenate(
        [
            jnp.concatenate([normed[f], normed[f - 1], normed[f - 2]], axis=1)
            for f in range(2, FRAMES)
        ],
        axis=0,
    )
    third = jnp.dot(rest, taps(3 * C), preferred_element_type=jnp.float32)
    h = jnp.concatenate([first, second, third], axis=0)
    activated = (h + h * jnp.tanh(h)).astype(jnp.bfloat16)
    update = jnp.dot(activated, out_weight(), preferred_element_type=jnp.float32)
    for f in range(FRAMES):
        part = update[f * CLIPS * FRAME : (f + 1) * CLIPS * FRAME]
        dst[:, f * FRAME : (f + 1) * FRAME, :] = (
            (frames[f].astype(jnp.float32) + part)
            .astype(jnp.bfloat16)
            .reshape(CLIPS, FRAME, C)
        )


def prep_body(taps, out_weight, gain_hbm, piece, second, gain, sems):
    core = lax.axis_index("dp_2")
    gain_copy = pltpu.make_async_copy(gain_hbm, gain, sems.at[10])
    gain_copy.start()

    own = 2 * lax.rem(lax.axis_index("dp_0"), 2) + lax.rem(lax.axis_index("dp_1"), 2)

    def copies(target, colour, at):
        lanes = pl.ds(pl.multiple_of(colour * 128, 128), 128)
        lower = [
            pltpu.make_async_copy(
                taps.at[pl.ds(0, HALF), lanes], target.at[pl.ds(0, HALF)], sems.at[at]
            )
        ]
        upper = [
            pltpu.make_async_copy(
                taps.at[pl.ds(HALF, 512), lanes], target.at[pl.ds(0, 512)], sems.at[at]
            )
        ]
        for j in range(4):
            upper.append(
                pltpu.make_async_copy(
                    out_weight.at[lanes, pl.ds(128 * j, 128)],
                    target.at[pl.ds(512 + 128 * j, 128)],
                    sems.at[at + 1 + j],
                )
            )
        return lower, upper

    sets = [copies(piece, own, 0), copies(second, 3 - own, 5)]
    for side in range(2):

        @pl.when(core == side)
        def _(side=side):
            chosen = sets[0][side] + sets[1][side]
            for copy in chosen:
                copy.start()
            for copy in chosen:
                copy.wait()

    gain_copy.wait()
    wide = gain[...].astype(jnp.float32)
    rows = [wide[:, 128 * j : 128 * (j + 1)] for j in range(4)]
    rows.append(jnp.zeros((12, 128), jnp.float32))
    piece[HALF:, :] = jnp.concatenate(rows, axis=0).astype(jnp.bfloat16)


def batch_of(t):
    section = lax.axis_index("section")
    batch = jnp.int32(0)
    for k in range(4):
        if CHUNKS[k][t] is not None:
            batch = jnp.where(section == k, CHUNKS[k][t], batch)
    return batch


def has_chunk(t, sections):
    section = lax.axis_index("section")
    found = [section == k for k in sections if CHUNKS[k][t] is not None]
    return functools.reduce(jnp.logical_or, found)


def start_body(
    steps, pool, index_hbm, taps, out_weight, gain_hbm, qwt_hbm, qbias_hbm, postw_hbm,
    v, all_taps, all_out, all_gain, qw, qb, post,
    index, gain, qwt, qbias, postw, sems,
):
    own = lax.rem(lax.axis_index("section"), 2)
    pairs = [
        (index_hbm, index),
        (taps, all_taps.at[own]),
        (out_weight, all_out.at[own]),
        (gain_hbm, gain),
        (qwt_hbm, qwt),
        (qbias_hbm, qbias),
        (postw_hbm, postw),
    ]
    small = [pltpu.make_async_copy(a, b, sems.at[k]) for k, (a, b) in enumerate(pairs)]
    for copy in small:
        copy.start()
    small[0].wait()
    copies = []
    for t in range(STEPS):
        batch = batch_of(t)
        for c in range(CLIPS):
            copy = pltpu.make_async_copy(
                pool.at[index[c, batch]], v.at[t, c], sems.at[len(pairs) + t * CLIPS + c]
            )
            copy.start()
            copies.append(copy)
    for copy in small[1:]:
        copy.wait()
    all_gain[own] = jnp.broadcast_to(0.5 * gain[...].astype(jnp.float32), (8, C))
    wide = jnp.concatenate(
        [qwt[...].astype(jnp.float32), jnp.zeros((128 - BITS, C), jnp.float32)], axis=0
    )
    qw[...] = wide.T.astype(jnp.bfloat16)
    qb[...] = jnp.zeros((8, 128), jnp.float32)
    qb[0:1, 0:BITS] = qbias[...]
    post[...] = jnp.zeros((CODE_ROWS, C), jnp.bfloat16)
    post[0:BITS, :] = postw[...]
    for copy in copies[: steps * CLIPS]:
        copy.wait()
    first_block(0, steps, v, all_taps, all_out, all_gain)
    for copy in copies[steps * CLIPS :]:
        copy.wait()


def first_block(begin, end, v, all_taps, all_out, all_gain):
    @pl.when(lax.axis_index("section") == 0)
    def _():
        def step(t, _):
            block_at(0, v.at[t], all_taps, all_out, all_gain)
            return 0

        lax.fori_loop(begin, end, step, 0)


def more_body(begin, end, before, all_taps, all_out, all_gain, v):
    first_block(begin, end, v, all_taps, all_out, all_gain)


def join_body(*refs):
    pieces, (all_taps, all_out, all_gain), sems = refs[:8], refs[11:14], refs[14]
    section = lax.axis_index("section")
    core = lax.axis_index("dp_2")
    other = 1 - lax.rem(section, 2)

    def place(lower, upper):
        copies = []
        for j in range(4):
            lanes = pl.ds(128 * j, 128)
            copies.append(
                pltpu.make_async_copy(
                    lower[j].at[pl.ds(0, HALF)],
                    all_taps.at[other, pl.ds(0, HALF), lanes],
                    sems.at[j],
                )
            )
            copies.append(
                pltpu.make_async_copy(
                    upper[j].at[pl.ds(0, 512)],
                    all_taps.at[other, pl.ds(HALF, 512), lanes],
                    sems.at[4 + j],
                )
            )
            for k in range(4):
                copies.append(
                    pltpu.make_async_copy(
                        upper[j].at[pl.ds(512 + 128 * k, 128)],
                        all_out.at[other, pl.ds(128 * j, 128), pl.ds(128 * k, 128)],
                        sems.at[8 + 4 * j + k],
                    )
                )
        for copy in copies:
            copy.start()
        for copy in copies:
            copy.wait()

    @pl.when(core == 0)
    def _():
        place(pieces[:4], pieces[4:])

    @pl.when(core == 1)
    def _():
        place(pieces[4:], pieces[:4])

    rows = pieces[0][HALF:, :].astype(jnp.float32)
    row = jnp.concatenate([rows[k : k + 1, :] for k in range(4)], axis=1)
    all_gain[other] = jnp.broadcast_to(0.5 * row, (8, C))


def block_at(b, buf, all_taps, all_out, all_gain):
    run_block(
        buf,
        buf,
        lambda k: all_taps[b, :k, :],
        lambda: all_out[b],
        all_gain[b, 0:1, :],
    )


def encode_body(steps, last, v_in, all_taps, all_out, all_gain, qw, qb, *rest):
    section = lax.axis_index("section")
    v, codes, stats, sums = rest[-4:]
    sums[...] = rest[0][...] if len(rest) > 4 else jnp.zeros_like(sums)
    n = len(steps)
    span = CLIPS * ROWS

    def blocks(t):
        def step(b, _):
            block_at(b, v.at[t], all_taps, all_out, all_gain)
            return 0

        lax.fori_loop(1 - section, 2, step, 0)

    def quantize():
        row = lax.broadcasted_iota(jnp.int32, (CODE_ROWS, n * span), 0)
        top = lax.broadcasted_iota(jnp.int32, (CODE_ROWS, 128), 0)
        lane = lax.broadcasted_iota(jnp.int32, (CODE_ROWS, 128), 1)
        rows = v[steps[0] : steps[0] + n].reshape(n * span, C)
        logits = jnp.dot(rows, qw[...], preferred_element_type=jnp.float32)
        z = (4.0 * (logits + qb[0:1, :])).T[:CODE_ROWS]
        size = jnp.abs(z)
        e = jnp.exp(-size)
        r = 1.0 / (1.0 + e)
        valid = row < BITS
        p = jnp.where(valid, jnp.where(z >= 0, r, e * r), 0.0)
        entropy = jnp.where(valid, jnp.log1p(e) + size * (e * r), 0.0)
        code = jnp.where(valid, 2.0 * p - 1.0, 0.0).astype(jnp.bfloat16)
        added = jnp.zeros((CODE_ROWS, 128), jnp.float32)
        for i, t in enumerate(steps):
            at = slice(i * span, (i + 1) * span)
            codes[i] = code[:, at]
            bit_sums = jnp.sum(p[:, at], axis=1, keepdims=True)
            total = jnp.sum(
                jnp.sum(entropy[:, at], axis=0, keepdims=True), axis=1, keepdims=True
            )
            column = jnp.where(top == BITS, total, bit_sums)
            batch = jnp.where(has_chunk(t, (0, 1)), batch_of(t), -1)
            added = added + jnp.where(lane == batch, column, 0.0)
        sums[...] += added

    for t in steps:
        pl.when(has_chunk(t, (0, 1)))(functools.partial(blocks, t))
    active = functools.reduce(jnp.logical_or, [has_chunk(t, (0, 1)) for t in steps])
    pl.when(active)(quantize)

    if last:
        full = jnp.concatenate([sums[...], jnp.zeros((128 - CODE_ROWS, 128), jnp.float32)], axis=0)
        stats[...] = full.T[:8]
    else:
        stats[...] = sums[...]


def decode_body(steps, v, all_taps, all_out, all_gain, post, codes, errors, buf):
    def chunk(i, t):
        quantized = lax.dot_general(
            codes[i], post[...], (((0,), (0,)), ((), ())), preferred_element_type=jnp.float32
        )
        buf[...] = quantized.astype(jnp.bfloat16).reshape(CLIPS, ROWS, C)

        def step(b, _):
            block_at(b, buf, all_taps, all_out, all_gain)
            return 0

        lax.fori_loop(0, 2, step, 0)
        for c in range(CLIPS):
            differ = buf[c].astype(jnp.float32) - v[t, c].astype(jnp.float32)
            square = differ * differ
            part = (
                square[:, :128] + square[:, 128:256] + square[:, 256:384] + square[:, 384:]
            )
            mean = jnp.sum(part.T, axis=0, keepdims=True) * (1.0 / C)
            errors[i, 2 * c : 2 * c + 1, :] = mean[:, :128]
            errors[i, 2 * c + 1 : 2 * c + 2, :] = mean[:, 128:]

    for i, t in enumerate(steps):
        pl.when(has_chunk(t, (2, 3)))(functools.partial(chunk, i, t))


def unpack(target, source):
    for c in range(CLIPS):
        row = source[2 * c : 2 * c + 2, :]
        target[c : c + 1, :] = jnp.concatenate([row[0:1], row[1:2]], axis=1)


def final_body(rows_total, order, mine, cross, given, e0, e34, error, loss):
    section = lax.axis_index("section")
    sums = jnp.where(section <= 1, mine[...], cross[...]) * (1.0 / rows_total)
    row = lax.broadcasted_iota(jnp.int32, sums.shape, 0)
    lane = lax.broadcasted_iota(jnp.int32, sums.shape, 1)
    averaged = jnp.zeros_like(sums)
    running = None
    for t in range(8):
        here = row == order[t]
        marginal = jnp.sum(jnp.where(here, sums, 0.0), axis=0, keepdims=True)
        running = marginal if t == 0 else 0.5 * running + 0.5 * marginal
        averaged = jnp.where(here, running, averaged)
    smoothed = jnp.where(lane < BITS, 0.05 + 0.9 * averaged, 0.5)
    term = smoothed * jnp.log(smoothed) + (1.0 - smoothed) * jnp.log(1.0 - smoothed)
    term = jnp.where(lane < BITS, term, jnp.where(lane == BITS, sums, 0.0))
    result = jnp.sum(term, axis=1, keepdims=True)
    flat = jnp.sum(jnp.where(row == lane, result, 0.0), axis=0)
    loss[...] = flat[:8]

    @pl.when(section <= 1)
    def _():
        unpack(error.at[0], given.at[0])
        unpack(error.at[1], given.at[1])

    @pl.when(section == 2)
    def _():
        unpack(error.at[0], e0.at[0])
        unpack(error.at[1], e34.at[0])

    @pl.when(section == 3)
    def _():
        unpack(error.at[0], e34.at[0])
        unpack(error.at[1], e34.at[1])


PAIR = ((0, 1), (1, 0), (2, 3), (3, 2))
CROSS = ((0, 3), (3, 0), (1, 2), (2, 1))


def shifted(x, axis, by):
    n = lax.axis_size(axis)
    return lax.ppermute(x, axis, [(i, (i + by) % n) for i in range(n)])


def within_corner(x, first):
    n, m = lax.axis_size("dp_0"), lax.axis_size("dp_1")
    pairs = []
    for i in range(n):
        for j in range(m):
            for core in range(2):
                to = (i ^ 1, j) if (core == 0) == first else (i, j ^ 1)
                pairs.append(((i * m + j) * 2 + core, (to[0] * m + to[1]) * 2 + core))
    return lax.ppermute(x, DP, pairs)


def encoder_sum(x):
    n = lax.axis_size(DP)
    x = x + lax.ppermute(x, "section", PAIR)
    return jnp.sum(lax.all_to_all(jnp.broadcast_to(x[None], (n, *x.shape)), DP, 0, 0), axis=0)


def on_device(pool, index, order, taps, out_weight, gain, quant_weight, quant_bias, post_weight):
    bf16, f32 = jnp.bfloat16, jnp.float32
    taps = taps.reshape(3 * C, C)
    out_weight = out_weight.reshape(C, C)
    dma = pltpu.SemaphoreType.DMA
    index = index.T
    encoder = (lax.axis_index("section") <= 1).astype(jnp.int32)
    gain, encoder = lax.optimization_barrier((gain, encoder))
    chunk = (CLIPS, ROWS, C)
    kinds = [((2, 3 * C, C), bf16), ((2, C, C), bf16), ((2, 8, C), f32)]

    pool, taps, out_weight = (
        pltpu.with_memory_space_constraint(x, pltpu.HBM) for x in (pool, taps, out_weight)
    )
    gain, qwt, post_weight, index = (
        pltpu.with_memory_space_constraint(x, pltpu.HBM)
        for x in (gain, quant_weight.T, post_weight, index)
    )
    qbias = pltpu.with_memory_space_constraint(quant_bias.reshape(1, BITS), pltpu.HBM)
    piece, second = call(
        prep_body,
        [HB] * 3,
        [((PIECE, 128), bf16), ((HALF, 128), bf16)],
        [pltpu.VMEM((1, C), bf16), dma((11,))],
    )(taps, out_weight, gain)
    mine = lax.ppermute(piece, "section", PAIR)
    second = lax.ppermute(second, "section", PAIR)
    v_kind = ((STEPS, *chunk), bf16)
    v, *weights, qw, qb, post = call(
        functools.partial(start_body, 2),
        [HB] * 8,
        [v_kind, *kinds, ((C, 128), bf16), ((8, 128), f32), ((CODE_ROWS, C), bf16)],
        [
            pltpu.SMEM(index.shape, jnp.int32),
            pltpu.VMEM((1, C), bf16),
            pltpu.VMEM((BITS, C), bf16),
            pltpu.VMEM((1, BITS), f32),
            pltpu.VMEM((BITS, C), bf16),
            dma((7 + STEPS * CLIPS,)),
        ],
        blocks=2,
    )(pool, index, taps, out_weight, gain, qwt, qbias, post_weight)
    mine, v = lax.optimization_barrier((mine, v))
    up = within_corner(mine, True)
    down = within_corner(mine, False)
    mine_s = shifted(mine, "dp_2", 1)
    (v,) = call(
        functools.partial(more_body, 2, STEPS), [VM] * 4, [v_kind], blocks=3, aliases={0: 0}
    )(v, *weights)
    up, down, second, mine_s, v = lax.optimization_barrier((up, down, second, mine_s, v))
    swapped = [mine_s] + [shifted(x, "dp_2", 1) for x in (second, down, up)]
    weights = call(
        join_body, [VM] + [ANY] * 7 + [VM] * 3, kinds, [dma((24,))], aliases={8: 0, 9: 1, 10: 2}
    )(mine, second, up, down, *swapped, *weights)

    def encode(steps, v, before, last):
        n = len(steps)
        return call(
            functools.partial(encode_body, steps, last),
            [VM] * (6 + len(before)),
            [
                v_kind,
                ((n, CODE_ROWS, CLIPS * ROWS), bf16),
                ((8 if last else CODE_ROWS, 128), f32),
            ],
            [pltpu.VMEM((CODE_ROWS, 128), f32)],
            blocks=2 * n,
            aliases={0: 0},
        )(v, *weights, qw, qb, *before)

    def decode(steps, v, codes):
        n = len(steps)
        return call(
            functools.partial(decode_body, steps),
            [VM] * 6,
            [((n, 8, 128), f32)],
            [pltpu.VMEM(chunk, bf16)],
            blocks=2 * n,
        )(v, *weights, post, codes)[0]

    v, first, stats = encode((0,), v, (), False)
    v, codes, stats = encode((1, 2), v, (stats,), False)
    codes_b = lax.ppermute(codes, "section", CROSS)
    v, codes, stats = encode((3, 4), v, (stats,), True)
    codes_c = lax.ppermute(codes, "section", ((0, 3), (1, 2)))
    first, codes_b, stats = lax.optimization_barrier((first, codes_b, stats))
    codes_a = lax.ppermute(first, "section", ((0, 2),))
    e12 = decode((1, 2), v, codes_b)
    e0 = decode((0,), v, codes_a)
    given = lax.ppermute(e12, "section", ((3, 0), (2, 1)))
    e34 = decode((3, 4), v, codes_c)
    stats, e0, e34, encoder = lax.optimization_barrier((stats, e0, e34, encoder))
    total = lax.cond(encoder == 1, encoder_sum, lambda x: 0.0 * x, stats)
    cross = lax.ppermute(total, "section", ((0, 3), (1, 2)))
    rows_total = float(CLIPS * lax.axis_size(DP) * ROWS)
    error, loss = call(
        functools.partial(final_body, rows_total),
        [SM] + [VM] * 5,
        [((2, CLIPS, ROWS), f32), ((8,), f32)],
    )(order, total, cross, given, e0, e34)
    return error, loss


def solution(mesh):
    torus = Mesh(
        mesh.devices.reshape(mesh.shape["section"], 4, 4, 2), ("section", "dp_0", "dp_1", "dp_2")
    )
    return jax.shard_map(
        on_device,
        mesh=torus,
        in_specs=(
            P(DP, None, None),
            P(None, DP),
            P(),
            P("section", None, None, None),
            P("section", None, None),
            P("section", None),
            P(),
            P(),
            P(),
        ),
        out_specs=(P("section", DP, None), P()),
        check_vma=False,
    )
```
